32 devices in a mesh: gx: 8 (over z, core), gy: 4 (over y, x).
Axes of the slice: x: 2, y: 2, z: 4, core: 2. Of those that a mesh axis runs over, the one named last changes fastest.
Arguments:
- earlier_heat_field: float32 [6, 1024, 512], P(None, 'gx', 'gy'), may hold values from -6 to 6
- substance_per_voxel: int32 [6, 1024, 512], P(None, 'gx', 'gy'), may hold values from 0 to 7
- patch_wattage_category: int32 [64, 32], P('gx', 'gy'), may hold values from 0 to 63
- planar_coupling: float32 [8], replicated, may hold values from 0.3 to 3
- vertical_coupling_per_substance: float32 [8], replicated, may hold values from 0.05 to 0.5
- heat_mass_ratio: float32 [8], replicated, may hold values from 2e-05 to 0.0002
- wattage_per_category: float32 [64], replicated, may hold values from 2e-06 to 2e-05
Outputs:
- temperature: float32 [6, 1024, 512], P(None, 'gx', 'gy')
The draws below stay inside these ranges and needn't reach their ends.
All inputs are finite; a program needn't handle non-finite values.
Results may differ from the reference program's by a relative error of at most 0.0003.
Values sent between devices are 32-bit elements; how exact they have to be, the bound alone decides.
A program may use at most 192 MiB of HBM per device.

```python
import math
import jax
import jax.numpy as jnp
from jax import lax

DIE_COUNT = 6
MATERIALS = 8
POWER_LEVELS = 64
TILE = 16
LEVELS = 6
SWEEPS = 2
COARSE_ITERS = 12
CX = 128
GRID_LENGTH = 1024
GRID_WIDTH = 512


def draw_substance_per_voxel(key, part):
    block_key = jax.random.fold_in(key, 11)
    noise_key = jax.random.fold_in(key, 23)
    pick_key = jax.random.fold_in(key, 37)
    blocks = jax.random.randint(block_key, (DIE_COUNT, GRID_LENGTH // CX, GRID_WIDTH // CX), 0, MATERIALS)
    spread = jnp.repeat(jnp.repeat(blocks, CX, axis=1), CX, axis=2)
    shape = (DIE_COUNT, GRID_LENGTH, GRID_WIDTH)
    noise = jax.random.randint(noise_key, shape, 0, MATERIALS)
    pick = jax.random.randint(pick_key, shape, 0, 4)
    return jnp.where(pick == 0, noise, spread).astype(jnp.int32)


def plant(values, stream_key, smallest, high):
    dims = values.shape
    place = [jax.random.randint(jax.random.fold_in(stream_key, axis), (), 0, dims[axis]) for axis in range(len(dims))]
    values = values.at[tuple(place)].set(smallest)
    longest = dims.index(max(dims))
    place[longest] = (place[longest] + 1) % dims[longest]
    return values.at[tuple(place)].set(high)


def shard_levels(rng, dims, shards, least, top_value):
    loudness, own = 1.0, jax.random.fold_in(rng, 6)
    for axis_at, blocks in shards:
        draws = jnp.exp(jax.random.uniform(jax.random.fold_in(own, axis_at), (blocks,), jnp.float32, least / len(shards), top_value / len(shards)))
        loudness = loudness * jnp.repeat(draws, dims[axis_at] // blocks).reshape([-1 if axis == axis_at else 1 for axis in range(len(dims))])
    return loudness


def scatter_about(own_key, dims, width, limit, shards=(), held_as=jnp.bfloat16):
    loudness = shard_levels(own_key, dims, shards, -0.22, 0.18) if shards else 1.0
    values = jax.random.normal(own_key, dims, jnp.float32) * width * loudness
    return jnp.minimum(jnp.maximum(values, -limit), limit).astype(held_as)


def setup_inputs(seed: int = 0) -> dict:
    seeds = jax.random.split(jax.random.key(seed), 8)
    return {
        "earlier_heat_field": scatter_about(seeds[0], (DIE_COUNT, GRID_LENGTH, GRID_WIDTH), 1.0, 6.0, ((1, 8), (2, 4)), jnp.float32),
        "substance_per_voxel": draw_substance_per_voxel(jax.random.fold_in(seeds[7], 71), 0),
        "patch_wattage_category": plant(jax.random.randint(seeds[2], (GRID_LENGTH // TILE, GRID_WIDTH // TILE), 0, POWER_LEVELS), jax.random.fold_in(seeds[2], 1), 0, POWER_LEVELS - 1).astype(jnp.int32),
        "planar_coupling": jnp.clip(jnp.exp(jax.random.uniform(seeds[3], (MATERIALS,), jnp.float32, math.log(0.3), math.log(3.0))), 0.3, 3.0),
        "vertical_coupling_per_substance": jnp.clip(jnp.exp(jax.random.uniform(seeds[4], (MATERIALS,), jnp.float32, math.log(0.05), math.log(0.5))), 0.05, 0.5),
        "heat_mass_ratio": jnp.clip(jnp.exp(jax.random.uniform(seeds[5], (MATERIALS,), jnp.float32, math.log(1.9999999494757503e-05), math.log(0.0002))), 1.9999999494757503e-05, 0.0002),
        "wattage_per_category": jnp.clip(jnp.exp(jax.random.uniform(seeds[6], (POWER_LEVELS,), jnp.float32, math.log(1.9999999949504854e-06), math.log(1.9999999494757503e-05))), 1.9999999949504854e-06, 1.9999999494757503e-05),
    }


def previous(values, dimension):
    widths = [(0, 0)] * values.ndim
    widths[dimension] = (1, 0)
    return lax.slice_in_dim(jnp.pad(values, widths), 0, values.shape[dimension], axis=dimension)


def following(values, dimension):
    widths = [(0, 0)] * values.ndim
    widths[dimension] = (0, 1)
    return lax.slice_in_dim(jnp.pad(values, widths), 1, values.shape[dimension] + 1, axis=dimension)


def stencil(lateral, vertical, capacity_diagonal, inside, factor):
    row_before = factor * 0.5 * (lateral + previous(lateral, 1))
    row_after = factor * 0.5 * (lateral + following(lateral, 1))
    col_before = factor * 0.5 * (lateral + previous(lateral, 2))
    col_after = factor * 0.5 * (lateral + following(lateral, 2))
    faces = 0.5 * (vertical[1:] + vertical[:-1])
    no_face = jnp.zeros_like(vertical[:1])
    layer_below = jnp.concatenate([no_face, faces], 0)
    layer_above = jnp.concatenate([faces, no_face], 0)
    diagonal = capacity_diagonal + row_before + row_after + col_before + col_after + layer_below + layer_above
    diagonal = jnp.where(inside > 0, diagonal, 1.0)
    return (row_before, row_after, col_before, col_after, layer_below, layer_above, diagonal)


def coupled(values, weights):
    summed = weights[0] * previous(values, 1) + weights[1] * following(values, 1)
    summed = summed + weights[2] * previous(values, 2) + weights[3] * following(values, 2)
    return summed + weights[4] * previous(values, 0) + weights[5] * following(values, 0)


def parity(extent):
    summed = lax.broadcasted_iota(jnp.int32, extent, 0) + lax.broadcasted_iota(jnp.int32, extent, 1)
    return (summed + lax.broadcasted_iota(jnp.int32, extent, 2)) % 2


def restrict(values):
    layers, height, breadth = values.shape
    blocks = values.reshape(layers, height // 2, 2, breadth // 2, 2)
    return (blocks[:, :, 0, :, 0] + blocks[:, :, 1, :, 0] + blocks[:, :, 0, :, 1] + blocks[:, :, 1, :, 1]) * 0.25


def prolong(values):
    return jnp.repeat(jnp.repeat(values, 2, axis=1), 2, axis=2)


def lookup(labels, entries):
    summed = jnp.zeros(labels.shape, entries.dtype)
    for number in range(entries.shape[0]):
        summed = summed + jnp.where(labels == number, entries[number], 0.0)
    return summed


def conjugate(source_vector, weights):
    solution = jnp.zeros_like(source_vector)
    residue = source_vector
    precond = residue / weights[6]
    search = precond
    inner = jnp.sum(residue * precond)
    for step_index in range(COARSE_ITERS):
        image = weights[6] * search - coupled(search, weights)
        alpha_step = inner / jnp.sum(search * image)
        solution = solution + alpha_step * search
        residue = residue - alpha_step * image
        precond = residue / weights[6]
        inner_next = jnp.sum(residue * precond)
        search = precond + (inner_next / inner) * search
        inner = inner_next
    return solution


def smooth(present_guess, source_vector, weights, colours):
    for sweep_index in range(SWEEPS):
        for colour in (0, 1):
            candidate = (source_vector + coupled(present_guess, weights)) / weights[6]
            present_guess = jnp.where(colours == colour, candidate, present_guess)
    return present_guess


def reference(earlier_heat_field, substance_per_voxel, patch_wattage_category, planar_coupling, vertical_coupling_per_substance, heat_mass_ratio, wattage_per_category):
    lateral = lookup(substance_per_voxel, planar_coupling)
    vertical = lookup(substance_per_voxel, vertical_coupling_per_substance)
    capacity_diagonal = lookup(substance_per_voxel, heat_mass_ratio)
    heat = jnp.repeat(jnp.repeat(lookup(patch_wattage_category, wattage_per_category), TILE, axis=0), TILE, axis=1)
    source_vector = capacity_diagonal * earlier_heat_field
    source_vector = jnp.concatenate([source_vector[:1] + heat[None], source_vector[1:]], 0)
    coefficients = [(lateral, vertical, capacity_diagonal)]
    for level_index in range(LEVELS):
        last = coefficients[-1]
        coefficients.append((restrict(last[0]), restrict(last[1]), restrict(last[2])))
    present_guess = earlier_heat_field
    saved = []
    for level_index in range(LEVELS):
        level_coef = coefficients[level_index]
        weights = stencil(level_coef[0], level_coef[1], level_coef[2], jnp.ones_like(source_vector), 0.25 ** level_index)
        colours = parity(source_vector.shape)
        present_guess = smooth(present_guess, source_vector, weights, colours)
        residual = source_vector - (weights[6] * present_guess - coupled(present_guess, weights))
        saved.append((present_guess, source_vector, weights, colours))
        source_vector = restrict(residual)
        present_guess = jnp.zeros_like(source_vector)
    coarse_coef = coefficients[LEVELS]
    coarse_weights = stencil(coarse_coef[0], coarse_coef[1], coarse_coef[2], jnp.ones_like(source_vector), 0.25 ** LEVELS)
    correction = conjugate(source_vector, coarse_weights)
    for level_index in reversed(range(LEVELS)):
        present_guess, source_vector, weights, colours = saved[level_index]
        present_guess = smooth(present_guess + prolong(correction), source_vector, weights, colours)
        correction = present_guess
    return correction
```

```python
import functools

import jax
import jax.numpy as jnp
from jax import lax
from jax.experimental import pallas as pl
from jax.experimental.pallas import tpu as pltpu
from jax.sharding import PartitionSpec as P

TILE = 16
LEVELS = 6
SWEEPS = 2
COARSE_ITERS = 12
LOCAL = 3
FRAME = 64
WIDE = 56
PAD = 8
F32 = jnp.float32
VM = 60 * 1024 * 1024


def up_to(count, step):
    return -(-count // step) * step


def spans(low, high, columns):
    step = max(8, 8 * (4096 // columns // 8) * 2)
    return [(r, min(step, high - r)) for r in range(low, high, step)]


def split_dot(matrix_left, values, matrix_right):
    def parts(x):
        a = x.astype(jnp.bfloat16)
        x = x - a.astype(F32)
        b = x.astype(jnp.bfloat16)
        x = x - b.astype(F32)
        return a, b, x.astype(jnp.bfloat16)

    dot = functools.partial(jnp.dot, preferred_element_type=F32)
    a, b, c = parts(values)
    values = (dot(matrix_left, c) + dot(matrix_left, b)) + dot(matrix_left, a)
    a, b, c = parts(values)
    return (dot(c, matrix_right) + dot(b, matrix_right)) + dot(a, matrix_right)


def pairs(rows, columns, weight, tall):
    r = lax.broadcasted_iota(jnp.int32, (rows, columns), 0)
    c = lax.broadcasted_iota(jnp.int32, (rows, columns), 1)
    hit = (r // 2 == c) if tall else (c // 2 == r)
    return jnp.where(hit, F32(weight), F32(0.0)).astype(jnp.bfloat16)


def restrict(fine, coarse, layers_fine, layers_coarse):
    rf, cf = fine.shape[1] - 2 * PAD, fine.shape[2]
    rc, cc = coarse.shape[1] - 2 * PAD, coarse.shape[2]
    left = pairs(rc, rf, 0.5, False)
    right = pairs(cf, cc, 0.5, True)

    def body(k, carry):
        x = fine[k + layers_fine, PAD : PAD + rf, :]
        coarse[k + layers_coarse, PAD : PAD + rc, :] = split_dot(left, x, right)
        return carry

    lax.fori_loop(0, 6, body, 0)


def prolong_add(coarse, fine):
    rf, cf = fine.shape[1] - 2 * PAD, fine.shape[2]
    rc, cc = coarse.shape[1] - 2 * PAD, coarse.shape[2]
    left = pairs(rf, rc, 1.0, True)
    right = pairs(cc, cf, 1.0, False)

    def body(k, carry):
        x = coarse[k + 1, PAD : PAD + rc, :]
        fine[k + 1, PAD : PAD + rf, :] += split_dot(left, x, right)
        return carry

    lax.fori_loop(0, 6, body, 0)


def build(coef, weights, scale):
    lat, ver, sto = coef
    wr, wc, wv, inv, diag = weights
    rows, columns = lat.shape[1] - 2 * PAD, lat.shape[2]
    half = F32(0.5 * scale)
    wr[...] = jnp.zeros_like(wr)
    wv[0] = jnp.zeros(wv.shape[1:], F32)
    wv[6] = jnp.zeros(wv.shape[1:], F32)

    def faces(k, carry):
        for r, n in spans(PAD, PAD + rows, columns):
            here = lat[k, r : r + n, :]
            wr[k, r : r + n, :] = half * (here + lat[k, r - 1 : r - 1 + n, :])
            wc[k, r : r + n, :] = half * (here + pltpu.roll(here, 1, 1))
        wr[k, PAD + rows : PAD + rows + 8, :] = half * (
            lat[k, PAD + rows : PAD + rows + 8, :]
            + lat[k, PAD + rows - 1 : PAD + rows + 7, :]
        )
        return carry

    lax.fori_loop(0, 6, faces, 0)

    def layer(k, carry):
        for r, n in spans(PAD, PAD + rows, columns):
            wv[k, r : r + n, :] = F32(0.5) * (ver[k, r : r + n, :] + ver[k - 1, r : r + n, :])
        return carry

    lax.fori_loop(1, 6, layer, 0)

    def total(k, carry):
        for r, n in spans(PAD, PAD + rows, columns):
            left = wc[k, r : r + n, :]
            s = sto[k, r : r + n, :]
            d = s + wr[k, r : r + n, :] + wr[k, r + 1 : r + 1 + n, :]
            d = d + left + pltpu.roll(left, columns - 1, 1)
            d = d + wv[k, r : r + n, :] + wv[k + 1, r : r + n, :]
            diag[k, r : r + n, :] = d
            inv[k, r : r + n, :] = jnp.where(s > 0.0, F32(1.0) / jnp.where(s > 0.0, d, 1.0), 0.0)
        return carry

    lax.fori_loop(0, 6, total, 0)


def beside(u, weights, k, r, n, here):
    wr, wc, wv = weights[:3]
    columns = u.shape[2]
    left = wc[k, r : r + n, :]
    summed = wr[k, r : r + n, :] * u[k + 1, r - 1 : r - 1 + n, :]
    summed += wr[k, r + 1 : r + 1 + n, :] * u[k + 1, r + 1 : r + 1 + n, :]
    summed += left * pltpu.roll(here, 1, 1)
    summed += pltpu.roll(left * here, columns - 1, 1)
    summed += wv[k, r : r + n, :] * u[k, r : r + n, :]
    summed += wv[k + 1, r : r + n, :] * u[k + 2, r : r + n, :]
    return summed


def smooth(u, rhs, weights, low, high):
    inv = weights[3]
    columns = u.shape[2]

    def half_sweep(step, carry):
        colour = step % 2

        def layer(k, inner):
            for r, n in spans(PAD + low, PAD + high, columns):
                here = u[k + 1, r : r + n, :]
                new = (rhs[k, r : r + n, :] + beside(u, weights, k, r, n, here)) * inv[
                    k, r : r + n, :
                ]
                odd = lax.broadcasted_iota(jnp.int32, (n, columns), 0)
                odd = (odd + lax.broadcasted_iota(jnp.int32, (n, columns), 1) + k + colour) & 1
                u[k + 1, r : r + n, :] = jnp.where(odd == 0, new, here)
            return inner

        return lax.fori_loop(0, 6, layer, carry)

    lax.fori_loop(0, 2 * SWEEPS, half_sweep, 0)


def residual(u, rhs, weights, out):
    diag = weights[4]
    rows, columns = u.shape[1] - 2 * PAD, u.shape[2]

    def layer(k, carry):
        for r, n in spans(PAD, PAD + rows, columns):
            here = u[k + 1, r : r + n, :]
            out[k, r : r + n, :] = rhs[k, r : r + n, :] - (
                diag[k, r : r + n, :] * here - beside(u, weights, k, r, n, here)
            )
        return carry

    lax.fori_loop(0, 6, layer, 0)


def down_level(index, u, rhs, coef, weights, temp, nxt_rhs, nxt_coef, low, high):
    if index > 0:
        u[...] = jnp.zeros_like(u)
    build(coef, weights, 0.25**index)
    smooth(u, rhs, weights, low, high)
    residual(u, rhs, weights, temp)
    restrict(temp, nxt_rhs, 0, 0)
    for mine, following in zip(coef, nxt_coef):
        following[...] = jnp.zeros_like(following)
        restrict(mine, following, 0, 0)


def down_kernel(x_ref, lat_t, ver_t, sto_t, *refs):
    outs, packed, scratch = refs[: 6 * LOCAL], refs[6 * LOCAL], refs[6 * LOCAL + 1 :]
    level = [outs[6 * i : 6 * i + 6] for i in range(LOCAL)]
    coarse = scratch[5 * LOCAL :]
    own = [scratch[5 * i : 5 * i + 5] for i in range(LOCAL)]
    u, rhs = level[0][:2]
    lat, ver, sto = own[0][:3]
    rows, columns = x_ref.shape[1:]
    for ref in (u, lat):
        ref[...] = jnp.zeros_like(ref)

    def look(k, carry):
        for r, n in spans(0, rows, columns):
            labels = x_ref[k + 6, r : r + n, :]
            a = jnp.zeros((n, columns), F32)
            b, c = a, a
            for m in range(lat_t.shape[0]):
                hit = labels == F32(m + 1)
                a = jnp.where(hit, lat_t[m], a)
                b = jnp.where(hit, ver_t[m], b)
                c = jnp.where(hit, sto_t[m], c)
            t = x_ref[k, r : r + n, :]
            lat[k, r + PAD : r + PAD + n, :] = a
            ver[k, r + PAD : r + PAD + n, :] = b
            sto[k, r + PAD : r + PAD + n, :] = c
            u[k + 1, r + PAD : r + PAD + n, :] = t
            rhs[k, r + PAD : r + PAD + n, :] = c * t
        return carry

    lax.fori_loop(0, 6, look, 0)
    rhs[0, PAD : PAD + rows, :] += x_ref[12]
    for i in range(LOCAL):
        last = i == LOCAL - 1
        size = level[i][0].shape[1] - 2 * PAD
        cut = 8 if i < 2 else 0
        down_level(
            i,
            level[i][0],
            level[i][1],
            own[i][:3],
            level[i][2:6] + own[i][3:4],
            own[i][4],
            coarse[0] if last else level[i + 1][1],
            coarse[1:4] if last else own[i + 1][:3],
            cut,
            size - cut,
        )
    per, h, lanes = packed.shape
    off = FRAME >> LOCAL
    w = lanes * per // 24
    lane = lax.broadcasted_iota(jnp.int32, (h, lanes), 1) // w
    for i in range(per):
        total = jnp.zeros((h, lanes), F32)
        for j in range(24 // per):
            at = j * per + i
            x = coarse[at // 6][at % 6, PAD + off : PAD + off + h, :]
            total = jnp.where(lane == j, pltpu.roll(x, (j * w - off) % lanes, 1), total)
        packed[i] = total


def coarse_kernel(rows_of, g_ref, out_ref, *scratch):
    count = LEVELS - LOCAL
    blocks, per, h, lanes = g_ref.shape
    w = lanes * per // 24
    columns_of = blocks // rows_of
    rows = rows_of * h
    data = [scratch[11 * i : 11 * i + 11] for i in range(count + 1)]
    for j in range(4):
        ref = data[0][(1, 6, 7, 8)[j]]
        ref[...] = jnp.zeros_like(ref)
    lane = lax.broadcasted_iota(jnp.int32, (h, lanes), 1) // w

    def take(gx, carry):
        row = pl.multiple_of(PAD + gx * h, 8)
        for at in range(24):
            j, i = at // per, at % per
            ref = data[0][(1, 6, 7, 8)[at // 6]]
            for start in range(0, columns_of, lanes // w):
                total = jnp.zeros((h, lanes), F32)
                for gy in range(start, min(start + lanes // w, columns_of)):
                    x = g_ref[gx * columns_of + gy, i]
                    x = pltpu.roll(x, ((gy - start - j) * w) % lanes, 1)
                    total = jnp.where(lane == gy - start, x, total)
                ref[at % 6, pl.ds(row, h), start * w : start * w + lanes] = total
        return carry

    lax.fori_loop(0, rows_of, take, 0)
    for i in range(count):
        u, rhs, wr, wc, wv, inv, lat, ver, sto, diag, temp = data[i]
        down_level(
            LOCAL + i, u, rhs, (lat, ver, sto), (wr, wc, wv, inv, diag), temp,
            data[i + 1][1], data[i + 1][6:9], 0, u.shape[1] - 2 * PAD,
        )
    u, rhs, wr, wc, wv, inv, lat, ver, sto, diag, temp = data[count]
    build((lat, ver, sto), (wr, wc, wv, inv, diag), 0.25**LEVELS)
    n, columns = u.shape[1] - 2 * PAD, u.shape[2]
    u[...] = jnp.zeros_like(u)
    mid = slice(PAD, PAD + n)

    def summed(x):
        x = jnp.sum(x, axis=0)
        return jnp.sum(jnp.sum(x, axis=0, keepdims=True), axis=1, keepdims=True)

    r0 = rhs[:, mid, :]
    z0 = r0 * inv[:, mid, :]
    u[1:7, mid, :] = z0
    temp[:, mid, :] = r0
    lat[:, mid, :] = jnp.zeros_like(r0)

    def step(_, rz):
        p = u[1:7, mid, :]
        image = jnp.stack(
            [diag[k, mid, :] * p[k] - beside(u, (wr, wc, wv), k, PAD, n, p[k]) for k in range(6)]
        )
        alpha = rz / summed(p * image)
        lat[:, mid, :] += alpha[None] * p
        r = temp[:, mid, :] - alpha[None] * image
        temp[:, mid, :] = r
        z = r * inv[:, mid, :]
        rz_new = summed(r * z)
        u[1:7, mid, :] = z + (rz_new / rz)[None] * p
        return rz_new

    lax.fori_loop(0, COARSE_ITERS, step, summed(r0 * z0))
    u[1:7, mid, :] = lat[:, mid, :]
    for i in reversed(range(count)):
        u, rhs, wr, wc, wv, inv = data[i][:6]
        prolong_add(data[i + 1][0], u)
        smooth(u, rhs, (wr, wc, wv, inv), 0, u.shape[1] - 2 * PAD)
    u = data[0][0]

    def give(k, carry):
        out_ref[k] = u[k + 1, PAD : PAD + out_ref.shape[1], :]
        return carry

    lax.fori_loop(0, 6, give, 0)


def up_kernel(e_ref, *refs):
    ins = refs[: 6 * LOCAL]
    out_ref = refs[6 * LOCAL]
    us = refs[6 * LOCAL + 1 :]
    correction = e_ref
    for i in reversed(range(LOCAL)):
        u, rhs, wr, wc, wv, inv = ins[6 * i : 6 * i + 6]
        mine = us[i]
        mine[...] = u[...]
        prolong_add(correction, mine)
        size = u.shape[1] - 2 * PAD
        cut = (56, 24, 8)[i]
        smooth(mine, rhs, (wr, wc, wv, inv), cut, size - cut)
        correction = mine
    rows, columns = out_ref.shape[1:]
    wide = correction.shape[2]

    def give(k, carry):
        x = correction[k + 1, PAD + FRAME : PAD + FRAME + rows, :]
        out_ref[k] = pltpu.roll(x, wide - FRAME, 1)[:, :columns]
        return carry

    lax.fori_loop(0, 6, give, 0)


def extended(block, axis, dim):
    count = lax.axis_size(axis)
    forward = [(i, i + 1) for i in range(count - 1)]
    backward = [(target, source) for source, target in forward]
    size = block.shape[dim]
    low = lax.ppermute(lax.slice_in_dim(block, size - WIDE, None, axis=dim), axis, forward)
    high = lax.ppermute(lax.slice_in_dim(block, 0, WIDE, axis=dim), axis, backward)
    shape = list(block.shape)
    shape[dim] = FRAME - WIDE
    edge = jnp.zeros(shape, block.dtype)
    return jnp.concatenate([edge, low, block, high, edge], axis=dim)


def lookup(labels, entries):
    summed = jnp.zeros(labels.shape, entries.dtype)
    for number in range(entries.shape[0]):
        summed = summed + jnp.where(labels == number, entries[number], 0.0)
    return summed


def frame(layers, rows, columns):
    return (layers, rows + 2 * PAD, columns)


def on_device(field, substance, patch, planar, vertical, storage, wattage):
    levels = lax.broadcasted_iota(patch.dtype, patch.shape + wattage.shape, 2)
    chosen = jnp.where(patch[:, :, None] == levels, wattage[None, None, :], 0.0)
    small = lax.optimization_barrier(jnp.sum(chosen, axis=2))
    tall = jnp.repeat(jnp.eye(patch.shape[0], dtype=F32), TILE, axis=0)
    flat = jnp.repeat(jnp.eye(patch.shape[1], dtype=F32), TILE, axis=1)
    exact = functools.partial(jnp.dot, precision=lax.Precision.HIGHEST)
    heat = exact(exact(tall, small), flat)
    x = jnp.concatenate([field, substance.astype(F32) + 1.0, heat[None]], 0)
    x = extended(extended(x, "gy", 2), "gx", 1)
    local_rows, local_cols = field.shape[1:]
    vmem = pl.BlockSpec(memory_space=pltpu.VMEM)
    smem = pl.BlockSpec(memory_space=pltpu.SMEM)
    params = pltpu.CompilerParams(vmem_limit_bytes=VM)
    dims = []
    for i in range(LOCAL + 1):
        dims.append(
            (
                up_to((local_rows + 2 * FRAME) >> i, 8),
                up_to((local_cols + 2 * FRAME) >> i, 128),
            )
        )
    shapes, scratch = [], []
    for i in range(LOCAL):
        shapes += [jax.ShapeDtypeStruct(frame(n, *dims[i]), F32) for n in (8, 6, 6, 6, 7, 6)]
        scratch += [pltpu.VMEM(frame(6, *dims[i]), F32) for _ in range(5)]
    scratch += [pltpu.VMEM(frame(6, *dims[LOCAL]), F32) for _ in range(4)]
    h, w = local_rows >> LOCAL, local_cols >> LOCAL
    off = FRAME >> LOCAL
    lanes = dims[LOCAL][1]
    result = pl.pallas_call(
        down_kernel,
        out_shape=shapes + [jax.ShapeDtypeStruct((24 * w // lanes, h, lanes), F32)],
        in_specs=[vmem] + [smem] * 3,
        out_specs=[vmem] * (6 * LOCAL + 1),
        scratch_shapes=scratch,
        compiler_params=params,
    )(x, planar, vertical, storage)
    levels, mine = result[: 6 * LOCAL], result[6 * LOCAL]
    nx, ny = lax.axis_size("gx"), lax.axis_size("gy")
    whole = lax.all_gather(mine, ("gx", "gy"), axis=0, tiled=False)
    sizes = [
        (up_to(((nx * h) >> i) + 1, 8), up_to(((ny * w) >> i) + 1, 128))
        for i in range(LEVELS - LOCAL + 1)
    ]
    scratch = []
    for size in sizes:
        scratch += [
            pltpu.VMEM(frame(n, *size), F32) for n in (8, 6, 6, 6, 7, 6, 6, 6, 6, 6, 6)
        ]
    solved = pl.pallas_call(
        functools.partial(coarse_kernel, nx),
        out_shape=jax.ShapeDtypeStruct((6,) + sizes[0], F32),
        in_specs=[vmem],
        out_specs=vmem,
        scratch_shapes=scratch,
        compiler_params=params,
    )(whole)
    solved = jnp.pad(solved, ((1, 1), (off, off), (off, off)))
    zero = jnp.int32(0)
    window = lax.dynamic_slice(
        solved,
        (zero, lax.axis_index("gx") * h, lax.axis_index("gy") * w),
        (8, h + 2 * off, w + 2 * off),
    )
    r3, c3 = dims[LOCAL]
    window = jnp.pad(window, ((0, 0), (PAD, PAD), (0, c3 - (w + 2 * off))))
    return pl.pallas_call(
        up_kernel,
        out_shape=jax.ShapeDtypeStruct(field.shape, F32),
        in_specs=[vmem] * (1 + 6 * LOCAL),
        out_specs=vmem,
        scratch_shapes=[pltpu.VMEM(frame(8, *dims[i]), F32) for i in range(LOCAL)],
        compiler_params=params,
    )(window, *levels)


def solution(mesh):
    placed = (P(None, "gx", "gy"), P(None, "gx", "gy"), P("gx", "gy"), P(), P(), P(), P())
    return jax.shard_map(
        on_device, mesh=mesh, in_specs=placed, out_specs=P(None, "gx", "gy"), check_vma=False
    )
```

```python
import functools

import jax
import jax.numpy as jnp
from jax import lax
from jax.experimental import pallas as pl
from jax.experimental.pallas import tpu as pltpu
from jax.sharding import PartitionSpec as P

TILE = 16
LEVELS = 6
COARSE_ITERS = 12
LOCAL = 3
HALO = 8
BASE = 16
LEFT = 16
LANES = 128
F32 = jnp.float32
VM = 63 * 1024 * 1024
MESH = pl.DeviceIdType.MESH
SIDES = ((-1, 0), (1, 0), (0, -1), (0, 1), (-1, -1), (-1, 1), (1, -1), (1, 1))


def up_to(count, step):
    return -(-count // step) * step


def spans(low, high, columns):
    step = max(8, 48 * LANES // columns // 8 * 8)
    return [(r, min(step, high - r)) for r in range(low, high, step)]


def lane_of(shape):
    return lax.broadcasted_iota(jnp.int32, shape, len(shape) - 1)


def row_of(shape):
    return lax.broadcasted_iota(jnp.int32, shape, 0)


def split_dot(values, matrix, terms=3):
    total = None
    pieces = []
    for _ in range(terms):
        piece = values.astype(jnp.bfloat16)
        values = values - piece.astype(F32)
        pieces.append(piece)
    for piece in reversed(pieces):
        part = jnp.dot(piece, matrix, preferred_element_type=F32)
        total = part if total is None else total + part
    return total


def chosen(hit):
    return jnp.where(hit, F32(1.0), F32(0.0)).astype(jnp.bfloat16)


def near(dx, dy):
    ok = None
    for axis, step in (("gx", dx), ("gy", dy)):
        if step == 0:
            continue
        at = lax.axis_index(axis)
        this = (at + step < lax.axis_size(axis)) if step > 0 else (at + step >= 0)
        ok = this if ok is None else jnp.logical_and(ok, this)
    return ok


class Exchange:
    def __init__(self, width, rows, count, row_refs):
        self.width, self.rows, self.count = width, rows, count
        self.per = LANES // width
        self.packs = -(-count // self.per)
        self.row_refs = row_refs

    def scratch(self):
        packed = pltpu.VMEM((2, self.packs, self.rows, LANES), F32)
        landed = pltpu.VMEM((2, self.packs, self.rows + 2 * HALO, LANES), F32)
        tops = [pltpu.VMEM((2, n, HALO, LANES), F32) for n in self.row_refs]
        sems = pltpu.SemaphoreType.DMA((6 + 2 * len(self.row_refs),))
        return [packed, landed, sems, sems] + tops

    def bind(self, refs):
        self.packed, self.landed, self.send, self.recv = refs[:4]
        self.tops = refs[4 : 4 + len(self.row_refs)]
        return refs[4 + len(self.row_refs) :]

    def clear(self):
        self.landed[...] = jnp.zeros_like(self.landed)
        for top in self.tops:
            top[...] = jnp.zeros_like(top)

    def copies(self, sources):
        n = self.rows
        gx, gy = lax.axis_index("gx"), lax.axis_index("gy")
        out = []
        at = 0

        def add(dx, dy, source, target):
            nonlocal at
            out.append((dx, dy, source, target, at))
            at += 1

        for dy, side in ((1, 0), (-1, 1)):
            packed = self.packed.at[side]
            landed = self.landed.at[side]
            add(0, dy, packed, landed.at[:, HALO : HALO + n, :])
            add(1, dy, packed.at[:, n - HALO : n, :], landed.at[:, 0:HALO, :])
            add(-1, dy, packed.at[:, 0:HALO, :], landed.at[:, HALO + n : n + 2 * HALO, :])
        for source, top in zip(sources, self.tops):
            add(1, 0, source.at[:, BASE + n - HALO : BASE + n, :], top.at[0])
            add(-1, 0, source.at[:, BASE : BASE + HALO, :], top.at[1])
        made = []
        for dx, dy, source, target, i in out:
            copy = pltpu.make_async_remote_copy(
                src_ref=source,
                dst_ref=target,
                send_sem=self.send.at[i],
                recv_sem=self.recv.at[i],
                device_id=(gx + dx, gy + dy),
                device_id_type=MESH,
            )
            made.append((dx, dy, copy))
        return made

    def start(self, planes, sources):
        w = self.width
        n = self.rows
        for pack in range(self.packs):
            group = planes[pack * self.per : (pack + 1) * self.per]
            for r, m in spans(0, n, LANES):
                lane = lane_of((m, LANES)) // w
                right = jnp.zeros((m, LANES), F32)
                left = right
                for p, (ref, where) in enumerate(group):
                    x = ref[where + (slice(BASE + r, BASE + r + m),)]
                    hit = lane == p
                    a = pltpu.roll(x, (p * w - (LEFT + 64 - w)) % LANES, 1)
                    b = pltpu.roll(x, (p * w - LEFT) % LANES, 1)
                    right = jnp.where(hit, a, right)
                    left = jnp.where(hit, b, left)
                self.packed[0, pack, r : r + m, :] = right
                self.packed[1, pack, r : r + m, :] = left
        self.sources = sources
        for dx, dy, copy in self.copies(sources):
            pl.when(near(dx, dy))(copy.start)

    def finish(self):
        for dx, dy, copy in self.copies(self.sources):
            pl.when(near(dx, dy))(copy.wait_send)
            pl.when(near(-dx, -dy))(copy.wait_recv)

    def unpack(self, planes, tops, targets):
        w = self.width
        n = self.rows
        for i, (ref, where) in enumerate(planes):
            pack, p = i // self.per, i % self.per
            target, place = targets[i]
            pieces = [(0, HALO, 0)]
            pieces += [(HALO + r, m, None) for r, m in spans(0, n, LANES)]
            pieces += [(HALO + n, HALO, 1)]
            for r, m, side in pieces:
                if side is None:
                    x = ref[where + (slice(BASE - HALO + r, BASE - HALO + r + m),)]
                else:
                    top, plane = tops[i]
                    x = top[side, plane]
                lane = lane_of((m, LANES))
                a = pltpu.roll(self.landed[0, pack, r : r + m, :], (LEFT - w - p * w) % LANES, 1)
                b = pltpu.roll(self.landed[1, pack, r : r + m, :], (LEFT + 64 - p * w) % LANES, 1)
                x = jnp.where((lane >= LEFT - w) & (lane < LEFT), a, x)
                x = jnp.where((lane >= LEFT + 64) & (lane < LEFT + 64 + w), b, x)
                target[place + (slice(BASE - HALO + r, BASE - HALO + r + m),)] = x


def build(coef, wr, wc, wv, scale, gap, low, high):
    columns = coef.shape[2]
    half = F32(0.5 * scale)

    def faces(k, carry):
        for r, n in spans(low, high, columns):
            lane = lane_of((n, columns))
            here = coef[k, r : r + n, :]
            wr[k, r : r + n, :] = half * (here + coef[k, r - 1 : r - 1 + n, :])
            before = jnp.where(lane < gap, 0.0, pltpu.roll(here, gap, 1))
            wc[k, r : r + n, :] = jnp.where(lane < gap, 0.0, half * (here + before))
        here = coef[k, high : high + 8, :]
        wr[k, high : high + 8, :] = half * (here + coef[k, high - 1 : high + 7, :])
        for r, n in spans(low, high, columns):
            inside = F32(0.5) * (coef[6 + k, r : r + n, :] + coef[5 + k, r : r + n, :])
            wv[k, r : r + n, :] = jnp.where(k > 0, inside, 0.0)
        return carry

    lax.fori_loop(0, 6, faces, 0)

    def total(k, carry):
        for r, n in spans(low, high, columns):
            lane = lane_of((n, columns))
            here = coef[k, r : r + n, :]
            before = jnp.where(lane < gap, 0.0, pltpu.roll(here, gap, 1))
            after = jnp.where(lane >= columns - gap, 0.0, pltpu.roll(here, columns - gap, 1))
            s = coef[12 + k, r : r + n, :]
            d = s + wr[k, r : r + n, :] + wr[k, r + 1 : r + 1 + n, :]
            d = d + half * (here + before) + half * (here + after)
            d = d + wv[k, r : r + n, :] + wv[k + 1, r : r + n, :]
            coef[12 + k, r : r + n, :] = d
            coef[6 + k, r : r + n, :] = jnp.where(
                s > 0.0, F32(1.0) / jnp.where(s > 0.0, d, 1.0), 0.0
            )
        return carry

    lax.fori_loop(0, 6, total, 0)


def beside(u, wr, wc, wv, gap, k, r, n, here):
    columns = u.shape[2]
    left = wc[k, r : r + n, :]
    summed = wr[k, r : r + n, :] * u[k + 1, r - 1 : r - 1 + n, :]
    summed += wr[k, r + 1 : r + 1 + n, :] * u[k + 1, r + 1 : r + 1 + n, :]
    summed += left * pltpu.roll(here, gap, 1)
    summed += pltpu.roll(left * here, columns - gap, 1)
    summed += wv[k, r : r + n, :] * u[k, r : r + n, :]
    summed += wv[k + 1, r : r + n, :] * u[k + 2, r : r + n, :]
    return summed


def coloured(n, columns, gap, k, colour):
    shape = (n, columns)
    return ((row_of(shape) + lane_of(shape) // gap + k + colour) & 1) == 0


def smooth(level, low, high, fresh):
    u, rhs, coef, wr, wc, wv, gap = level
    columns = u.shape[2]
    if fresh:

        def begin(k, carry):
            for r, n in spans(low, high, columns):
                new = rhs[k, r : r + n, :] * coef[6 + k, r : r + n, :]
                u[k + 1, r : r + n, :] = jnp.where(coloured(n, columns, gap, k, 0), new, 0.0)
            return carry

        lax.fori_loop(0, 6, begin, 0)

    def half_sweep(step, carry):
        def layer(k, inner):
            for r, n in spans(low, high, columns):
                here = u[k + 1, r : r + n, :]
                new = rhs[k, r : r + n, :] + beside(u, wr, wc, wv, gap, k, r, n, here)
                new = new * coef[6 + k, r : r + n, :]
                u[k + 1, r : r + n, :] = jnp.where(coloured(n, columns, gap, k, step), new, here)
            return inner

        return lax.fori_loop(0, 6, layer, carry)

    lax.fori_loop(1 if fresh else 0, 4, half_sweep, 0)


def residual(level, temp, low, high):
    u, rhs, coef, wr, wc, wv, gap = level
    columns = u.shape[2]

    def layer(k, carry):
        for r, n in spans(low, high, columns):
            here = u[k + 1, r : r + n, :]
            left = rhs[k, r : r + n, :] + beside(u, wr, wc, wv, gap, k, r, n, here)
            left = left - coef[12 + k, r : r + n, :] * here
            temp[k, r : r + n, :] = jnp.where(coloured(n, columns, gap, k, 0), left, 0.0)
        return carry

    lax.fori_loop(0, 6, layer, 0)


def left_dot(matrix, values):
    a = values.astype(jnp.bfloat16)
    values = values - a.astype(F32)
    b = values.astype(jnp.bfloat16)
    c = (values - b.astype(F32)).astype(jnp.bfloat16)
    dot = functools.partial(jnp.dot, preferred_element_type=F32)
    return (dot(matrix, c) + dot(matrix, b)) + dot(matrix, a)


def pair_rows(ref, i, start, count):
    if ref.shape[2] > LANES:
        shape = (count, 2 * count)
        return left_dot(chosen(lane_of(shape) // 2 == row_of(shape)), ref[i, start : start + 2 * count, :])
    return ref[i, pl.ds(start, count, 2), :] + ref[i, pl.ds(start + 1, count, 2), :]


def halve(ref, i, start, count, gap):
    x = pair_rows(ref, i, start, count)
    x = (x + pltpu.roll(x, x.shape[1] - gap, 1)) * F32(0.25)
    return jnp.where(lane_of(x.shape) % (2 * gap) == 0, x, 0.0)


def restrict(fine, coarse, planes, low_fine, low_coarse, count, gap):
    def body(i, carry):
        coarse[i, low_coarse : low_coarse + count, :] = halve(fine, i, low_fine, count, gap)
        return carry

    lax.fori_loop(0, planes, body, 0)


def prolong(coarse, fine, low, count, to, gap):
    def body(k, carry):
        x = coarse[k + 1, low : low + count, :]
        if gap:
            x = x + pltpu.roll(x, gap, 1)
        if x.shape[1] > LANES:
            shape = (2 * count, count)
            twice = left_dot(chosen(row_of(shape) // 2 == lane_of(shape)), x)
            fine[k + 1, to : to + 2 * count, :] += twice
            return carry
        fine[k + 1, pl.ds(to, count, 2), :] += x
        fine[k + 1, pl.ds(to + 1, count, 2), :] += x
        return carry

    lax.fori_loop(0, 6, body, 0)


def turned(x, even):
    return jnp.where(even, pltpu.roll(x, 1, 1), pltpu.roll(x, LANES - 1, 1))


def even_of(n, k, colour):
    return ((row_of((n, LANES)) + k + colour) & 1) == 0


def look(lab, coef, tables, low, high):
    def body(i, carry):
        for r, n in spans(low, high, LANES):
            labels = lab[i, r : r + n, :]
            found = [jnp.zeros((n, LANES), F32)] * 3
            for m in range(tables[0].shape[0]):
                hit = labels == F32(m + 1)
                found = [jnp.where(hit, t[m], x) for t, x in zip(tables, found)]
            for t in range(3):
                coef[12 * t + i, r : r + n, :] = found[t]
        return carry

    lax.fori_loop(0, 12, body, 0)


def build_pair(coef, lab, u, rhs, face, side, low, high):
    half = F32(0.5)

    def faces(k, carry):
        for r, n in spans(low, high, LANES):
            here = coef[k, r : r + n, :]
            other = coef[6 + k, r : r + n, :]
            face[k, r : r + n, :] = half * (here + coef[6 + k, r - 1 : r - 1 + n, :])
            face[6 + k, r : r + n, :] = half * (here + coef[6 + k, r + 1 : r + 1 + n, :])
            face[12 + k, r : r + n, :] = half * (here + other)
            face[18 + k, r : r + n, :] = half * (here + turned(other, even_of(n, k, 0)))
            v = coef[12 + k, r : r + n, :]
            below = half * (v + coef[17 + k, r : r + n, :])
            above = half * (v + coef[19 + k, r : r + n, :])
            side[k + 1, r : r + n, :] = jnp.where(k > 0, below, 0.0)
            side[9 + k, r : r + n, :] = jnp.where(k < 5, above, 0.0)
        return carry

    lax.fori_loop(0, 6, faces, 0)

    def totals(k, carry):
        for r, n in spans(low, high, LANES):
            for colour in (0, 1):
                s = coef[24 + 6 * colour + k, r : r + n, :]
                if colour == 0:
                    d = s + face[k, r : r + n, :] + face[6 + k, r : r + n, :]
                    d = d + face[12 + k, r : r + n, :] + face[18 + k, r : r + n, :]
                    d = d + side[k + 1, r : r + n, :] + side[9 + k, r : r + n, :]
                else:
                    d = s + face[6 + k, r - 1 : r - 1 + n, :] + face[k, r + 1 : r + 1 + n, :]
                    d = d + face[12 + k, r : r + n, :]
                    d = d + turned(face[18 + k, r : r + n, :], even_of(n, k, 1))
                    d = d + side[8 + k, r : r + n, :] + side[k + 2, r : r + n, :]
                heat = jnp.where(k == 0, lab[12, r : r + n, :], 0.0)
                rhs[6 * colour + k, r : r + n, :] = s * u[8 * colour + k + 1, r : r + n, :] + heat
                coef[24 + 6 * colour + k, r : r + n, :] = d
                coef[12 + 6 * colour + k, r : r + n, :] = jnp.where(
                    s > 0.0, F32(1.0) / jnp.where(s > 0.0, d, 1.0), 0.0
                )
        return carry

    lax.fori_loop(0, 6, totals, 0)


def beside_pair(u, face, side, colour, k, r, n):
    o = 8 * (1 - colour)
    same = u[o + k + 1, r : r + n, :]
    before = u[o + k + 1, r - 1 : r - 1 + n, :]
    after = u[o + k + 1, r + 1 : r + 1 + n, :]
    even = even_of(n, k, colour)
    summed = face[12 + k, r : r + n, :] * same
    if colour == 0:
        summed += face[k, r : r + n, :] * before + face[6 + k, r : r + n, :] * after
        summed += face[18 + k, r : r + n, :] * turned(same, even)
        summed += side[k + 1, r : r + n, :] * u[o + k, r : r + n, :]
        summed += side[9 + k, r : r + n, :] * u[o + k + 2, r : r + n, :]
    else:
        summed += face[6 + k, r - 1 : r - 1 + n, :] * before
        summed += face[k, r + 1 : r + 1 + n, :] * after
        summed += turned(face[18 + k, r : r + n, :] * same, even)
        summed += side[8 + k, r : r + n, :] * u[o + k, r : r + n, :]
        summed += side[k + 2, r : r + n, :] * u[o + k + 2, r : r + n, :]
    return summed


def smooth_pair(u, rhs, coef, face, side, low, high):
    def sweep(_, carry):
        for colour in (0, 1):

            def layer(k, inner):
                for r, n in spans(low, high, LANES):
                    new = rhs[6 * colour + k, r : r + n, :]
                    new = new + beside_pair(u, face, side, colour, k, r, n)
                    new = new * coef[12 + 6 * colour + k, r : r + n, :]
                    u[8 * colour + k + 1, r : r + n, :] = new
                return inner

            carry = lax.fori_loop(0, 6, layer, carry)
        return carry

    lax.fori_loop(0, 2, sweep, 0)


def residual_pair(u, rhs, coef, face, side, temp, low, high):
    def layer(k, carry):
        for r, n in spans(low, high, LANES):
            left = rhs[k, r : r + n, :] + beside_pair(u, face, side, 0, k, r, n)
            temp[k, r : r + n, :] = left - coef[24 + k, r : r + n, :] * u[k + 1, r : r + n, :]
        return carry

    lax.fori_loop(0, 6, layer, 0)


def greet(waiting):
    barrier = pltpu.get_barrier_semaphore()
    gx, gy = lax.axis_index("gx"), lax.axis_index("gy")
    nx, ny = lax.axis_size("gx"), lax.axis_size("gy")
    if waiting:
        across = jnp.where(gx > 0, 1, 0) + jnp.where(gx < nx - 1, 1, 0)
        along = jnp.where(gy > 0, 1, 0) + jnp.where(gy < ny - 1, 1, 0)
        pl.semaphore_wait(barrier, nx + ny - 2 + across * along)
        return
    for step in range(1, nx):
        other = (lax.rem(gx + step, nx), gy)
        pl.semaphore_signal(barrier, inc=1, device_id=other, device_id_type=MESH)
    for step in range(1, ny):
        other = (gx, lax.rem(gy + step, ny))
        pl.semaphore_signal(barrier, inc=1, device_id=other, device_id_type=MESH)
    for dx, dy in SIDES[4:]:

        @pl.when(near(dx, dy))
        def _(dx=dx, dy=dy):
            other = (gx + dx, gy + dy)
            pl.semaphore_signal(barrier, inc=1, device_id=other, device_id_type=MESH)


def gather_copies(whole, sems, axis):
    size = lax.axis_size(axis)
    gx, gy = lax.axis_index("gx"), lax.axis_index("gy")
    made = []
    for step in range(1, size):
        if axis == "gx":
            target = (lax.rem(gx + step, size), gy)
            source = whole.at[gy, gx]
            origin = whole.at[gy, lax.rem(gx + size - step, size)]
        else:
            target = (gx, lax.rem(gy + step, size))
            source = whole.at[gy]
            origin = whole.at[lax.rem(gy + size - step, size)]
        out = pltpu.make_async_remote_copy(
            src_ref=source, dst_ref=source, send_sem=sems[0].at[step],
            recv_sem=sems[1].at[step], device_id=target, device_id_type=MESH,
        )
        into = pltpu.make_async_remote_copy(
            src_ref=origin, dst_ref=origin, send_sem=sems[0].at[step],
            recv_sem=sems[1].at[step], device_id=target, device_id_type=MESH,
        )
        made.append((out, into))
    return made


def begin(made):
    for out, _ in made:
        out.start()


def end(made):
    for out, into in made:
        out.wait_send()
        into.wait_recv()


def squeeze(planes):
    rows = 6 * LANES
    r = lax.broadcasted_iota(jnp.int32, (rows, LANES), 0)
    c = lax.broadcasted_iota(jnp.int32, (rows, LANES), 1)
    at = (c // 16) * LANES + LEFT + 4 * (c % 16)
    return split_dot(jnp.concatenate(planes, axis=1), chosen(r == at))


def place(whole, targets, h):
    ny, nx = whole.shape[:2]
    wide = min(ny, LANES // 16)

    def body(gx, carry):
        row = pl.multiple_of(8 + gx * h, 8)
        for t, (ref, first) in enumerate(targets):
            for k in range(6):
                for start in range(0, ny, wide):
                    total = jnp.zeros((h, LANES), F32)
                    lane = lane_of((h, LANES)) // 16
                    for gy in range(start, min(start + wide, ny)):
                        x = whole[gy, gx, t * h : (t + 1) * h, :]
                        x = pltpu.roll(x, (16 * (gy - start - k)) % LANES, 1)
                        total = jnp.where(lane == gy - start, x, total)
                    ref[first + k, pl.ds(row, h), start * 16 : start * 16 + LANES] = total
        return carry

    lax.fori_loop(0, nx, body, 0)


def conjugate(level, temp, out):
    u, rhs, coef, wr, wc, wv, gap = level
    n, columns = u.shape[1] - 16, u.shape[2]
    mid = slice(8, 8 + n)

    def summed(x):
        x = jnp.sum(x, axis=0)
        return jnp.sum(jnp.sum(x, axis=0, keepdims=True), axis=1, keepdims=True)

    inv = slice(6, 12)
    r0 = rhs[:, mid, :]
    z0 = r0 * coef[inv, mid, :]
    u[1:7, mid, :] = z0
    temp[:, mid, :] = r0
    out[:, mid, :] = jnp.zeros_like(r0)

    def step(_, rz):
        p = u[1:7, mid, :]
        image = jnp.stack(
            [
                coef[12 + k, mid, :] * p[k] - beside(u, wr, wc, wv, gap, k, 8, n, p[k])
                for k in range(6)
            ]
        )
        alpha = rz / summed(p * image)
        out[:, mid, :] += alpha[None] * p
        r = temp[:, mid, :] - alpha[None] * image
        temp[:, mid, :] = r
        z = r * coef[inv, mid, :]
        rz_new = summed(r * z)
        u[1:7, mid, :] = z + (rz_new / rz)[None] * p
        return rz_new

    lax.fori_loop(0, COARSE_ITERS, step, summed(r0 * z0))
    u[1:7, mid, :] = out[:, mid, :]


def exchanges(n0):
    n1, n2 = n0 // 2, n0 // 4
    return {
        "near": Exchange(4, n0, 25, (12, 13)),
        "coef1": Exchange(8, n1, 18, (18,)),
        "coef2": Exchange(16, n2, 18, (18,)),
        "u0": Exchange(4, n0, 12, (12,)),
        "rhs1": Exchange(8, n1, 6, (6,)),
        "u1": Exchange(8, n1, 6, (6,)),
        "rhs2": Exchange(16, n2, 6, (6,)),
        "u2": Exchange(16, n2, 6, (6,)),
    }


def scratches(n0, nx, ny):
    def planes(n, rows, columns=LANES):
        return pltpu.VMEM((n, rows, columns), F32)

    rows = n0 + 2 * BASE
    shapes = [planes(n, rows) for n in (16, 13, 36, 12, 24, 16, 12)]
    for i in (1, 2):
        r = (n0 >> i) + 2 * BASE
        shapes += [planes(n, r) for n in (8, 6, 18, 6, 6, 7)]
    h = n0 >> LOCAL
    shapes += [pltpu.VMEM((ny, nx, 3 * h, LANES), F32), pltpu.VMEM((ny, nx, h, LANES), F32)]
    shapes += [pltpu.SemaphoreType.DMA((nx,)), pltpu.SemaphoreType.DMA((nx,))] * 2
    shapes += [pltpu.SemaphoreType.DMA((ny,)), pltpu.SemaphoreType.DMA((ny,))] * 2
    columns = up_to(ny * h, LANES)
    for i in range(LEVELS - LOCAL + 1):
        r = ((nx * h) >> i) + 16
        shapes += [planes(n, r, columns) for n in (8, 6, 18, 6, 6, 7)]
    shapes += [planes(6, (nx * h) + 16, columns)]
    return shapes


def whole_kernel(field, labels, patch, lat_t, ver_t, sto_t, wattage, out, *refs):
    n0 = field.shape[1]
    n1, n2, h = n0 // 2, n0 // 4, n0 // 8
    nx, ny = lax.axis_size("gx"), lax.axis_size("gy")
    u0, lab, coef0, rhs0, face, side, lab_own = refs[:7]
    levels = {}
    at = 7
    for i in (1, 2):
        u, rhs, coef, wr, wc, wv = refs[at : at + 6]
        levels[i] = (u, rhs, coef, wr, wc, wv, i)
        at += 6
    gathered_coef, gathered_rhs = refs[at : at + 2]
    sems = refs[at + 2 : at + 10]
    at += 10
    for i in range(LOCAL, LEVELS + 1):
        u, rhs, coef, wr, wc, wv = refs[at : at + 6]
        levels[i] = (u, rhs, coef, wr, wc, wv, 1 << (i - LOCAL))
        at += 6
    temp3 = refs[at]
    rest = refs[at + 1 :]
    ex = exchanges(n0)
    for e in ex.values():
        rest = e.bind(rest)
        e.clear()
    greet(False)
    for ref in (u0, lab, coef0, rhs0, face, side):
        ref[...] = jnp.zeros_like(ref)
    for level in levels.values():
        for ref in level[:6]:
            ref[...] = jnp.zeros_like(ref)

    r = lax.broadcasted_iota(jnp.int32, (n0, 2 * LANES), 0)
    c = lax.broadcasted_iota(jnp.int32, (n0, 2 * LANES), 1)
    spread = chosen(r == 2 * (c % LANES - LEFT) + c // LANES)
    own = slice(BASE, BASE + n0)

    def part(k, carry):
        even = even_of(n0, k, 0)
        both = split_dot(field[k], spread)
        a, b = both[:, :LANES], both[:, LANES:]
        u0[k + 1, own, :] = jnp.where(even, a, b)
        u0[k + 9, own, :] = jnp.where(even, b, a)
        both = split_dot(labels[k].astype(F32) + F32(1.0), spread, 1)
        inside = (lane_of((n0, LANES)) >= LEFT) & (lane_of((n0, LANES)) < LEFT + 64)
        a, b = both[:, :LANES], both[:, LANES:]
        lab[k, own, :] = jnp.where(inside, jnp.where(even, a, b), 0.0)
        lab[k + 6, own, :] = jnp.where(inside, jnp.where(even, b, a), 0.0)
        return carry

    lax.fori_loop(0, 6, part, 0)
    tiles = patch[...]
    small = jnp.zeros(tiles.shape, F32)
    for m in range(wattage.shape[0]):
        small = jnp.where(tiles == m, wattage[m], small)
    th, tw = tiles.shape
    r = lax.broadcasted_iota(jnp.int32, (tw, LANES), 0)
    c = lax.broadcasted_iota(jnp.int32, (tw, LANES), 1)
    flat = chosen((c >= LEFT) & ((c - LEFT) // (TILE // 2) == r))
    heat = split_dot(small, flat)
    for i in range(th):
        lab[12, BASE + i * TILE : BASE + (i + 1) * TILE, :] = jnp.broadcast_to(
            heat[i : i + 1, :], (TILE, LANES)
        )

    fields = [(u0, (1 + k + 8 * c,)) for c in (0, 1) for k in range(6)]
    labs = [(lab, (i,)) for i in range(13)]
    edge = ex["near"]
    stage = lab_own
    for c in (0, 1):
        stage[6 * c : 6 * c + 6, own, :] = u0[1 + 8 * c : 7 + 8 * c, own, :]
    greet(True)
    edge.start(fields + labs, (stage, lab))

    tables = (lat_t, ver_t, sto_t)
    look(lab, coef0, tables, BASE, BASE + n0)
    coef1, coef2 = levels[1][2], levels[2][2]

    def first(i, carry):
        t, k = i // 6, i % 6
        x = pair_rows(coef0, 12 * t + k, BASE, n1) + pair_rows(coef0, 12 * t + 6 + k, BASE, n1)
        coef1[i, BASE : BASE + n1, :] = x * F32(0.25)
        return carry

    lax.fori_loop(0, 18, first, 0)
    restrict(coef1, coef2, 18, BASE, BASE, n2, 1)
    ex["coef1"].start([(coef1, (i,)) for i in range(18)], (coef1,))
    ex["coef2"].start([(coef2, (i,)) for i in range(18)], (coef2,))
    gx, gy = lax.axis_index("gx"), lax.axis_index("gy")
    for t in range(3):
        planes = [halve(coef2, 6 * t + k, BASE, h, 2) for k in range(6)]
        gathered_coef[gy, gx, t * h : (t + 1) * h, :] = squeeze(planes)
    coef_x = gather_copies(gathered_coef, sems[0:2], "gx")
    begin(coef_x)

    edge.finish()
    tops = [(edge.tops[0], i) for i in range(12)] + [(edge.tops[1], i) for i in range(13)]
    edge.unpack(fields + labs, tops, fields + labs)
    lo, hi0, hi1, hi2 = BASE - HALO, BASE + n0 + HALO, BASE + n1 + HALO, BASE + n2 + HALO
    look(lab, coef0, tables, lo, hi0)
    build_pair(coef0, lab, u0, rhs0, face, side, lo, hi0)
    smooth_pair(u0, rhs0, coef0, face, side, lo, hi0)
    temp = coef0
    residual_pair(u0, rhs0, coef0, face, side, temp, BASE, BASE + n0)
    rhs1, rhs2 = levels[1][1], levels[2][1]

    def down(k, carry):
        rhs1[k, BASE : BASE + n1, :] = pair_rows(temp, k, BASE, n1) * F32(0.25)
        return carry

    lax.fori_loop(0, 6, down, 0)
    ex["rhs1"].start([(rhs1, (k,)) for k in range(6)], (rhs1,))
    for c in (0, 1):
        stage[6 * c : 6 * c + 6, own, :] = u0[1 + 8 * c : 7 + 8 * c, own, :]
    ex["u0"].start(fields, (stage,))

    def fill(name, ref, count, first=0):
        e = ex[name]
        e.finish()
        planes = [(ref, (first + i,)) for i in range(count)]
        e.unpack(planes, [(e.tops[0], i) for i in range(count)], planes)

    def weigh(i, low, high):
        u, rhs, coef, wr, wc, wv, gap = levels[i]
        build(coef, wr, wc, wv, 0.25**i, gap, low, high)

    fill("coef1", coef1, 18)
    weigh(1, lo, hi1)
    fill("coef2", coef2, 18)
    weigh(2, lo, hi2)
    end(coef_x)
    coef_y = gather_copies(gathered_coef, sems[4:6], "gy")
    begin(coef_y)

    fill("rhs1", rhs1, 6)
    smooth(levels[1], lo, hi1, True)
    u1 = levels[1][0]
    residual(levels[1], temp, BASE, BASE + n1)
    restrict(temp, rhs2, 6, BASE, BASE, n2, 1)
    ex["rhs2"].start([(rhs2, (k,)) for k in range(6)], (rhs2,))
    ex["u1"].start([(u1, (k + 1,)) for k in range(6)], (u1.at[1:7],))
    end(coef_y)
    coef3 = levels[3][2]
    place(gathered_coef, [(coef3, 0), (coef3, 6), (coef3, 12)], h)

    fill("rhs2", rhs2, 6)
    smooth(levels[2], lo, hi2, True)
    u2 = levels[2][0]
    residual(levels[2], temp, BASE, BASE + n2)
    gathered_rhs[gy, gx] = squeeze([halve(temp, k, BASE, h, 2) for k in range(6)])
    rhs_x = gather_copies(gathered_rhs, sems[2:4], "gx")
    begin(rhs_x)
    ex["u2"].start([(u2, (k + 1,)) for k in range(6)], (u2.at[1:7],))

    sizes = {i: (nx * h) >> (i - LOCAL) for i in range(LOCAL, LEVELS + 1)}
    for i in range(LOCAL, LEVELS):
        restrict(levels[i][2], levels[i + 1][2], 18, 8, 8, sizes[i + 1], levels[i][6])
    end(rhs_x)
    rhs_y = gather_copies(gathered_rhs, sems[6:8], "gy")
    begin(rhs_y)
    for i in range(LOCAL, LEVELS + 1):
        weigh(i, 8, 8 + sizes[i])
    end(rhs_y)
    place(gathered_rhs, [(levels[3][1], 0)], h)

    for i in range(LOCAL, LEVELS):
        smooth(levels[i], 8, 8 + sizes[i], True)
        residual(levels[i], temp3, 8, 8 + sizes[i])
        restrict(temp3, levels[i + 1][1], 6, 8, 8, sizes[i + 1], levels[i][6])
    conjugate(levels[LEVELS], temp3, levels[LEVELS][1])
    for i in reversed(range(LOCAL, LEVELS)):
        prolong(levels[i + 1][0], levels[i][0], 8, sizes[i + 1], 8, levels[i][6])
        smooth(levels[i], 8, 8 + sizes[i], False)

    u3 = levels[3][0]
    columns = u3.shape[2]
    r = lax.broadcasted_iota(jnp.int32, (columns, LANES), 0)
    c = lax.broadcasted_iota(jnp.int32, (columns, LANES), 1)
    hit = ((c & 1) == 0) & (c // 4 - LEFT // 4 + gy * 16 == r)
    widen = chosen(hit)
    fill("u2", u2, 6, 1)

    def window(k, carry):
        x = u3[k + 1, pl.ds(pl.multiple_of(gx * h, 8), h + 16), :]
        x = split_dot(x, widen)
        u2[k + 1, pl.ds(0, h + 16, 2), :] += x
        u2[k + 1, pl.ds(1, h + 16, 2), :] += x
        return carry

    lax.fori_loop(0, 6, window, 0)
    smooth(levels[2], lo, hi2, False)
    fill("u1", u1, 6, 1)
    prolong(u2, u1, lo, n2 + 16, 0, 1)
    smooth(levels[1], lo, hi1, False)
    e = ex["u0"]
    e.finish()
    e.unpack(fields, [(e.tops[0], i) for i in range(12)], fields)

    def up(k, carry):
        x = u1[k + 1, lo : lo + n1 + 16, :]
        for c in (0, 8):
            u0[c + k + 1, pl.ds(0, n1 + 16, 2), :] += x
            u0[c + k + 1, pl.ds(1, n1 + 16, 2), :] += x
        return carry

    lax.fori_loop(0, 6, up, 0)
    smooth_pair(u0, rhs0, coef0, face, side, lo, hi0)

    r = lax.broadcasted_iota(jnp.int32, (2 * LANES, n0), 0)
    c = lax.broadcasted_iota(jnp.int32, (2 * LANES, n0), 1)
    join = chosen(c == 2 * (r % LANES - LEFT) + r // LANES)

    def give(k, carry):
        even = even_of(n0, k, 0)
        red, black = u0[k + 1, own, :], u0[k + 9, own, :]
        both = jnp.concatenate(
            [jnp.where(even, red, black), jnp.where(even, black, red)], axis=1
        )
        out[k] = split_dot(both, join)
        return carry

    lax.fori_loop(0, 6, give, 0)


def on_device(field, substance, patch, planar, vertical, storage, wattage):
    n0 = field.shape[1]
    nx, ny = lax.axis_size("gx"), lax.axis_size("gy")
    vmem = pl.BlockSpec(memory_space=pltpu.VMEM)
    smem = pl.BlockSpec(memory_space=pltpu.SMEM)
    scratch = scratches(n0, nx, ny)
    for e in exchanges(n0).values():
        scratch += e.scratch()
    return pl.pallas_call(
        whole_kernel,
        out_shape=jax.ShapeDtypeStruct(field.shape, F32),
        in_specs=[vmem] * 3 + [smem] * 4,
        out_specs=vmem,
        scratch_shapes=scratch,
        compiler_params=pltpu.CompilerParams(vmem_limit_bytes=VM, has_side_effects=True, collective_id=0),
    )(field, substance, patch, planar, vertical, storage, wattage)


def solution(mesh):
    placed = (P(None, "gx", "gy"), P(None, "gx", "gy"), P("gx", "gy"), P(), P(), P(), P())
    return jax.shard_map(
        on_device, mesh=mesh, in_specs=placed, out_specs=P(None, "gx", "gy"), check_vma=False
    )
```

```python
import functools

import jax
import jax.numpy as jnp
from jax import lax
from jax.experimental import pallas as pl
from jax.experimental.pallas import tpu as pltpu
from jax.sharding import PartitionSpec as P

TILE = 16
LEVELS = 6
COARSE_ITERS = 12
LOCAL = 3
HALO = 8
BASE = 16
LEFT = 16
LANES = 128
F32 = jnp.float32
VM = 63 * 1024 * 1024
MESH = pl.DeviceIdType.MESH
SIDES = ((-1, 0), (1, 0), (0, -1), (0, 1), (-1, -1), (-1, 1), (1, -1), (1, 1))


def up_to(count, step):
    return -(-count // step) * step


def spans(low, high, columns):
    step = max(8, 48 * LANES // columns // 8 * 8)
    return [(r, min(step, high - r)) for r in range(low, high, step)]


def lane_of(shape):
    return lax.broadcasted_iota(jnp.int32, shape, len(shape) - 1)


def row_of(shape):
    return lax.broadcasted_iota(jnp.int32, shape, 0)


def split_dot(values, matrix, terms=3):
    total = None
    pieces = []
    for _ in range(terms):
        piece = values.astype(jnp.bfloat16)
        values = values - piece.astype(F32)
        pieces.append(piece)
    for piece in reversed(pieces):
        part = jnp.dot(piece, matrix, preferred_element_type=F32)
        total = part if total is None else total + part
    return total


def chosen(hit):
    return jnp.where(hit, F32(1.0), F32(0.0)).astype(jnp.bfloat16)


def near(dx, dy):
    ok = None
    for axis, step in (("gx", dx), ("gy", dy)):
        if step == 0:
            continue
        at = lax.axis_index(axis)
        this = (at + step < lax.axis_size(axis)) if step > 0 else (at + step >= 0)
        ok = this if ok is None else jnp.logical_and(ok, this)
    return ok


class Exchange:
    def __init__(self, width, rows, count, row_refs):
        self.width, self.rows, self.count = width, rows, count
        self.per = LANES // width
        self.packs = -(-count // self.per)
        self.row_refs = row_refs

    def scratch(self):
        packed = pltpu.VMEM((2, self.packs, self.rows, LANES), F32)
        landed = pltpu.VMEM((2, self.packs, self.rows + 2 * HALO, LANES), F32)
        tops = [pltpu.VMEM((2, n, HALO, LANES), F32) for n in self.row_refs]
        sems = pltpu.SemaphoreType.DMA((6 + 2 * len(self.row_refs),))
        return [packed, landed, sems, sems] + tops

    def bind(self, refs):
        self.packed, self.landed, self.send, self.recv = refs[:4]
        self.tops = refs[4 : 4 + len(self.row_refs)]
        return refs[4 + len(self.row_refs) :]

    def clear(self):
        self.landed[...] = jnp.zeros_like(self.landed)
        for top in self.tops:
            top[...] = jnp.zeros_like(top)

    def copies(self, sources):
        n = self.rows
        gx, gy = lax.axis_index("gx"), lax.axis_index("gy")
        out = []
        at = 0

        def add(dx, dy, source, target):
            nonlocal at
            out.append((dx, dy, source, target, at))
            at += 1

        for dy, side in ((1, 0), (-1, 1)):
            packed = self.packed.at[side]
            landed = self.landed.at[side]
            add(0, dy, packed, landed.at[:, HALO : HALO + n, :])
            add(1, dy, packed.at[:, n - HALO : n, :], landed.at[:, 0:HALO, :])
            add(-1, dy, packed.at[:, 0:HALO, :], landed.at[:, HALO + n : n + 2 * HALO, :])
        for source, top in zip(sources, self.tops):
            add(1, 0, source.at[:, BASE + n - HALO : BASE + n, :], top.at[0])
            add(-1, 0, source.at[:, BASE : BASE + HALO, :], top.at[1])
        made = []
        for dx, dy, source, target, i in out:
            copy = pltpu.make_async_remote_copy(
                src_ref=source,
                dst_ref=target,
                send_sem=self.send.at[i],
                recv_sem=self.recv.at[i],
                device_id=(gx + dx, gy + dy),
                device_id_type=MESH,
            )
            made.append((dx, dy, copy))
        return made

    def start(self, planes, sources):
        w = self.width
        n = self.rows
        for pack in range(self.packs):
            group = planes[pack * self.per : (pack + 1) * self.per]
            for r, m in spans(0, n, LANES):
                lane = lane_of((m, LANES)) // w
                right = jnp.zeros((m, LANES), F32)
                left = right
                for p, (ref, where) in enumerate(group):
                    x = ref[where + (slice(BASE + r, BASE + r + m),)]
                    hit = lane == p
                    a = pltpu.roll(x, (p * w - (LEFT + 64 - w)) % LANES, 1)
                    b = pltpu.roll(x, (p * w - LEFT) % LANES, 1)
                    right = jnp.where(hit, a, right)
                    left = jnp.where(hit, b, left)
                self.packed[0, pack, r : r + m, :] = right
                self.packed[1, pack, r : r + m, :] = left
        self.sources = sources
        for dx, dy, copy in self.copies(sources):
            pl.when(near(dx, dy))(copy.start)

    def finish(self):
        for dx, dy, copy in self.copies(self.sources):
            pl.when(near(dx, dy))(copy.wait_send)
            pl.when(near(-dx, -dy))(copy.wait_recv)

    def unpack(self, planes, tops, targets):
        w = self.width
        n = self.rows
        for i, (ref, where) in enumerate(planes):
            pack, p = i // self.per, i % self.per
            target, place = targets[i]
            pieces = [(0, HALO, 0)]
            pieces += [(HALO + r, m, None) for r, m in spans(0, n, LANES)]
            pieces += [(HALO + n, HALO, 1)]
            for r, m, side in pieces:
                if side is None:
                    x = ref[where + (slice(BASE - HALO + r, BASE - HALO + r + m),)]
                else:
                    top, plane = tops[i]
                    x = top[side, plane]
                lane = lane_of((m, LANES))
                a = pltpu.roll(self.landed[0, pack, r : r + m, :], (LEFT - w - p * w) % LANES, 1)
                b = pltpu.roll(self.landed[1, pack, r : r + m, :], (LEFT + 64 - p * w) % LANES, 1)
                x = jnp.where((lane >= LEFT - w) & (lane < LEFT), a, x)
                x = jnp.where((lane >= LEFT + 64) & (lane < LEFT + 64 + w), b, x)
                target[place + (slice(BASE - HALO + r, BASE - HALO + r + m),)] = x


def build(coef, wr, wc, wv, scale, gap, low, high):
    columns = coef.shape[2]
    half = F32(0.5 * scale)
    wv[6] = jnp.zeros(wv.shape[1:], F32)
    for k in range(6):
        for r, n in spans(low, high, columns):
            lane = lane_of((n, columns))
            here = coef[k, r : r + n, :]
            wr[k, r : r + n, :] = half * (here + coef[k, r - 1 : r - 1 + n, :])
            before = jnp.where(lane < gap, 0.0, pltpu.roll(here, gap, 1))
            wc[k, r : r + n, :] = jnp.where(lane < gap, 0.0, half * (here + before))
        here = coef[k, high : high + 8, :]
        wr[k, high : high + 8, :] = half * (here + coef[k, high - 1 : high + 7, :])
        for r, n in spans(low, high, columns):
            if k:
                inside = coef[6 + k, r : r + n, :] + coef[5 + k, r : r + n, :]
                wv[k, r : r + n, :] = F32(0.5) * inside
            else:
                wv[k, r : r + n, :] = jnp.zeros((n, columns), F32)
    for k in range(6):
        for r, n in spans(low, high, columns):
            lane = lane_of((n, columns))
            here = coef[k, r : r + n, :]
            before = jnp.where(lane < gap, 0.0, pltpu.roll(here, gap, 1))
            after = jnp.where(lane >= columns - gap, 0.0, pltpu.roll(here, columns - gap, 1))
            s = coef[12 + k, r : r + n, :]
            d = s + wr[k, r : r + n, :] + wr[k, r + 1 : r + 1 + n, :]
            d = d + half * (here + before) + half * (here + after)
            d = d + wv[k, r : r + n, :] + wv[k + 1, r : r + n, :]
            coef[12 + k, r : r + n, :] = d
            coef[6 + k, r : r + n, :] = jnp.where(
                s > 0.0, F32(1.0) / jnp.where(s > 0.0, d, 1.0), 0.0
            )


def beside(u, wr, wc, wv, gap, k, r, n, here):
    columns = u.shape[2]
    left = wc[k, r : r + n, :]
    summed = left * pltpu.roll(here, gap, 1)
    summed += pltpu.roll(left * here, columns - gap, 1)
    summed += wr[k, r : r + n, :] * u[k + 1, r - 1 : r - 1 + n, :]
    summed += wr[k, r + 1 : r + 1 + n, :] * u[k + 1, r + 1 : r + 1 + n, :]
    if k > 0:
        summed += wv[k, r : r + n, :] * u[k, r : r + n, :]
    if k < 5:
        summed += wv[k + 1, r : r + n, :] * u[k + 2, r : r + n, :]
    return summed


def coloured(n, columns, gap, k, colour):
    shape = (n, columns)
    return ((row_of(shape) + lane_of(shape) // gap + k + colour) & 1) == 0


def half_sweep(level, source, target, colour, low, high):
    rhs, coef, wr, wc, wv, gap = level[2:]
    columns = source.shape[2]
    for k in range(6):
        for r, n in spans(low, high, columns):
            here = source[k + 1, r : r + n, :]
            new = rhs[k, r : r + n, :] + beside(source, wr, wc, wv, gap, k, r, n, here)
            new = new * coef[6 + k, r : r + n, :]
            mask = coloured(n, columns, gap, k, colour)
            target[k + 1, r : r + n, :] = jnp.where(mask, new, here)


def smooth(level, low, high, fresh):
    u, v, rhs, coef, wr, wc, wv, gap = level
    columns = u.shape[2]
    if fresh:
        for k in range(6):
            for r, n in spans(low, high, columns):
                new = rhs[k, r : r + n, :] * coef[6 + k, r : r + n, :]
                v[k + 1, r : r + n, :] = jnp.where(coloured(n, columns, gap, k, 0), new, 0.0)
        half_sweep(level, v, u, 1, low, high)
        half_sweep(level, u, v, 0, low, high)
        half_sweep(level, v, u, 1, low, high)
        return

    def sweep(_, carry):
        half_sweep(level, u, v, 0, low, high)
        half_sweep(level, v, u, 1, low, high)
        return carry

    lax.fori_loop(0, 2, sweep, 0)


def residual(level, temp, low, high):
    u, _, rhs, coef, wr, wc, wv, gap = level
    columns = u.shape[2]
    for k in range(6):
        for r, n in spans(low, high, columns):
            here = u[k + 1, r : r + n, :]
            left = rhs[k, r : r + n, :] + beside(u, wr, wc, wv, gap, k, r, n, here)
            left = left - coef[12 + k, r : r + n, :] * here
            temp[k, r : r + n, :] = jnp.where(coloured(n, columns, gap, k, 0), left, 0.0)


def left_dot(matrix, values):
    a = values.astype(jnp.bfloat16)
    values = values - a.astype(F32)
    b = values.astype(jnp.bfloat16)
    c = (values - b.astype(F32)).astype(jnp.bfloat16)
    dot = functools.partial(jnp.dot, preferred_element_type=F32)
    return (dot(matrix, c) + dot(matrix, b)) + dot(matrix, a)


def pair_rows(ref, i, start, count):
    if ref.shape[2] > LANES:
        shape = (count, 2 * count)
        pick = chosen(lane_of(shape) // 2 == row_of(shape))
        return left_dot(pick, ref[i, start : start + 2 * count, :])
    return ref[i, pl.ds(start, count, 2), :] + ref[i, pl.ds(start + 1, count, 2), :]


def halve(ref, i, start, count, gap):
    x = pair_rows(ref, i, start, count)
    x = (x + pltpu.roll(x, x.shape[1] - gap, 1)) * F32(0.25)
    return jnp.where(lane_of(x.shape) % (2 * gap) == 0, x, 0.0)


def restrict(fine, coarse, planes, low_fine, low_coarse, count, gap):
    def body(i, carry):
        coarse[i, low_coarse : low_coarse + count, :] = halve(fine, i, low_fine, count, gap)
        return carry

    if fine.shape[2] > LANES:
        lax.fori_loop(0, planes, body, 0)
    else:
        for i in range(planes):
            body(i, 0)


def prolong(coarse, fine, low, count, to, gap):
    def body(k, carry):
        x = coarse[k + 1, low : low + count, :]
        x = x + pltpu.roll(x, gap, 1)
        if x.shape[1] > LANES:
            shape = (2 * count, count)
            twice = left_dot(chosen(row_of(shape) // 2 == lane_of(shape)), x)
            fine[k + 1, to : to + 2 * count, :] += twice
            return carry
        fine[k + 1, pl.ds(to, count, 2), :] += x
        fine[k + 1, pl.ds(to + 1, count, 2), :] += x
        return carry

    for k in range(6):
        body(k, 0)


def border(ref, planes, pad):
    rows = ref.shape[1]
    for start in (0, rows - pad):
        ref[0:planes, start : start + pad, :] = jnp.zeros((planes, pad, ref.shape[2]), F32)


def turned(x, even):
    return jnp.where(even, pltpu.roll(x, 1, 1), pltpu.roll(x, LANES - 1, 1))


def even_of(n, k, colour):
    return ((row_of((n, LANES)) + k + colour) & 1) == 0


def look(lab, coef, tables, low, high):
    def body(i, carry):
        for r, n in spans(low, high, LANES):
            labels = lab[i, r : r + n, :]
            found = [jnp.zeros((n, LANES), F32)] * 3
            for m in range(tables[0].shape[0]):
                hit = labels == F32(m + 1)
                found = [jnp.where(hit, t[m], x) for t, x in zip(tables, found)]
            for t in range(3):
                coef[12 * t + i, r : r + n, :] = found[t]
        return carry

    lax.fori_loop(0, 12, body, 0)


def build_pair(coef, lab, u, rhs, face, side, low, high):
    half = F32(0.5)
    for k in range(6):
        for r, n in spans(low, high, LANES):
            here = coef[k, r : r + n, :]
            other = coef[6 + k, r : r + n, :]
            face[k, r : r + n, :] = half * (here + coef[6 + k, r - 1 : r - 1 + n, :])
            face[6 + k, r : r + n, :] = half * (here + coef[6 + k, r + 1 : r + 1 + n, :])
            face[12 + k, r : r + n, :] = half * (here + other)
            face[18 + k, r : r + n, :] = half * (here + turned(other, even_of(n, k, 0)))
            v = coef[12 + k, r : r + n, :]
            if k > 0:
                side[k + 1, r : r + n, :] = half * (v + coef[17 + k, r : r + n, :])
            if k < 5:
                side[9 + k, r : r + n, :] = half * (v + coef[19 + k, r : r + n, :])
    for k in range(6):
        for r, n in spans(low, high, LANES):
            for colour in (0, 1):
                s = coef[24 + 6 * colour + k, r : r + n, :]
                if colour == 0:
                    d = s + face[k, r : r + n, :] + face[6 + k, r : r + n, :]
                    d = d + face[12 + k, r : r + n, :] + face[18 + k, r : r + n, :]
                    below, above = side[k + 1, r : r + n, :], side[9 + k, r : r + n, :]
                else:
                    d = s + face[6 + k, r - 1 : r - 1 + n, :] + face[k, r + 1 : r + 1 + n, :]
                    d = d + face[12 + k, r : r + n, :]
                    d = d + turned(face[18 + k, r : r + n, :], even_of(n, k, 1))
                    below, above = side[8 + k, r : r + n, :], side[k + 2, r : r + n, :]
                if k > 0:
                    d = d + below
                if k < 5:
                    d = d + above
                source = s * u[8 * colour + k + 1, r : r + n, :]
                if k == 0:
                    source = source + lab[12, r : r + n, :]
                rhs[6 * colour + k, r : r + n, :] = source
                coef[24 + 6 * colour + k, r : r + n, :] = d
                coef[12 + 6 * colour + k, r : r + n, :] = jnp.where(
                    s > 0.0, F32(1.0) / jnp.where(s > 0.0, d, 1.0), 0.0
                )


def beside_pair(u, face, side, colour, k, r, n):
    o = 8 * (1 - colour)
    same = u[o + k + 1, r : r + n, :]
    before = u[o + k + 1, r - 1 : r - 1 + n, :]
    after = u[o + k + 1, r + 1 : r + 1 + n, :]
    even = even_of(n, k, colour)
    if colour == 0:
        summed = face[18 + k, r : r + n, :] * turned(same, even)
        summed += face[12 + k, r : r + n, :] * same
        summed += face[k, r : r + n, :] * before + face[6 + k, r : r + n, :] * after
        below, above = k + 1, k + 9
    else:
        summed = turned(face[18 + k, r : r + n, :] * same, even)
        summed += face[12 + k, r : r + n, :] * same
        summed += face[6 + k, r - 1 : r - 1 + n, :] * before
        summed += face[k, r + 1 : r + 1 + n, :] * after
        below, above = k + 8, k + 2
    if k > 0:
        summed += side[below, r : r + n, :] * u[o + k, r : r + n, :]
    if k < 5:
        summed += side[above, r : r + n, :] * u[o + k + 2, r : r + n, :]
    return summed


def smooth_pair(u, rhs, coef, face, side, low, high):
    def sweep(_, carry):
        for colour in (0, 1):
            for k in range(6):
                for r, n in spans(low, high, LANES):
                    new = rhs[6 * colour + k, r : r + n, :]
                    new = new + beside_pair(u, face, side, colour, k, r, n)
                    new = new * coef[12 + 6 * colour + k, r : r + n, :]
                    u[8 * colour + k + 1, r : r + n, :] = new
        return carry

    lax.fori_loop(0, 2, sweep, 0)


def residual_pair(u, rhs, coef, face, side, temp, low, high):
    for k in range(6):
        for r, n in spans(low, high, LANES):
            left = rhs[k, r : r + n, :] + beside_pair(u, face, side, 0, k, r, n)
            temp[k, r : r + n, :] = left - coef[24 + k, r : r + n, :] * u[k + 1, r : r + n, :]


def greet(waiting):
    barrier = pltpu.get_barrier_semaphore()
    gx, gy = lax.axis_index("gx"), lax.axis_index("gy")
    nx, ny = lax.axis_size("gx"), lax.axis_size("gy")
    if waiting:
        across = jnp.where(gx > 0, 1, 0) + jnp.where(gx < nx - 1, 1, 0)
        along = jnp.where(gy > 0, 1, 0) + jnp.where(gy < ny - 1, 1, 0)
        pl.semaphore_wait(barrier, nx + ny - 2 + across * along)
        return
    for step in range(1, nx):
        other = (lax.rem(gx + step, nx), gy)
        pl.semaphore_signal(barrier, inc=1, device_id=other, device_id_type=MESH)
    for step in range(1, ny):
        other = (gx, lax.rem(gy + step, ny))
        pl.semaphore_signal(barrier, inc=1, device_id=other, device_id_type=MESH)
    for dx, dy in SIDES[4:]:

        @pl.when(near(dx, dy))
        def _(dx=dx, dy=dy):
            other = (gx + dx, gy + dy)
            pl.semaphore_signal(barrier, inc=1, device_id=other, device_id_type=MESH)


def gather_copies(whole, sems, axis):
    size = lax.axis_size(axis)
    gx, gy = lax.axis_index("gx"), lax.axis_index("gy")
    made = []
    for step in range(1, size):
        if axis == "gx":
            target = (lax.rem(gx + step, size), gy)
            source = whole.at[gy, gx]
            origin = whole.at[gy, lax.rem(gx + size - step, size)]
        else:
            target = (gx, lax.rem(gy + step, size))
            source = whole.at[gy]
            origin = whole.at[lax.rem(gy + size - step, size)]
        out = pltpu.make_async_remote_copy(
            src_ref=source, dst_ref=source, send_sem=sems[0].at[step],
            recv_sem=sems[1].at[step], device_id=target, device_id_type=MESH,
        )
        into = pltpu.make_async_remote_copy(
            src_ref=origin, dst_ref=origin, send_sem=sems[0].at[step],
            recv_sem=sems[1].at[step], device_id=target, device_id_type=MESH,
        )
        made.append((out, into))
    return made


def begin(made):
    for out, _ in made:
        out.start()


def end(made):
    for out, into in made:
        out.wait_send()
        into.wait_recv()


def squeeze(planes):
    rows = 6 * LANES
    r = lax.broadcasted_iota(jnp.int32, (rows, LANES), 0)
    c = lax.broadcasted_iota(jnp.int32, (rows, LANES), 1)
    at = (c // 16) * LANES + LEFT + 4 * (c % 16)
    return split_dot(jnp.concatenate(planes, axis=1), chosen(r == at))


def place(whole, targets, h):
    ny, nx = whole.shape[:2]
    wide = min(ny, LANES // 16)

    def body(gx, carry):
        row = pl.multiple_of(8 + gx * h, 8)
        for t, (ref, first) in enumerate(targets):
            for k in range(6):
                for start in range(0, ny, wide):
                    total = jnp.zeros((h, LANES), F32)
                    lane = lane_of((h, LANES)) // 16
                    for gy in range(start, min(start + wide, ny)):
                        x = whole[gy, gx, t * h : (t + 1) * h, :]
                        x = pltpu.roll(x, (16 * (gy - start - k)) % LANES, 1)
                        total = jnp.where(lane == gy - start, x, total)
                    ref[first + k, pl.ds(row, h), start * 16 : start * 16 + LANES] = total
        return carry

    lax.fori_loop(0, nx, body, 0)


def conjugate(level, temp, out):
    u, _, rhs, coef, wr, wc, wv, gap = level
    n, columns = u.shape[1] - 16, u.shape[2]
    mid = slice(8, 8 + n)

    def summed(x):
        x = jnp.sum(x, axis=0)
        return jnp.sum(jnp.sum(x, axis=0, keepdims=True), axis=1, keepdims=True)

    inv = slice(6, 12)
    r0 = rhs[:, mid, :]
    z0 = r0 * coef[inv, mid, :]
    u[1:7, mid, :] = z0
    temp[:, mid, :] = r0
    out[:, mid, :] = jnp.zeros_like(r0)

    def step(_, rz):
        p = u[1:7, mid, :]
        image = jnp.stack(
            [
                coef[12 + k, mid, :] * p[k] - beside(u, wr, wc, wv, gap, k, 8, n, p[k])
                for k in range(6)
            ]
        )
        alpha = rz / summed(p * image)
        out[:, mid, :] += alpha[None] * p
        r = temp[:, mid, :] - alpha[None] * image
        temp[:, mid, :] = r
        z = r * coef[inv, mid, :]
        rz_new = summed(r * z)
        u[1:7, mid, :] = z + (rz_new / rz)[None] * p
        return rz_new

    lax.fori_loop(0, COARSE_ITERS, step, summed(r0 * z0))
    u[1:7, mid, :] = out[:, mid, :]


def exchanges(n0):
    n1, n2 = n0 // 2, n0 // 4
    return {
        "near": Exchange(4, n0, 25, (12, 13)),
        "coef1": Exchange(8, n1, 18, (18,)),
        "coef2": Exchange(16, n2, 18, (18,)),
        "u0": Exchange(4, n0, 12, (12,)),
        "rhs1": Exchange(8, n1, 6, (6,)),
        "u1": Exchange(8, n1, 6, (6,)),
        "rhs2": Exchange(16, n2, 6, (6,)),
        "u2": Exchange(16, n2, 6, (6,)),
    }


def scratches(n0, nx, ny):
    def planes(n, rows, columns=LANES):
        return pltpu.VMEM((n, rows, columns), F32)

    rows = n0 + 2 * BASE
    shapes = [planes(n, rows) for n in (16, 13, 36, 12, 24, 16, 12)]
    for i in (1, 2):
        r = (n0 >> i) + 2 * BASE
        shapes += [planes(n, r) for n in (8, 8, 6, 18, 6, 6, 7)]
    h = n0 >> LOCAL
    shapes += [pltpu.VMEM((ny, nx, 3 * h, LANES), F32), pltpu.VMEM((ny, nx, h, LANES), F32)]
    shapes += [pltpu.SemaphoreType.DMA((nx,)), pltpu.SemaphoreType.DMA((nx,))] * 2
    shapes += [pltpu.SemaphoreType.DMA((ny,)), pltpu.SemaphoreType.DMA((ny,))] * 2
    columns = up_to(ny * h, LANES)
    for i in range(LEVELS - LOCAL + 1):
        r = ((nx * h) >> i) + 16
        shapes += [planes(n, r, columns) for n in (8, 8, 6, 18, 6, 6, 7)]
    shapes += [planes(6, (nx * h) + 16, columns)]
    return shapes


def whole_kernel(field, labels, patch, lat_t, ver_t, sto_t, wattage, out, *refs):
    n0 = field.shape[1]
    n1, n2, h = n0 // 2, n0 // 4, n0 // 8
    nx, ny = lax.axis_size("gx"), lax.axis_size("gy")
    u0, lab, coef0, rhs0, face, side, lab_own = refs[:7]
    levels = {}
    at = 7
    for i in (1, 2):
        levels[i] = tuple(refs[at : at + 7]) + (i,)
        at += 7
    gathered_coef, gathered_rhs = refs[at : at + 2]
    sems = refs[at + 2 : at + 10]
    at += 10
    for i in range(LOCAL, LEVELS + 1):
        levels[i] = tuple(refs[at : at + 7]) + (1 << (i - LOCAL),)
        at += 7
    temp3 = refs[at]
    rest = refs[at + 1 :]
    ex = exchanges(n0)
    for e in ex.values():
        rest = e.bind(rest)
        e.clear()
    greet(False)
    for ref, planes in ((u0, 16), (coef0, 12), (face, 24)):
        border(ref, planes, BASE - HALO)
    for i, level in levels.items():
        pad = BASE - HALO if i < LOCAL else 8
        for ref, planes in ((level[0], 8), (level[1], 8), (level[3], 6)):
            border(ref, planes, pad)

    r = lax.broadcasted_iota(jnp.int32, (n0, 2 * LANES), 0)
    c = lax.broadcasted_iota(jnp.int32, (n0, 2 * LANES), 1)
    spread = chosen(r == 2 * (c % LANES - LEFT) + c // LANES)
    own = slice(BASE, BASE + n0)

    def part(k, carry):
        even = even_of(n0, k, 0)
        both = split_dot(field[k], spread)
        a, b = both[:, :LANES], both[:, LANES:]
        u0[k + 1, own, :] = jnp.where(even, a, b)
        u0[k + 9, own, :] = jnp.where(even, b, a)
        both = split_dot(labels[k].astype(F32) + F32(1.0), spread, 1)
        inside = (lane_of((n0, LANES)) >= LEFT) & (lane_of((n0, LANES)) < LEFT + 64)
        a, b = both[:, :LANES], both[:, LANES:]
        lab[k, own, :] = jnp.where(inside, jnp.where(even, a, b), 0.0)
        lab[k + 6, own, :] = jnp.where(inside, jnp.where(even, b, a), 0.0)
        return carry

    lax.fori_loop(0, 6, part, 0)
    tiles = patch[...]
    small = jnp.zeros(tiles.shape, F32)
    for m in range(wattage.shape[0]):
        small = jnp.where(tiles == m, wattage[m], small)
    th, tw = tiles.shape
    r = lax.broadcasted_iota(jnp.int32, (tw, LANES), 0)
    c = lax.broadcasted_iota(jnp.int32, (tw, LANES), 1)
    flat = chosen((c >= LEFT) & ((c - LEFT) // (TILE // 2) == r))
    heat = split_dot(small, flat)
    for i in range(th):
        lab[12, BASE + i * TILE : BASE + (i + 1) * TILE, :] = jnp.broadcast_to(
            heat[i : i + 1, :], (TILE, LANES)
        )

    fields = [(u0, (1 + k + 8 * c,)) for c in (0, 1) for k in range(6)]
    labs = [(lab, (i,)) for i in range(13)]
    edge = ex["near"]
    stage = lab_own
    for c in (0, 1):
        stage[6 * c : 6 * c + 6, own, :] = u0[1 + 8 * c : 7 + 8 * c, own, :]
    greet(True)
    edge.start(fields + labs, (stage, lab))

    tables = (lat_t, ver_t, sto_t)
    look(lab, coef0, tables, BASE, BASE + n0)
    coef1, coef2 = levels[1][3], levels[2][3]

    def first(i):
        t, k = i // 6, i % 6
        x = pair_rows(coef0, 12 * t + k, BASE, n1) + pair_rows(coef0, 12 * t + 6 + k, BASE, n1)
        coef1[i, BASE : BASE + n1, :] = x * F32(0.25)

    for i in range(18):
        first(i)
    restrict(coef1, coef2, 18, BASE, BASE, n2, 1)
    ex["coef1"].start([(coef1, (i,)) for i in range(18)], (coef1,))
    ex["coef2"].start([(coef2, (i,)) for i in range(18)], (coef2,))
    gx, gy = lax.axis_index("gx"), lax.axis_index("gy")
    for t in range(3):
        planes = [halve(coef2, 6 * t + k, BASE, h, 2) for k in range(6)]
        gathered_coef[gy, gx, t * h : (t + 1) * h, :] = squeeze(planes)
    coef_x = gather_copies(gathered_coef, sems[0:2], "gx")
    begin(coef_x)

    edge.finish()
    tops = [(edge.tops[0], i) for i in range(12)] + [(edge.tops[1], i) for i in range(13)]
    edge.unpack(fields + labs, tops, fields + labs)
    lo, hi0, hi1, hi2 = BASE - HALO, BASE + n0 + HALO, BASE + n1 + HALO, BASE + n2 + HALO
    look(lab, coef0, tables, lo, hi0)
    build_pair(coef0, lab, u0, rhs0, face, side, lo, hi0)
    smooth_pair(u0, rhs0, coef0, face, side, lo, hi0)
    temp = coef0
    residual_pair(u0, rhs0, coef0, face, side, temp, BASE, BASE + n0)
    rhs1, rhs2 = levels[1][2], levels[2][2]

    for k in range(6):
        rhs1[k, BASE : BASE + n1, :] = pair_rows(temp, k, BASE, n1) * F32(0.25)
    ex["rhs1"].start([(rhs1, (k,)) for k in range(6)], (rhs1,))
    for c in (0, 1):
        stage[6 * c : 6 * c + 6, own, :] = u0[1 + 8 * c : 7 + 8 * c, own, :]
    ex["u0"].start(fields, (stage,))

    def fill(name, ref, count, first=0):
        e = ex[name]
        e.finish()
        planes = [(ref, (first + i,)) for i in range(count)]
        e.unpack(planes, [(e.tops[0], i) for i in range(count)], planes)

    def weigh(i, low, high):
        coef, wr, wc, wv, gap = levels[i][3:]
        build(coef, wr, wc, wv, 0.25**i, gap, low, high)

    fill("coef1", coef1, 18)
    weigh(1, lo, hi1)
    fill("coef2", coef2, 18)
    weigh(2, lo, hi2)
    end(coef_x)
    coef_y = gather_copies(gathered_coef, sems[4:6], "gy")
    begin(coef_y)

    fill("rhs1", rhs1, 6)
    smooth(levels[1], lo, hi1, True)
    u1 = levels[1][0]
    residual(levels[1], temp, BASE, BASE + n1)
    restrict(temp, rhs2, 6, BASE, BASE, n2, 1)
    ex["rhs2"].start([(rhs2, (k,)) for k in range(6)], (rhs2,))
    ex["u1"].start([(u1, (k + 1,)) for k in range(6)], (u1.at[1:7],))
    end(coef_y)
    coef3 = levels[3][3]
    place(gathered_coef, [(coef3, 0), (coef3, 6), (coef3, 12)], h)

    fill("rhs2", rhs2, 6)
    smooth(levels[2], lo, hi2, True)
    u2 = levels[2][0]
    residual(levels[2], temp, BASE, BASE + n2)
    gathered_rhs[gy, gx] = squeeze([halve(temp, k, BASE, h, 2) for k in range(6)])
    rhs_x = gather_copies(gathered_rhs, sems[2:4], "gx")
    begin(rhs_x)
    ex["u2"].start([(u2, (k + 1,)) for k in range(6)], (u2.at[1:7],))

    sizes = {i: (nx * h) >> (i - LOCAL) for i in range(LOCAL, LEVELS + 1)}
    for i in range(LOCAL, LEVELS):
        restrict(levels[i][3], levels[i + 1][3], 18, 8, 8, sizes[i + 1], levels[i][-1])
    end(rhs_x)
    rhs_y = gather_copies(gathered_rhs, sems[6:8], "gy")
    begin(rhs_y)
    for i in range(LOCAL, LEVELS + 1):
        weigh(i, 8, 8 + sizes[i])
    end(rhs_y)
    place(gathered_rhs, [(levels[3][2], 0)], h)

    for i in range(LOCAL, LEVELS):
        smooth(levels[i], 8, 8 + sizes[i], True)
        residual(levels[i], temp3, 8, 8 + sizes[i])
        restrict(temp3, levels[i + 1][2], 6, 8, 8, sizes[i + 1], levels[i][-1])
    conjugate(levels[LEVELS], temp3, levels[LEVELS][2])
    for i in reversed(range(LOCAL, LEVELS)):
        prolong(levels[i + 1][0], levels[i][0], 8, sizes[i + 1], 8, levels[i][-1])
        smooth(levels[i], 8, 8 + sizes[i], False)

    u3 = levels[3][0]
    columns = u3.shape[2]
    r = lax.broadcasted_iota(jnp.int32, (columns, LANES), 0)
    c = lax.broadcasted_iota(jnp.int32, (columns, LANES), 1)
    hit = ((c & 1) == 0) & (c // 4 - LEFT // 4 + gy * 16 == r)
    widen = chosen(hit)
    fill("u2", u2, 6, 1)

    for k in range(6):
        x = u3[k + 1, pl.ds(pl.multiple_of(gx * h, 8), h + 16), :]
        x = split_dot(x, widen)
        u2[k + 1, pl.ds(0, h + 16, 2), :] += x
        u2[k + 1, pl.ds(1, h + 16, 2), :] += x
    smooth(levels[2], lo, hi2, False)
    fill("u1", u1, 6, 1)
    prolong(u2, u1, lo, n2 + 16, 0, 1)
    smooth(levels[1], lo, hi1, False)
    e = ex["u0"]
    e.finish()
    e.unpack(fields, [(e.tops[0], i) for i in range(12)], fields)

    for k in range(6):
        x = u1[k + 1, lo : lo + n1 + 16, :]
        for c in (0, 8):
            u0[c + k + 1, pl.ds(0, n1 + 16, 2), :] += x
            u0[c + k + 1, pl.ds(1, n1 + 16, 2), :] += x
    smooth_pair(u0, rhs0, coef0, face, side, lo, hi0)

    r = lax.broadcasted_iota(jnp.int32, (2 * LANES, n0), 0)
    c = lax.broadcasted_iota(jnp.int32, (2 * LANES, n0), 1)
    join = chosen(c == 2 * (r % LANES - LEFT) + r // LANES)

    def give(k, carry):
        even = even_of(n0, k, 0)
        red, black = u0[k + 1, own, :], u0[k + 9, own, :]
        both = jnp.concatenate(
            [jnp.where(even, red, black), jnp.where(even, black, red)], axis=1
        )
        out[k] = split_dot(both, join)
        return carry

    lax.fori_loop(0, 6, give, 0)


def on_device(field, substance, patch, planar, vertical, storage, wattage):
    n0 = field.shape[1]
    nx, ny = lax.axis_size("gx"), lax.axis_size("gy")
    vmem = pl.BlockSpec(memory_space=pltpu.VMEM)
    smem = pl.BlockSpec(memory_space=pltpu.SMEM)
    scratch = scratches(n0, nx, ny)
    for e in exchanges(n0).values():
        scratch += e.scratch()
    return pl.pallas_call(
        whole_kernel,
        out_shape=jax.ShapeDtypeStruct(field.shape, F32),
        in_specs=[vmem] * 3 + [smem] * 4,
        out_specs=vmem,
        scratch_shapes=scratch,
        compiler_params=pltpu.CompilerParams(vmem_limit_bytes=VM, has_side_effects=True, collective_id=0),
    )(field, substance, patch, planar, vertical, storage, wattage)


def solution(mesh):
    placed = (P(None, "gx", "gy"), P(None, "gx", "gy"), P("gx", "gy"), P(), P(), P(), P())
    return jax.shard_map(
        on_device, mesh=mesh, in_specs=placed, out_specs=P(None, "gx", "gy"), check_vma=False
    )
```

```python
import functools

import jax
import jax.numpy as jnp
from jax import lax
from jax.experimental import pallas as pl
from jax.experimental.pallas import tpu as pltpu
from jax.sharding import PartitionSpec as P

TILE = 16
LEVELS = 6
COARSE_ITERS = 12
LOCAL = 3
HALO = 8
BASE = 16
LEFT = 16
LANES = 128
F32 = jnp.float32
VM = 63 * 1024 * 1024
MESH = pl.DeviceIdType.MESH
SIDES = ((-1, 0), (1, 0), (0, -1), (0, 1), (-1, -1), (-1, 1), (1, -1), (1, 1))


def up_to(count, step):
    return -(-count // step) * step


def spans(low, high, columns):
    step = max(8, 48 * LANES // columns // 8 * 8)
    return [(r, min(step, high - r)) for r in range(low, high, step)]


def lane_of(shape):
    return lax.broadcasted_iota(jnp.int32, shape, len(shape) - 1)


def row_of(shape):
    return lax.broadcasted_iota(jnp.int32, shape, 0)


def split_dot(values, matrix, terms=3):
    total = None
    pieces = []
    for _ in range(terms):
        piece = values.astype(jnp.bfloat16)
        values = values - piece.astype(F32)
        pieces.append(piece)
    for piece in reversed(pieces):
        part = jnp.dot(piece, matrix, preferred_element_type=F32)
        total = part if total is None else total + part
    return total


def chosen(hit):
    return jnp.where(hit, F32(1.0), F32(0.0)).astype(jnp.bfloat16)


def near(dx, dy):
    ok = None
    for axis, step in (("gx", dx), ("gy", dy)):
        if step == 0:
            continue
        at = lax.axis_index(axis)
        this = (at + step < lax.axis_size(axis)) if step > 0 else (at + step >= 0)
        ok = this if ok is None else jnp.logical_and(ok, this)
    return ok


class Exchange:
    def __init__(self, rows, groups, row_refs):
        self.rows, self.row_refs = rows, row_refs
        self.twin = [g[2] for g in groups]
        self.slots, pack, lane = [], 0, 0
        for width, count, _ in groups:
            group = []
            for _ in range(count):
                if lane + width > LANES:
                    pack, lane = pack + 1, 0
                group.append((pack, lane, width))
                lane += width
            self.slots.append(group)
        self.packs = pack + 1

    def scratch(self):
        packed = pltpu.VMEM((2, self.packs, self.rows, LANES), F32)
        landed = pltpu.VMEM((2, self.packs, self.rows + 2 * HALO, LANES), F32)
        tops = [pltpu.VMEM((2, n, HALO, LANES), F32) for n, _ in self.row_refs]
        sems = pltpu.SemaphoreType.DMA((6 + 2 * len(self.row_refs),))
        return [packed, landed, sems, sems] + tops

    def bind(self, refs):
        self.packed, self.landed, self.send, self.recv = refs[:4]
        self.tops = refs[4 : 4 + len(self.row_refs)]
        return refs[4 + len(self.row_refs) :]

    def clear(self):
        self.landed[...] = jnp.zeros_like(self.landed)
        for top in self.tops:
            top[...] = jnp.zeros_like(top)

    def copies(self):
        n = self.rows
        gx, gy = lax.axis_index("gx"), lax.axis_index("gy")
        out = []
        for dy, side in ((1, 0), (-1, 1)):
            packed = self.packed.at[side]
            landed = self.landed.at[side]
            out.append((0, dy, packed, landed.at[:, HALO : HALO + n, :]))
            out.append((1, dy, packed.at[:, n - HALO : n, :], landed.at[:, 0:HALO, :]))
            out.append(
                (-1, dy, packed.at[:, 0:HALO, :], landed.at[:, HALO + n : n + 2 * HALO, :])
            )
        for source, top, (_, m) in zip(self.sources, self.tops, self.row_refs):
            out.append((1, 0, source.at[:, BASE + m - HALO : BASE + m, :], top.at[0]))
            out.append((-1, 0, source.at[:, BASE : BASE + HALO, :], top.at[1]))
        made = []
        for i, (dx, dy, source, target) in enumerate(out):
            copy = pltpu.make_async_remote_copy(
                src_ref=source,
                dst_ref=target,
                send_sem=self.send.at[i],
                recv_sem=self.recv.at[i],
                device_id=(gx + dx, gy + dy),
                device_id_type=MESH,
            )
            made.append((dx, dy, copy))
        return made

    def start(self, groups, sources):
        slots = [x for group in self.slots for x in group]
        takes = [x for group in groups for x in group]
        for r, m in spans(0, self.rows, LANES):
            lane = lane_of((m, LANES))
            packs = [[jnp.zeros((m, LANES), F32)] * 2 for _ in range(self.packs)]
            for (pack, at, w), take in zip(slots, takes):
                x = take(r, m)
                hit = (lane >= at) & (lane < at + w)
                a = pltpu.roll(x, (at - (LEFT + 64 - w)) % LANES, 1)
                b = pltpu.roll(x, (at - LEFT) % LANES, 1)
                right, left = packs[pack]
                packs[pack] = [jnp.where(hit, a, right), jnp.where(hit, b, left)]
            for pack, both in enumerate(packs):
                for side in (0, 1):
                    self.packed[side, pack, r : r + m, :] = both[side]
        self.sources = sources
        for dx, dy, copy in self.copies():
            pl.when(near(dx, dy))(copy.start)

    def finish(self):
        for dx, dy, copy in self.copies():
            pl.when(near(dx, dy))(copy.wait_send)
            pl.when(near(-dx, -dy))(copy.wait_recv)

    def merge(self, x, slot, r, m, shift=None):
        pack, at, w = slot
        lane = lane_of((m, LANES))
        inside = (lane >= LEFT - w) & (lane < LEFT)
        beyond = (lane >= LEFT + 64) & (lane < LEFT + 64 + w)
        if shift is not None:
            inside, beyond = inside & (lane % 2 == 0), beyond & (lane % 2 == 0)
        back = shift or 0
        a = pltpu.roll(self.landed[0, pack, r : r + m, :], (LEFT - w - at - back) % LANES, 1)
        b = pltpu.roll(self.landed[1, pack, r : r + m, :], (LEFT + 64 - at - back) % LANES, 1)
        return jnp.where(beyond, b, jnp.where(inside, a, x))

    def unpack(self, group, planes, tops):
        n = self.rows
        for i, (ref, plane) in enumerate(planes):
            twin = self.twin[group]
            slot = self.slots[group][i // 2 if twin else i]
            pieces = [(0, HALO, 0)]
            pieces += [(HALO + r, m, None) for r, m in spans(0, n, LANES)]
            pieces += [(HALO + n, HALO, 1)]
            for r, m, side in pieces:
                rows = slice(BASE - HALO + r, BASE - HALO + r + m)
                if side is None:
                    x = ref[plane, rows]
                else:
                    x = tops[i][0][side, tops[i][1]]
                ref[plane, rows] = self.merge(x, slot, r, m, i % 2 if twin else None)

    def unpack_folded(self, group, planes, tops):
        n = self.rows
        for i, (ref, plane) in enumerate(planes):
            top, at = tops[i]
            ref[plane, BASE - HALO : BASE] = top[0, at]
            ref[plane, BASE + 2 * n : BASE + 2 * n + HALO] = top[1, at]
            for odd in (0, 1):
                for r, m in spans(HALO // 2, n + HALO + HALO // 2, LANES):
                    rows = pl.ds(BASE + 2 * (r - HALO) + odd, m, 2)
                    slot = self.slots[group][2 * i + odd]
                    ref[plane, rows, :] = self.merge(ref[plane, rows, :], slot, r, m)


def rows_of(ref, plane):
    return lambda r, m: ref[plane, BASE + r : BASE + r + m, :]


def twins_of(ref, plane):
    def take(r, m):
        a, b = ref[plane, BASE + r : BASE + r + m, :], ref[plane + 1, BASE + r : BASE + r + m, :]
        return jnp.where(lane_of(a.shape) % 2 == 0, a, pltpu.roll(b, 1, 1))

    return take


def folds_of(ref, plane, odd):
    return lambda r, m: ref[plane, pl.ds(BASE + odd + 2 * r, m, 2), :]


def build(coef, wr, wc, wv, scale, gap, low, high):
    columns = coef.shape[2]
    half = F32(0.5 * scale)
    wv[6] = jnp.zeros(wv.shape[1:], F32)
    for k in range(6):
        for r, n in spans(low, high, columns):
            lane = lane_of((n, columns))
            here = coef[k, r : r + n, :]
            wr[k, r : r + n, :] = half * (here + coef[k, r - 1 : r - 1 + n, :])
            before = jnp.where(lane < gap, 0.0, pltpu.roll(here, gap, 1))
            wc[k, r : r + n, :] = jnp.where(lane < gap, 0.0, half * (here + before))
        here = coef[k, high : high + 8, :]
        wr[k, high : high + 8, :] = half * (here + coef[k, high - 1 : high + 7, :])
        for r, n in spans(low, high, columns):
            if k:
                inside = coef[6 + k, r : r + n, :] + coef[5 + k, r : r + n, :]
                wv[k, r : r + n, :] = F32(0.5) * inside
            else:
                wv[k, r : r + n, :] = jnp.zeros((n, columns), F32)
    for k in range(6):
        for r, n in spans(low, high, columns):
            lane = lane_of((n, columns))
            here = coef[k, r : r + n, :]
            before = jnp.where(lane < gap, 0.0, pltpu.roll(here, gap, 1))
            after = jnp.where(lane >= columns - gap, 0.0, pltpu.roll(here, columns - gap, 1))
            s = coef[12 + k, r : r + n, :]
            d = s + wr[k, r : r + n, :] + wr[k, r + 1 : r + 1 + n, :]
            d = d + half * (here + before) + half * (here + after)
            d = d + wv[k, r : r + n, :] + wv[k + 1, r : r + n, :]
            coef[12 + k, r : r + n, :] = d
            coef[6 + k, r : r + n, :] = jnp.where(
                s > 0.0, F32(1.0) / jnp.where(s > 0.0, d, 1.0), 0.0
            )


def beside(u, wr, wc, wv, gap, k, r, n, here):
    columns = u.shape[2]
    left = wc[k, r : r + n, :]
    summed = left * pltpu.roll(here, gap, 1)
    summed += pltpu.roll(left * here, columns - gap, 1)
    summed += wr[k, r : r + n, :] * u[k + 1, r - 1 : r - 1 + n, :]
    summed += wr[k, r + 1 : r + 1 + n, :] * u[k + 1, r + 1 : r + 1 + n, :]
    if k > 0:
        summed += wv[k, r : r + n, :] * u[k, r : r + n, :]
    if k < 5:
        summed += wv[k + 1, r : r + n, :] * u[k + 2, r : r + n, :]
    return summed


def coloured(n, columns, gap, k, colour):
    shape = (n, columns)
    return ((row_of(shape) + lane_of(shape) // gap + k + colour) & 1) == 0


def half_sweep(level, source, target, colour, low, high):
    rhs, coef, wr, wc, wv, gap = level[2:]
    columns = source.shape[2]
    for k in range(6):
        for r, n in spans(low, high, columns):
            here = source[k + 1, r : r + n, :]
            new = rhs[k, r : r + n, :] + beside(source, wr, wc, wv, gap, k, r, n, here)
            new = new * coef[6 + k, r : r + n, :]
            mask = coloured(n, columns, gap, k, colour)
            target[k + 1, r : r + n, :] = jnp.where(mask, new, here)


def smooth(level, low, high, fresh):
    u, v, rhs, coef, wr, wc, wv, gap = level
    columns = u.shape[2]
    if fresh:
        for k in range(6):
            for r, n in spans(low, high, columns):
                new = rhs[k, r : r + n, :] * coef[6 + k, r : r + n, :]
                v[k + 1, r : r + n, :] = jnp.where(coloured(n, columns, gap, k, 0), new, 0.0)
        half_sweep(level, v, u, 1, low, high)
        half_sweep(level, u, v, 0, low, high)
        half_sweep(level, v, u, 1, low, high)
        return

    def sweep(_, carry):
        half_sweep(level, u, v, 0, low, high)
        half_sweep(level, v, u, 1, low, high)
        return carry

    lax.fori_loop(0, 2, sweep, 0)


def residual(level, temp, low, high):
    u, _, rhs, coef, wr, wc, wv, gap = level
    columns = u.shape[2]
    for k in range(6):
        for r, n in spans(low, high, columns):
            here = u[k + 1, r : r + n, :]
            left = rhs[k, r : r + n, :] + beside(u, wr, wc, wv, gap, k, r, n, here)
            left = left - coef[12 + k, r : r + n, :] * here
            temp[k, r : r + n, :] = jnp.where(coloured(n, columns, gap, k, 0), left, 0.0)


def left_dot(matrix, values):
    a = values.astype(jnp.bfloat16)
    values = values - a.astype(F32)
    b = values.astype(jnp.bfloat16)
    c = (values - b.astype(F32)).astype(jnp.bfloat16)
    dot = functools.partial(jnp.dot, preferred_element_type=F32)
    return (dot(matrix, c) + dot(matrix, b)) + dot(matrix, a)


def pair_rows(ref, i, start, count):
    if ref.shape[2] > LANES:
        shape = (count, 2 * count)
        pick = chosen(lane_of(shape) // 2 == row_of(shape))
        return left_dot(pick, ref[i, start : start + 2 * count, :])
    return ref[i, pl.ds(start, count, 2), :] + ref[i, pl.ds(start + 1, count, 2), :]


def halve(ref, i, start, count, gap):
    x = pair_rows(ref, i, start, count)
    x = (x + pltpu.roll(x, x.shape[1] - gap, 1)) * F32(0.25)
    return jnp.where(lane_of(x.shape) % (2 * gap) == 0, x, 0.0)


def restrict(fine, coarse, planes, low_fine, low_coarse, count, gap):
    def body(i, carry):
        coarse[i, low_coarse : low_coarse + count, :] = halve(fine, i, low_fine, count, gap)
        return carry

    if fine.shape[2] > LANES:
        lax.fori_loop(0, planes, body, 0)
    else:
        for i in range(planes):
            body(i, 0)


def prolong(coarse, fine, low, count, to, gap):
    def body(k, carry):
        x = coarse[k + 1, low : low + count, :]
        x = x + pltpu.roll(x, gap, 1)
        if x.shape[1] > LANES:
            shape = (2 * count, count)
            twice = left_dot(chosen(row_of(shape) // 2 == lane_of(shape)), x)
            fine[k + 1, to : to + 2 * count, :] += twice
            return carry
        fine[k + 1, pl.ds(to, count, 2), :] += x
        fine[k + 1, pl.ds(to + 1, count, 2), :] += x
        return carry

    for k in range(6):
        body(k, 0)


def border(ref, planes, pad):
    rows = ref.shape[1]
    for start in (0, rows - pad):
        ref[0:planes, start : start + pad, :] = jnp.zeros((planes, pad, ref.shape[2]), F32)


def turned(x, even):
    return jnp.where(even, pltpu.roll(x, 1, 1), pltpu.roll(x, LANES - 1, 1))


def even_of(n, k, colour):
    return ((row_of((n, LANES)) + k + colour) & 1) == 0


def look(lab, coef, tables, low, high):
    def body(i, carry):
        for r, n in spans(low, high, LANES):
            labels = lab[i, r : r + n, :]
            found = [jnp.zeros((n, LANES), F32)] * 3
            for m in range(tables[0].shape[0]):
                hit = labels == F32(m + 1)
                found = [jnp.where(hit, t[m], x) for t, x in zip(tables, found)]
            for t in range(3):
                coef[12 * t + i, r : r + n, :] = found[t]
        return carry

    lax.fori_loop(0, 12, body, 0)


def build_pair(coef, lab, u, rhs, face, side, low, high):
    half = F32(0.5)
    for k in range(6):
        for r, n in spans(low, high, LANES):
            here = coef[k, r : r + n, :]
            other = coef[6 + k, r : r + n, :]
            face[k, r : r + n, :] = half * (here + coef[6 + k, r - 1 : r - 1 + n, :])
            face[6 + k, r : r + n, :] = half * (here + coef[6 + k, r + 1 : r + 1 + n, :])
            face[12 + k, r : r + n, :] = half * (here + other)
            face[18 + k, r : r + n, :] = half * (here + turned(other, even_of(n, k, 0)))
            v = coef[12 + k, r : r + n, :]
            if k > 0:
                side[k + 1, r : r + n, :] = half * (v + coef[17 + k, r : r + n, :])
            if k < 5:
                side[9 + k, r : r + n, :] = half * (v + coef[19 + k, r : r + n, :])
    for k in range(6):
        for r, n in spans(low, high, LANES):
            for colour in (0, 1):
                s = coef[24 + 6 * colour + k, r : r + n, :]
                if colour == 0:
                    d = s + face[k, r : r + n, :] + face[6 + k, r : r + n, :]
                    d = d + face[12 + k, r : r + n, :] + face[18 + k, r : r + n, :]
                    below, above = side[k + 1, r : r + n, :], side[9 + k, r : r + n, :]
                else:
                    d = s + face[6 + k, r - 1 : r - 1 + n, :] + face[k, r + 1 : r + 1 + n, :]
                    d = d + face[12 + k, r : r + n, :]
                    d = d + turned(face[18 + k, r : r + n, :], even_of(n, k, 1))
                    below, above = side[8 + k, r : r + n, :], side[k + 2, r : r + n, :]
                if k > 0:
                    d = d + below
                if k < 5:
                    d = d + above
                source = s * u[8 * colour + k + 1, r : r + n, :]
                if k == 0:
                    source = source + lab[12, r : r + n, :]
                rhs[6 * colour + k, r : r + n, :] = source
                coef[24 + 6 * colour + k, r : r + n, :] = d
                coef[12 + 6 * colour + k, r : r + n, :] = jnp.where(
                    s > 0.0, F32(1.0) / jnp.where(s > 0.0, d, 1.0), 0.0
                )


def beside_pair(u, face, side, colour, k, r, n):
    o = 8 * (1 - colour)
    same = u[o + k + 1, r : r + n, :]
    before = u[o + k + 1, r - 1 : r - 1 + n, :]
    after = u[o + k + 1, r + 1 : r + 1 + n, :]
    even = even_of(n, k, colour)
    if colour == 0:
        summed = face[18 + k, r : r + n, :] * turned(same, even)
        summed += face[12 + k, r : r + n, :] * same
        summed += face[k, r : r + n, :] * before + face[6 + k, r : r + n, :] * after
        below, above = k + 1, k + 9
    else:
        summed = turned(face[18 + k, r : r + n, :] * same, even)
        summed += face[12 + k, r : r + n, :] * same
        summed += face[6 + k, r - 1 : r - 1 + n, :] * before
        summed += face[k, r + 1 : r + 1 + n, :] * after
        below, above = k + 8, k + 2
    if k > 0:
        summed += side[below, r : r + n, :] * u[o + k, r : r + n, :]
    if k < 5:
        summed += side[above, r : r + n, :] * u[o + k + 2, r : r + n, :]
    return summed


def smooth_pair(u, rhs, coef, face, side, low, high):
    def sweep(_, carry):
        for colour in (0, 1):
            for k in range(6):
                for r, n in spans(low, high, LANES):
                    new = rhs[6 * colour + k, r : r + n, :]
                    new = new + beside_pair(u, face, side, colour, k, r, n)
                    new = new * coef[12 + 6 * colour + k, r : r + n, :]
                    u[8 * colour + k + 1, r : r + n, :] = new
        return carry

    lax.fori_loop(0, 2, sweep, 0)


def residual_pair(u, rhs, coef, face, side, temp, low, high):
    for k in range(6):
        for r, n in spans(low, high, LANES):
            left = rhs[k, r : r + n, :] + beside_pair(u, face, side, 0, k, r, n)
            temp[k, r : r + n, :] = left - coef[24 + k, r : r + n, :] * u[k + 1, r : r + n, :]


def greet(waiting):
    barrier = pltpu.get_barrier_semaphore()
    gx, gy = lax.axis_index("gx"), lax.axis_index("gy")
    nx, ny = lax.axis_size("gx"), lax.axis_size("gy")
    if waiting:
        across = jnp.where(gx > 0, 1, 0) + jnp.where(gx < nx - 1, 1, 0)
        along = jnp.where(gy > 0, 1, 0) + jnp.where(gy < ny - 1, 1, 0)
        pl.semaphore_wait(barrier, nx + ny - 2 + across * along)
        return
    for step in range(1, nx):
        other = (lax.rem(gx + step, nx), gy)
        pl.semaphore_signal(barrier, inc=1, device_id=other, device_id_type=MESH)
    for step in range(1, ny):
        other = (gx, lax.rem(gy + step, ny))
        pl.semaphore_signal(barrier, inc=1, device_id=other, device_id_type=MESH)
    for dx, dy in SIDES[4:]:

        @pl.when(near(dx, dy))
        def _(dx=dx, dy=dy):
            other = (gx + dx, gy + dy)
            pl.semaphore_signal(barrier, inc=1, device_id=other, device_id_type=MESH)


def gather_copies(whole, sems, phase):
    nx, ny = lax.axis_size("gx"), lax.axis_size("gy")
    gx, gy = lax.axis_index("gx"), lax.axis_index("gy")
    half = nx // 2
    kind, at = lax.rem(gx, 2), gx // 2
    moves = []
    if phase == 0:
        for step in range(1, half):
            target = (2 * lax.rem(at + step, half) + kind, gy)
            origin = lax.rem(at + half - step, half)
            moves.append((target, whole.at[kind, gy, at], whole.at[kind, gy, origin]))
    elif phase == 1:
        for step in range(1, ny):
            target = (gx, lax.rem(gy + step, ny))
            origin = lax.rem(gy + ny - step, ny)
            moves.append((target, whole.at[kind, gy], whole.at[kind, origin]))
    else:
        moves.append(((gx + 1 - 2 * kind, gy), whole.at[kind], whole.at[1 - kind]))
    made = []
    for i, (target, source, arriving) in enumerate(moves):
        both = []
        for ref in (source, arriving):
            both.append(
                pltpu.make_async_remote_copy(
                    src_ref=ref, dst_ref=ref, send_sem=sems[2 * phase].at[i],
                    recv_sem=sems[2 * phase + 1].at[i], device_id=target, device_id_type=MESH,
                )
            )
        made.append(both)
    return made


def begin(made):
    for out, _ in made:
        out.start()


def end(made):
    for out, into in made:
        out.wait_send()
        into.wait_recv()


def squeeze(planes):
    rows = 6 * LANES
    r = lax.broadcasted_iota(jnp.int32, (rows, LANES), 0)
    c = lax.broadcasted_iota(jnp.int32, (rows, LANES), 1)
    at = (c // 16) * LANES + LEFT + 4 * (c % 16)
    return split_dot(jnp.concatenate(planes, axis=1), chosen(r == at))


def place(whole, targets, h):
    _, ny, half = whole.shape[:3]
    wide = min(ny, LANES // 16)

    def body(at, carry):
        lane = lane_of((h, LANES)) // 16
        for kind in (0, 1):
            row = pl.multiple_of(8 + (2 * at + kind) * h, 8)
            for t, (ref, first) in enumerate(targets):
                for k in range(6):
                    for start in range(0, ny, wide):
                        total = jnp.zeros((h, LANES), F32)
                        for gy in range(start, min(start + wide, ny)):
                            x = whole[kind, gy, at, t * h : (t + 1) * h, :]
                            x = pltpu.roll(x, (16 * (gy - start - k)) % LANES, 1)
                            total = jnp.where(lane == gy - start, x, total)
                        ref[first + k, pl.ds(row, h), start * 16 : start * 16 + LANES] = total
        return carry

    lax.fori_loop(0, half, body, 0)


def conjugate(level, temp, out):
    u, _, rhs, coef, wr, wc, wv, gap = level
    n, columns = u.shape[1] - 16, u.shape[2]
    mid = slice(8, 8 + n)

    def summed(x):
        x = jnp.sum(x, axis=0)
        return jnp.sum(jnp.sum(x, axis=0, keepdims=True), axis=1, keepdims=True)

    inv = slice(6, 12)
    r0 = rhs[:, mid, :]
    z0 = r0 * coef[inv, mid, :]
    u[1:7, mid, :] = z0
    temp[:, mid, :] = r0
    out[:, mid, :] = jnp.zeros_like(r0)

    def step(_, rz):
        p = u[1:7, mid, :]
        image = jnp.stack(
            [
                coef[12 + k, mid, :] * p[k] - beside(u, wr, wc, wv, gap, k, 8, n, p[k])
                for k in range(6)
            ]
        )
        alpha = rz / summed(p * image)
        out[:, mid, :] += alpha[None] * p
        r = temp[:, mid, :] - alpha[None] * image
        temp[:, mid, :] = r
        z = r * coef[inv, mid, :]
        rz_new = summed(r * z)
        u[1:7, mid, :] = z + (rz_new / rz)[None] * p
        return rz_new

    lax.fori_loop(0, COARSE_ITERS, step, summed(r0 * z0))
    u[1:7, mid, :] = out[:, mid, :]


def exchanges(n0):
    n1, n2 = n0 // 2, n0 // 4
    return {
        "near": Exchange(n0, [(4, 12, False), (4, 13, False)], [(12, n0), (13, n0)]),
        "coef1": Exchange(n1, [(7, 18, False)], [(18, n1)]),
        "coef2": Exchange(n2, [(14, 9, True)], [(18, n2)]),
        "rhs1": Exchange(n1, [(6, 6, False), (2, 24, False)], [(6, n1), (12, n0)]),
        "rhs2": Exchange(n2, [(12, 3, True), (6, 12, False)], [(6, n2), (6, n1)]),
        "u2": Exchange(n2, [(14, 3, True)], [(6, n2)]),
    }


def scratches(n0, nx, ny):
    def planes(n, rows, columns=LANES):
        return pltpu.VMEM((n, rows, columns), F32)

    rows = n0 + 2 * BASE
    shapes = [planes(n, rows) for n in (16, 13, 36, 12, 24, 16, 12)]
    for i in (1, 2):
        r = (n0 >> i) + 2 * BASE
        shapes += [planes(n, r) for n in (8, 8, 6, 18, 6, 6, 7)]
    h = n0 >> LOCAL
    for n in (3 * h, h):
        shapes += [pltpu.VMEM((2, ny, nx // 2, n, LANES), F32)]
    for _ in range(2):
        for n in (nx, nx, ny, ny, 1, 1):
            shapes += [pltpu.SemaphoreType.DMA((n,))]
    columns = up_to(ny * h, LANES)
    for i in range(LEVELS - LOCAL + 1):
        r = ((nx * h) >> i) + 16
        shapes += [planes(n, r, columns) for n in (8, 8, 6, 18, 6, 6, 7)]
    shapes += [planes(6, (nx * h) + 16, columns)]
    return shapes


def whole_kernel(field, labels, patch, lat_t, ver_t, sto_t, wattage, out, *refs):
    n0 = field.shape[1]
    n1, n2, h = n0 // 2, n0 // 4, n0 // 8
    nx, ny = lax.axis_size("gx"), lax.axis_size("gy")
    u0, lab, coef0, rhs0, face, side, lab_own = refs[:7]
    levels = {}
    at = 7
    for i in (1, 2):
        levels[i] = tuple(refs[at : at + 7]) + (i,)
        at += 7
    gathered_coef, gathered_rhs = refs[at : at + 2]
    coef_sems, rhs_sems = refs[at + 2 : at + 8], refs[at + 8 : at + 14]
    at += 14
    for i in range(LOCAL, LEVELS + 1):
        levels[i] = tuple(refs[at : at + 7]) + (1 << (i - LOCAL),)
        at += 7
    temp3 = refs[at]
    rest = refs[at + 1 :]
    ex = exchanges(n0)
    for e in ex.values():
        rest = e.bind(rest)
        e.clear()
    greet(False)
    for ref, planes in ((u0, 16), (coef0, 12), (face, 24)):
        border(ref, planes, BASE - HALO)
    for i, level in levels.items():
        pad = BASE - HALO if i < LOCAL else 8
        for ref, planes in ((level[0], 8), (level[1], 8), (level[3], 6)):
            border(ref, planes, pad)

    r = lax.broadcasted_iota(jnp.int32, (n0, 2 * LANES), 0)
    c = lax.broadcasted_iota(jnp.int32, (n0, 2 * LANES), 1)
    spread = chosen(r == 2 * (c % LANES - LEFT) + c // LANES)
    own = slice(BASE, BASE + n0)

    def part(k, carry):
        even = even_of(n0, k, 0)
        both = split_dot(field[k], spread)
        a, b = both[:, :LANES], both[:, LANES:]
        u0[k + 1, own, :] = jnp.where(even, a, b)
        u0[k + 9, own, :] = jnp.where(even, b, a)
        both = split_dot(labels[k].astype(F32) + F32(1.0), spread, 1)
        inside = (lane_of((n0, LANES)) >= LEFT) & (lane_of((n0, LANES)) < LEFT + 64)
        a, b = both[:, :LANES], both[:, LANES:]
        lab[k, own, :] = jnp.where(inside, jnp.where(even, a, b), 0.0)
        lab[k + 6, own, :] = jnp.where(inside, jnp.where(even, b, a), 0.0)
        return carry

    lax.fori_loop(0, 6, part, 0)
    tiles = patch[...]
    small = jnp.zeros(tiles.shape, F32)
    for m in range(wattage.shape[0]):
        small = jnp.where(tiles == m, wattage[m], small)
    th, tw = tiles.shape
    r = lax.broadcasted_iota(jnp.int32, (tw, LANES), 0)
    c = lax.broadcasted_iota(jnp.int32, (tw, LANES), 1)
    flat = chosen((c >= LEFT) & ((c - LEFT) // (TILE // 2) == r))
    heat = split_dot(small, flat)
    for i in range(th):
        lab[12, BASE + i * TILE : BASE + (i + 1) * TILE, :] = jnp.broadcast_to(
            heat[i : i + 1, :], (TILE, LANES)
        )

    fields = [(u0, 1 + k + 8 * c) for c in (0, 1) for k in range(6)]
    labs = [(lab, i) for i in range(13)]
    edge = ex["near"]
    stage = lab_own

    def restage():
        for c in (0, 1):
            for r in (BASE, BASE + n0 - HALO):
                rows = slice(r, r + HALO)
                stage[6 * c : 6 * c + 6, rows, :] = u0[1 + 8 * c : 7 + 8 * c, rows, :]

    restage()
    greet(True)
    edge.start([[rows_of(*p) for p in fields], [rows_of(*p) for p in labs]], (stage, lab))

    tables = (lat_t, ver_t, sto_t)
    look(lab, coef0, tables, BASE, BASE + n0)
    coef1, coef2 = levels[1][3], levels[2][3]

    def first(i):
        t, k = i // 6, i % 6
        x = pair_rows(coef0, 12 * t + k, BASE, n1) + pair_rows(coef0, 12 * t + 6 + k, BASE, n1)
        coef1[i, BASE : BASE + n1, :] = x * F32(0.25)

    for i in range(18):
        first(i)
    restrict(coef1, coef2, 18, BASE, BASE, n2, 1)
    ex["coef1"].start([[rows_of(coef1, i) for i in range(18)]], (coef1,))
    ex["coef2"].start([[twins_of(coef2, i) for i in range(0, 18, 2)]], (coef2,))
    gx, gy = lax.axis_index("gx"), lax.axis_index("gy")
    mine = (lax.rem(gx, 2), gy, gx // 2)
    for t in range(3):
        planes = [halve(coef2, 6 * t + k, BASE, h, 2) for k in range(6)]
        gathered_coef[mine + (slice(t * h, (t + 1) * h),)] = squeeze(planes)
    coef_moves = [gather_copies(gathered_coef, coef_sems, phase) for phase in range(3)]
    begin(coef_moves[0])

    edge.finish()
    edge.unpack(0, fields, [(edge.tops[0], i) for i in range(12)])
    edge.unpack(1, labs, [(edge.tops[1], i) for i in range(13)])
    lo, hi0, hi1, hi2 = BASE - HALO, BASE + n0 + HALO, BASE + n1 + HALO, BASE + n2 + HALO
    look(lab, coef0, tables, lo, hi0)
    build_pair(coef0, lab, u0, rhs0, face, side, lo, hi0)
    end(coef_moves[0])
    begin(coef_moves[1])
    smooth_pair(u0, rhs0, coef0, face, side, lo, hi0)
    temp = coef0
    residual_pair(u0, rhs0, coef0, face, side, temp, BASE, BASE + n0)
    rhs1, rhs2 = levels[1][2], levels[2][2]

    for k in range(6):
        rhs1[k, BASE : BASE + n1, :] = pair_rows(temp, k, BASE, n1) * F32(0.25)
    restage()
    folded = [folds_of(ref, plane, odd) for ref, plane in fields for odd in (0, 1)]
    ex["rhs1"].start([[rows_of(rhs1, k) for k in range(6)], folded], (rhs1, stage))

    def fill(name, ref, count, first=0):
        e = ex[name]
        e.finish()
        e.unpack(0, [(ref, first + i) for i in range(count)], [(e.tops[0], i) for i in range(count)])

    def weigh(i, low, high):
        coef, wr, wc, wv, gap = levels[i][3:]
        build(coef, wr, wc, wv, 0.25**i, gap, low, high)

    fill("coef1", coef1, 18)
    weigh(1, lo, hi1)
    fill("coef2", coef2, 18)
    weigh(2, lo, hi2)

    fill("rhs1", rhs1, 6)
    smooth(levels[1], lo, hi1, True)
    u1 = levels[1][0]
    residual(levels[1], temp, BASE, BASE + n1)
    restrict(temp, rhs2, 6, BASE, BASE, n2, 1)
    folded = [folds_of(u1, k + 1, odd) for k in range(6) for odd in (0, 1)]
    ex["rhs2"].start([[twins_of(rhs2, k) for k in (0, 2, 4)], folded], (rhs2, u1.at[1:7]))
    end(coef_moves[1])
    begin(coef_moves[2])

    fill("rhs2", rhs2, 6)
    smooth(levels[2], lo, hi2, True)
    u2 = levels[2][0]
    residual(levels[2], temp, BASE, BASE + n2)
    gathered_rhs[mine] = squeeze([halve(temp, k, BASE, h, 2) for k in range(6)])
    rhs_moves = [gather_copies(gathered_rhs, rhs_sems, phase) for phase in range(3)]
    begin(rhs_moves[0])
    ex["u2"].start([[twins_of(u2, k) for k in (1, 3, 5)]], (u2.at[1:7],))
    end(coef_moves[2])
    coef3 = levels[3][3]
    place(gathered_coef, [(coef3, 0), (coef3, 6), (coef3, 12)], h)

    sizes = {i: (nx * h) >> (i - LOCAL) for i in range(LOCAL, LEVELS + 1)}
    for i in range(LOCAL, LEVELS):
        restrict(levels[i][3], levels[i + 1][3], 18, 8, 8, sizes[i + 1], levels[i][-1])
    end(rhs_moves[0])
    begin(rhs_moves[1])
    for i in range(LOCAL, LEVELS + 1):
        weigh(i, 8, 8 + sizes[i])
    end(rhs_moves[1])
    begin(rhs_moves[2])
    end(rhs_moves[2])
    place(gathered_rhs, [(levels[3][2], 0)], h)

    for i in range(LOCAL, LEVELS):
        smooth(levels[i], 8, 8 + sizes[i], True)
        residual(levels[i], temp3, 8, 8 + sizes[i])
        restrict(temp3, levels[i + 1][2], 6, 8, 8, sizes[i + 1], levels[i][-1])
    conjugate(levels[LEVELS], temp3, levels[LEVELS][2])
    for i in reversed(range(LOCAL, LEVELS)):
        prolong(levels[i + 1][0], levels[i][0], 8, sizes[i + 1], 8, levels[i][-1])
        smooth(levels[i], 8, 8 + sizes[i], False)

    u3 = levels[3][0]
    columns = u3.shape[2]
    r = lax.broadcasted_iota(jnp.int32, (columns, LANES), 0)
    c = lax.broadcasted_iota(jnp.int32, (columns, LANES), 1)
    hit = ((c & 1) == 0) & (c // 4 - LEFT // 4 + gy * 16 == r)
    widen = chosen(hit)
    fill("u2", u2, 6, 1)

    for k in range(6):
        x = u3[k + 1, pl.ds(pl.multiple_of(gx * h, 8), h + 16), :]
        x = split_dot(x, widen)
        u2[k + 1, pl.ds(0, h + 16, 2), :] += x
        u2[k + 1, pl.ds(1, h + 16, 2), :] += x
    smooth(levels[2], lo, hi2, False)
    e = ex["rhs2"]
    e.unpack_folded(1, [(u1, k + 1) for k in range(6)], [(e.tops[1], k) for k in range(6)])
    prolong(u2, u1, lo, n2 + 16, 0, 1)
    smooth(levels[1], lo, hi1, False)
    e = ex["rhs1"]
    e.unpack_folded(1, fields, [(e.tops[1], i) for i in range(12)])

    for k in range(6):
        x = u1[k + 1, lo : lo + n1 + 16, :]
        for c in (0, 8):
            u0[c + k + 1, pl.ds(0, n1 + 16, 2), :] += x
            u0[c + k + 1, pl.ds(1, n1 + 16, 2), :] += x
    smooth_pair(u0, rhs0, coef0, face, side, lo, hi0)

    r = lax.broadcasted_iota(jnp.int32, (2 * LANES, n0), 0)
    c = lax.broadcasted_iota(jnp.int32, (2 * LANES, n0), 1)
    join = chosen(c == 2 * (r % LANES - LEFT) + r // LANES)

    def give(k, carry):
        even = even_of(n0, k, 0)
        red, black = u0[k + 1, own, :], u0[k + 9, own, :]
        both = jnp.concatenate(
            [jnp.where(even, red, black), jnp.where(even, black, red)], axis=1
        )
        out[k] = split_dot(both, join)
        return carry

    lax.fori_loop(0, 6, give, 0)


def on_device(field, substance, patch, planar, vertical, storage, wattage):
    n0 = field.shape[1]
    nx, ny = lax.axis_size("gx"), lax.axis_size("gy")
    vmem = pl.BlockSpec(memory_space=pltpu.VMEM)
    smem = pl.BlockSpec(memory_space=pltpu.SMEM)
    scratch = scratches(n0, nx, ny)
    for e in exchanges(n0).values():
        scratch += e.scratch()
    return pl.pallas_call(
        whole_kernel,
        out_shape=jax.ShapeDtypeStruct(field.shape, F32),
        in_specs=[vmem] * 3 + [smem] * 4,
        out_specs=vmem,
        scratch_shapes=scratch,
        compiler_params=pltpu.CompilerParams(vmem_limit_bytes=VM, has_side_effects=True, collective_id=0),
    )(field, substance, patch, planar, vertical, storage, wattage)


def solution(mesh):
    placed = (P(None, "gx", "gy"), P(None, "gx", "gy"), P("gx", "gy"), P(), P(), P(), P())
    return jax.shard_map(
        on_device, mesh=mesh, in_specs=placed, out_specs=P(None, "gx", "gy"), check_vma=False
    )
```

```python
import functools

import jax
import jax.numpy as jnp
from jax import lax
from jax.experimental import pallas as pl
from jax.experimental.pallas import tpu as pltpu
from jax.sharding import PartitionSpec as P

TILE = 16
LEVELS = 6
COARSE_ITERS = 12
LOCAL = 3
HALO = 8
BASE = 16
LEFT = 16
LANES = 128
F32 = jnp.float32
VM = 63 * 1024 * 1024
MESH = pl.DeviceIdType.MESH
SIDES = ((-1, 0), (1, 0), (0, -1), (0, 1), (-1, -1), (-1, 1), (1, -1), (1, 1))


def up_to(count, step):
    return -(-count // step) * step


def spans(low, high, columns):
    step = max(8, 48 * LANES // columns // 8 * 8)
    return [(r, min(step, high - r)) for r in range(low, high, step)]


def lane_of(shape):
    return lax.broadcasted_iota(jnp.int32, shape, len(shape) - 1)


def row_of(shape):
    return lax.broadcasted_iota(jnp.int32, shape, 0)


def split_dot(values, matrix, terms=3):
    total = None
    pieces = []
    for _ in range(terms):
        piece = values.astype(jnp.bfloat16)
        values = values - piece.astype(F32)
        pieces.append(piece)
    for piece in reversed(pieces):
        part = jnp.dot(piece, matrix, preferred_element_type=F32)
        total = part if total is None else total + part
    return total


def chosen(hit):
    return jnp.where(hit, F32(1.0), F32(0.0)).astype(jnp.bfloat16)


def near(dx, dy):
    ok = None
    for axis, step in (("gx", dx), ("gy", dy)):
        if step == 0:
            continue
        at = lax.axis_index(axis)
        this = (at + step < lax.axis_size(axis)) if step > 0 else (at + step >= 0)
        ok = this if ok is None else jnp.logical_and(ok, this)
    return ok


class Exchange:
    def __init__(self, rows, groups, row_refs):
        self.rows, self.row_refs = rows, row_refs
        self.twin = [g[2] for g in groups]
        self.slots, pack, lane = [], 0, 0
        for width, count, _ in groups:
            group = []
            for _ in range(count):
                if lane + width > LANES:
                    pack, lane = pack + 1, 0
                group.append((pack, lane, width))
                lane += width
            self.slots.append(group)
        self.packs = pack + 1

    def scratch(self):
        packed = pltpu.VMEM((2, self.packs, self.rows, LANES), F32)
        landed = pltpu.VMEM((2, self.packs, self.rows + 2 * HALO, LANES), F32)
        tops = [pltpu.VMEM((2, n, HALO, LANES), F32) for n, _ in self.row_refs]
        sems = pltpu.SemaphoreType.DMA((6 + 2 * len(self.row_refs),))
        return [packed, landed, sems, sems] + tops

    def bind(self, refs):
        self.packed, self.landed, self.send, self.recv = refs[:4]
        self.tops = refs[4 : 4 + len(self.row_refs)]
        return refs[4 + len(self.row_refs) :]

    def clear(self):
        self.landed[...] = jnp.zeros_like(self.landed)
        for top in self.tops:
            top[...] = jnp.zeros_like(top)

    def copies(self):
        n = self.rows
        gx, gy = lax.axis_index("gx"), lax.axis_index("gy")
        out = []
        for dy, side in ((1, 0), (-1, 1)):
            packed = self.packed.at[side]
            landed = self.landed.at[side]
            out.append((0, dy, packed, landed.at[:, HALO : HALO + n, :]))
            out.append((1, dy, packed.at[:, n - HALO : n, :], landed.at[:, 0:HALO, :]))
            out.append(
                (-1, dy, packed.at[:, 0:HALO, :], landed.at[:, HALO + n : n + 2 * HALO, :])
            )
        for source, top, (_, m) in zip(self.sources, self.tops, self.row_refs):
            out.append((1, 0, source.at[:, BASE + m - HALO : BASE + m, :], top.at[0]))
            out.append((-1, 0, source.at[:, BASE : BASE + HALO, :], top.at[1]))
        made = []
        for i, (dx, dy, source, target) in enumerate(out):
            copy = pltpu.make_async_remote_copy(
                src_ref=source,
                dst_ref=target,
                send_sem=self.send.at[i],
                recv_sem=self.recv.at[i],
                device_id=(gx + dx, gy + dy),
                device_id_type=MESH,
            )
            made.append((dx, dy, copy))
        return made

    def start(self, groups, sources, now=True):
        slots = [x for group in self.slots for x in group]
        takes = [x for group in groups for x in group]
        for r, m in spans(0, self.rows, LANES):
            lane = lane_of((m, LANES))
            packs = [[jnp.zeros((m, LANES), F32)] * 2 for _ in range(self.packs)]
            for (pack, at, w), take in zip(slots, takes):
                x = take(r, m)
                hit = (lane >= at) & (lane < at + w)
                a = pltpu.roll(x, (at - (LEFT + 64 - w)) % LANES, 1)
                b = pltpu.roll(x, (at - LEFT) % LANES, 1)
                right, left = packs[pack]
                packs[pack] = [jnp.where(hit, a, right), jnp.where(hit, b, left)]
            for pack, both in enumerate(packs):
                for side in (0, 1):
                    self.packed[side, pack, r : r + m, :] = both[side]
        self.sources = sources
        if now:
            self.launch()

    def launch(self):
        for dx, dy, copy in self.copies():
            pl.when(near(dx, dy))(copy.start)

    def finish(self):
        for dx, dy, copy in self.copies():
            pl.when(near(dx, dy))(copy.wait_send)
            pl.when(near(-dx, -dy))(copy.wait_recv)

    def merge(self, x, slot, r, m, shift=None):
        pack, at, w = slot
        lane = lane_of((m, LANES))
        inside = (lane >= LEFT - w) & (lane < LEFT)
        beyond = (lane >= LEFT + 64) & (lane < LEFT + 64 + w)
        if shift is not None:
            inside, beyond = inside & (lane % 2 == 0), beyond & (lane % 2 == 0)
        back = shift or 0
        a = pltpu.roll(self.landed[0, pack, r : r + m, :], (LEFT - w - at - back) % LANES, 1)
        b = pltpu.roll(self.landed[1, pack, r : r + m, :], (LEFT + 64 - at - back) % LANES, 1)
        return jnp.where(beyond, b, jnp.where(inside, a, x))

    def unpack(self, group, planes, tops):
        n = self.rows
        for i, (ref, plane) in enumerate(planes):
            twin = self.twin[group]
            slot = self.slots[group][i // 2 if twin else i]
            pieces = [(0, HALO, 0)]
            pieces += [(HALO + r, m, None) for r, m in spans(0, n, LANES)]
            pieces += [(HALO + n, HALO, 1)]
            for r, m, side in pieces:
                rows = slice(BASE - HALO + r, BASE - HALO + r + m)
                if side is None:
                    x = ref[plane, rows]
                else:
                    x = tops[i][0][side, tops[i][1]]
                ref[plane, rows] = self.merge(x, slot, r, m, i % 2 if twin else None)

    def unpack_folded(self, group, planes, tops):
        n = self.rows
        for i, (ref, plane) in enumerate(planes):
            top, at = tops[i]
            ref[plane, BASE - HALO : BASE] = top[0, at]
            ref[plane, BASE + 2 * n : BASE + 2 * n + HALO] = top[1, at]
            for odd in (0, 1):
                for r, m in spans(HALO // 2, n + HALO + HALO // 2, LANES):
                    rows = pl.ds(BASE + 2 * (r - HALO) + odd, m, 2)
                    slot = self.slots[group][2 * i + odd]
                    ref[plane, rows, :] = self.merge(ref[plane, rows, :], slot, r, m)


def rows_of(ref, plane):
    return lambda r, m: ref[plane, BASE + r : BASE + r + m, :]


def twins_of(ref, plane):
    def take(r, m):
        a, b = ref[plane, BASE + r : BASE + r + m, :], ref[plane + 1, BASE + r : BASE + r + m, :]
        return jnp.where(lane_of(a.shape) % 2 == 0, a, pltpu.roll(b, 1, 1))

    return take


def folds_of(ref, plane, odd):
    return lambda r, m: ref[plane, pl.ds(BASE + odd + 2 * r, m, 2), :]


def build(coef, wr, wc, wv, scale, gap, low, high):
    columns = coef.shape[2]
    half = F32(0.5 * scale)
    wv[6] = jnp.zeros(wv.shape[1:], F32)
    for k in range(6):
        for r, n in spans(low, high, columns):
            lane = lane_of((n, columns))
            here = coef[k, r : r + n, :]
            wr[k, r : r + n, :] = half * (here + coef[k, r - 1 : r - 1 + n, :])
            before = jnp.where(lane < gap, 0.0, pltpu.roll(here, gap, 1))
            wc[k, r : r + n, :] = jnp.where(lane < gap, 0.0, half * (here + before))
        here = coef[k, high : high + 8, :]
        wr[k, high : high + 8, :] = half * (here + coef[k, high - 1 : high + 7, :])
        for r, n in spans(low, high, columns):
            if k:
                inside = coef[6 + k, r : r + n, :] + coef[5 + k, r : r + n, :]
                wv[k, r : r + n, :] = F32(0.5) * inside
            else:
                wv[k, r : r + n, :] = jnp.zeros((n, columns), F32)
    for k in range(6):
        for r, n in spans(low, high, columns):
            lane = lane_of((n, columns))
            here = coef[k, r : r + n, :]
            before = jnp.where(lane < gap, 0.0, pltpu.roll(here, gap, 1))
            after = jnp.where(lane >= columns - gap, 0.0, pltpu.roll(here, columns - gap, 1))
            s = coef[12 + k, r : r + n, :]
            d = s + wr[k, r : r + n, :] + wr[k, r + 1 : r + 1 + n, :]
            d = d + half * (here + before) + half * (here + after)
            d = d + wv[k, r : r + n, :] + wv[k + 1, r : r + n, :]
            coef[12 + k, r : r + n, :] = d
            coef[6 + k, r : r + n, :] = jnp.where(
                s > 0.0, F32(1.0) / jnp.where(s > 0.0, d, 1.0), 0.0
            )


def beside(u, wr, wc, wv, gap, k, r, n, here):
    columns = u.shape[2]
    left = wc[k, r : r + n, :]
    summed = left * pltpu.roll(here, gap, 1)
    summed += pltpu.roll(left * here, columns - gap, 1)
    summed += wr[k, r : r + n, :] * u[k + 1, r - 1 : r - 1 + n, :]
    summed += wr[k, r + 1 : r + 1 + n, :] * u[k + 1, r + 1 : r + 1 + n, :]
    if k > 0:
        summed += wv[k, r : r + n, :] * u[k, r : r + n, :]
    if k < 5:
        summed += wv[k + 1, r : r + n, :] * u[k + 2, r : r + n, :]
    return summed


def coloured(n, columns, gap, k, colour):
    shape = (n, columns)
    return ((row_of(shape) + lane_of(shape) // gap + k + colour) & 1) == 0


def half_sweep(level, source, target, colour, low, high):
    rhs, coef, wr, wc, wv, gap = level[2:]
    columns = source.shape[2]
    for k in range(6):
        for r, n in spans(low, high, columns):
            here = source[k + 1, r : r + n, :]
            new = rhs[k, r : r + n, :] + beside(source, wr, wc, wv, gap, k, r, n, here)
            new = new * coef[6 + k, r : r + n, :]
            mask = coloured(n, columns, gap, k, colour)
            target[k + 1, r : r + n, :] = jnp.where(mask, new, here)


def smooth(level, low, high, fresh):
    u, v, rhs, coef, wr, wc, wv, gap = level
    columns = u.shape[2]
    if fresh:
        for k in range(6):
            for r, n in spans(low, high, columns):
                new = rhs[k, r : r + n, :] * coef[6 + k, r : r + n, :]
                v[k + 1, r : r + n, :] = jnp.where(coloured(n, columns, gap, k, 0), new, 0.0)
        half_sweep(level, v, u, 1, low, high)
        half_sweep(level, u, v, 0, low, high)
        half_sweep(level, v, u, 1, low, high)
        return

    def sweep(_, carry):
        half_sweep(level, u, v, 0, low, high)
        half_sweep(level, v, u, 1, low, high)
        return carry

    lax.fori_loop(0, 2, sweep, 0)


def residual(level, temp, low, high):
    u, _, rhs, coef, wr, wc, wv, gap = level
    columns = u.shape[2]
    for k in range(6):
        for r, n in spans(low, high, columns):
            here = u[k + 1, r : r + n, :]
            left = rhs[k, r : r + n, :] + beside(u, wr, wc, wv, gap, k, r, n, here)
            left = left - coef[12 + k, r : r + n, :] * here
            temp[k, r : r + n, :] = jnp.where(coloured(n, columns, gap, k, 0), left, 0.0)


def left_dot(matrix, values):
    a = values.astype(jnp.bfloat16)
    values = values - a.astype(F32)
    b = values.astype(jnp.bfloat16)
    c = (values - b.astype(F32)).astype(jnp.bfloat16)
    dot = functools.partial(jnp.dot, preferred_element_type=F32)
    return (dot(matrix, c) + dot(matrix, b)) + dot(matrix, a)


def pair_rows(ref, i, start, count):
    if ref.shape[2] > LANES:
        shape = (count, 2 * count)
        pick = chosen(lane_of(shape) // 2 == row_of(shape))
        return left_dot(pick, ref[i, start : start + 2 * count, :])
    return ref[i, pl.ds(start, count, 2), :] + ref[i, pl.ds(start + 1, count, 2), :]


def halve(ref, i, start, count, gap):
    x = pair_rows(ref, i, start, count)
    x = (x + pltpu.roll(x, x.shape[1] - gap, 1)) * F32(0.25)
    return jnp.where(lane_of(x.shape) % (2 * gap) == 0, x, 0.0)


def restrict(fine, coarse, planes, low_fine, low_coarse, count, gap):
    def body(i, carry):
        coarse[i, low_coarse : low_coarse + count, :] = halve(fine, i, low_fine, count, gap)
        return carry

    if fine.shape[2] > LANES:
        lax.fori_loop(0, planes, body, 0)
    else:
        for i in range(planes):
            body(i, 0)


def prolong(coarse, fine, low, count, to, gap):
    def body(k, carry):
        x = coarse[k + 1, low : low + count, :]
        x = x + pltpu.roll(x, gap, 1)
        if x.shape[1] > LANES:
            shape = (2 * count, count)
            twice = left_dot(chosen(row_of(shape) // 2 == lane_of(shape)), x)
            fine[k + 1, to : to + 2 * count, :] += twice
            return carry
        fine[k + 1, pl.ds(to, count, 2), :] += x
        fine[k + 1, pl.ds(to + 1, count, 2), :] += x
        return carry

    for k in range(6):
        body(k, 0)


def border(ref, planes, pad):
    rows = ref.shape[1]
    for start in (0, rows - pad):
        ref[0:planes, start : start + pad, :] = jnp.zeros((planes, pad, ref.shape[2]), F32)


def turned(x, even):
    return jnp.where(even, pltpu.roll(x, 1, 1), pltpu.roll(x, LANES - 1, 1))


def even_of(n, k, colour):
    return ((row_of((n, LANES)) + k + colour) & 1) == 0


def look(lab, coef, tables, low, high):
    def body(i, carry):
        for r, n in spans(low, high, LANES):
            labels = lab[i, r : r + n, :]
            found = [jnp.zeros((n, LANES), F32)] * 3
            for m in range(tables[0].shape[0]):
                hit = labels == F32(m + 1)
                found = [jnp.where(hit, t[m], x) for t, x in zip(tables, found)]
            for t in range(3):
                coef[12 * t + i, r : r + n, :] = found[t]
        return carry

    lax.fori_loop(0, 12, body, 0)


def build_pair(coef, lab, u, rhs, face, side, low, high):
    half = F32(0.5)
    for k in range(6):
        for r, n in spans(low, high, LANES):
            here = coef[k, r : r + n, :]
            other = coef[6 + k, r : r + n, :]
            face[k, r : r + n, :] = half * (here + coef[6 + k, r - 1 : r - 1 + n, :])
            face[6 + k, r : r + n, :] = half * (here + coef[6 + k, r + 1 : r + 1 + n, :])
            face[12 + k, r : r + n, :] = half * (here + other)
            face[18 + k, r : r + n, :] = half * (here + turned(other, even_of(n, k, 0)))
            v = coef[12 + k, r : r + n, :]
            if k > 0:
                side[k + 1, r : r + n, :] = half * (v + coef[17 + k, r : r + n, :])
            if k < 5:
                side[9 + k, r : r + n, :] = half * (v + coef[19 + k, r : r + n, :])
    for k in range(6):
        for r, n in spans(low, high, LANES):
            for colour in (0, 1):
                s = coef[24 + 6 * colour + k, r : r + n, :]
                if colour == 0:
                    d = s + face[k, r : r + n, :] + face[6 + k, r : r + n, :]
                    d = d + face[12 + k, r : r + n, :] + face[18 + k, r : r + n, :]
                    below, above = side[k + 1, r : r + n, :], side[9 + k, r : r + n, :]
                else:
                    d = s + face[6 + k, r - 1 : r - 1 + n, :] + face[k, r + 1 : r + 1 + n, :]
                    d = d + face[12 + k, r : r + n, :]
                    d = d + turned(face[18 + k, r : r + n, :], even_of(n, k, 1))
                    below, above = side[8 + k, r : r + n, :], side[k + 2, r : r + n, :]
                if k > 0:
                    d = d + below
                if k < 5:
                    d = d + above
                source = s * u[8 * colour + k + 1, r : r + n, :]
                if k == 0:
                    source = source + lab[12, r : r + n, :]
                rhs[6 * colour + k, r : r + n, :] = source
                coef[24 + 6 * colour + k, r : r + n, :] = d
                coef[12 + 6 * colour + k, r : r + n, :] = jnp.where(
                    s > 0.0, F32(1.0) / jnp.where(s > 0.0, d, 1.0), 0.0
                )


def beside_pair(u, face, side, colour, k, r, n):
    o = 8 * (1 - colour)
    same = u[o + k + 1, r : r + n, :]
    before = u[o + k + 1, r - 1 : r - 1 + n, :]
    after = u[o + k + 1, r + 1 : r + 1 + n, :]
    even = even_of(n, k, colour)
    if colour == 0:
        summed = face[18 + k, r : r + n, :] * turned(same, even)
        summed += face[12 + k, r : r + n, :] * same
        summed += face[k, r : r + n, :] * before + face[6 + k, r : r + n, :] * after
        below, above = k + 1, k + 9
    else:
        summed = turned(face[18 + k, r : r + n, :] * same, even)
        summed += face[12 + k, r : r + n, :] * same
        summed += face[6 + k, r - 1 : r - 1 + n, :] * before
        summed += face[k, r + 1 : r + 1 + n, :] * after
        below, above = k + 8, k + 2
    if k > 0:
        summed += side[below, r : r + n, :] * u[o + k, r : r + n, :]
    if k < 5:
        summed += side[above, r : r + n, :] * u[o + k + 2, r : r + n, :]
    return summed


def smooth_pair(u, rhs, coef, face, side, low, high):
    def sweep(_, carry):
        for colour in (0, 1):
            for k in range(6):
                for r, n in spans(low, high, LANES):
                    new = rhs[6 * colour + k, r : r + n, :]
                    new = new + beside_pair(u, face, side, colour, k, r, n)
                    new = new * coef[12 + 6 * colour + k, r : r + n, :]
                    u[8 * colour + k + 1, r : r + n, :] = new
        return carry

    lax.fori_loop(0, 2, sweep, 0)


def residual_pair(u, rhs, coef, face, side, temp, low, high):
    for k in range(6):
        for r, n in spans(low, high, LANES):
            left = rhs[k, r : r + n, :] + beside_pair(u, face, side, 0, k, r, n)
            temp[k, r : r + n, :] = left - coef[24 + k, r : r + n, :] * u[k + 1, r : r + n, :]


def greet(waiting):
    barrier = pltpu.get_barrier_semaphore()
    gx, gy = lax.axis_index("gx"), lax.axis_index("gy")
    nx, ny = lax.axis_size("gx"), lax.axis_size("gy")
    if waiting:
        across = jnp.where(gx > 0, 1, 0) + jnp.where(gx < nx - 1, 1, 0)
        along = jnp.where(gy > 0, 1, 0) + jnp.where(gy < ny - 1, 1, 0)
        pl.semaphore_wait(barrier, nx + ny - 2 + across * along)
        return
    for step in range(1, nx):
        other = (lax.rem(gx + step, nx), gy)
        pl.semaphore_signal(barrier, inc=1, device_id=other, device_id_type=MESH)
    for step in range(1, ny):
        other = (gx, lax.rem(gy + step, ny))
        pl.semaphore_signal(barrier, inc=1, device_id=other, device_id_type=MESH)
    for dx, dy in SIDES[4:]:

        @pl.when(near(dx, dy))
        def _(dx=dx, dy=dy):
            other = (gx + dx, gy + dy)
            pl.semaphore_signal(barrier, inc=1, device_id=other, device_id_type=MESH)


def gather_copies(whole, sems, phase):
    nx, ny = lax.axis_size("gx"), lax.axis_size("gy")
    gx, gy = lax.axis_index("gx"), lax.axis_index("gy")
    half = nx // 2
    kind, at = lax.rem(gx, 2), gx // 2
    moves = []
    if phase == 0:
        for step in range(1, half):
            target = (2 * lax.rem(at + step, half) + kind, gy)
            origin = lax.rem(at + half - step, half)
            moves.append((target, whole.at[kind, gy, at], whole.at[kind, gy, origin]))
    elif phase == 1:
        for step in range(1, ny):
            target = (gx, lax.rem(gy + step, ny))
            origin = lax.rem(gy + ny - step, ny)
            moves.append((target, whole.at[kind, gy], whole.at[kind, origin]))
    else:
        moves.append(((gx + 1 - 2 * kind, gy), whole.at[kind], whole.at[1 - kind]))
    made = []
    for i, (target, source, arriving) in enumerate(moves):
        both = []
        for ref in (source, arriving):
            both.append(
                pltpu.make_async_remote_copy(
                    src_ref=ref, dst_ref=ref, send_sem=sems[2 * phase].at[i],
                    recv_sem=sems[2 * phase + 1].at[i], device_id=target, device_id_type=MESH,
                )
            )
        made.append(both)
    return made


def begin(made):
    for out, _ in made:
        out.start()


def end(made):
    for out, into in made:
        out.wait_send()
        into.wait_recv()


def squeeze(planes):
    rows = 6 * LANES
    r = lax.broadcasted_iota(jnp.int32, (rows, LANES), 0)
    c = lax.broadcasted_iota(jnp.int32, (rows, LANES), 1)
    at = (c // 16) * LANES + LEFT + 4 * (c % 16)
    return split_dot(jnp.concatenate(planes, axis=1), chosen(r == at))


def place(whole, targets, h):
    _, ny, half = whole.shape[:3]
    wide = min(ny, LANES // 16)

    def body(at, carry):
        lane = lane_of((h, LANES)) // 16
        for kind in (0, 1):
            row = pl.multiple_of(8 + (2 * at + kind) * h, 8)
            for t, (ref, first) in enumerate(targets):
                for k in range(6):
                    for start in range(0, ny, wide):
                        total = jnp.zeros((h, LANES), F32)
                        for gy in range(start, min(start + wide, ny)):
                            x = whole[kind, gy, at, t * h : (t + 1) * h, :]
                            x = pltpu.roll(x, (16 * (gy - start - k)) % LANES, 1)
                            total = jnp.where(lane == gy - start, x, total)
                        ref[first + k, pl.ds(row, h), start * 16 : start * 16 + LANES] = total
        return carry

    lax.fori_loop(0, half, body, 0)


def conjugate(level, residue):
    u, v, rhs, coef, wr, wc, wv, gap = level
    n = u.shape[1] - 16
    mid = slice(8, 8 + n)

    def summed(x):
        total = (x[0] + x[1]) + (x[2] + x[3]) + (x[4] + x[5])
        return jnp.sum(jnp.sum(total, axis=0, keepdims=True), axis=1, keepdims=True)

    def turn(r):
        z = [r[k] * coef[6 + k, mid, :] for k in range(6)]
        for k in range(6):
            u[k + 1, mid, :] = z[k]
        w = [
            coef[12 + k, mid, :] * z[k] - beside(u, wr, wc, wv, gap, k, 8, n, z[k])
            for k in range(6)
        ]
        rz = summed([a * b for a, b in zip(r, z)])
        return z, w, rz, summed([a * b for a, b in zip(w, z)])

    r = [rhs[k, mid, :] for k in range(6)]
    z, w, rz, zaz = turn(r)
    for k in range(6):
        residue[k, mid, :] = r[k]
        v[k + 1, mid, :] = z[k]
        coef[k, mid, :] = w[k]
        rhs[k, mid, :] = jnp.zeros_like(r[k])

    def step(_, carry):
        rz, alpha = carry
        r = []
        for k in range(6):
            rhs[k, mid, :] += alpha * v[k + 1, mid, :]
            r.append(residue[k, mid, :] - alpha * coef[k, mid, :])
            residue[k, mid, :] = r[k]
        z, w, rz_new, zaz = turn(r)
        beta = rz_new / rz
        for k in range(6):
            v[k + 1, mid, :] = z[k] + beta * v[k + 1, mid, :]
            coef[k, mid, :] = w[k] + beta * coef[k, mid, :]
        return rz_new, rz_new / (zaz - beta * (rz_new / alpha))

    _, alpha = lax.fori_loop(0, COARSE_ITERS - 1, step, (rz, rz / zaz))
    for k in range(6):
        u[k + 1, mid, :] = rhs[k, mid, :] + alpha * v[k + 1, mid, :]


def exchanges(n0):
    n1, n2 = n0 // 2, n0 // 4
    return {
        "near": Exchange(n0, [(4, 12, False), (4, 13, False)], [(12, n0), (13, n0)]),
        "coef1": Exchange(n1, [(7, 18, False)], [(18, n1)]),
        "coef2": Exchange(n2, [(14, 9, True)], [(18, n2)]),
        "rhs1": Exchange(n1, [(6, 6, False), (2, 24, False)], [(6, n1), (12, n0)]),
        "rhs2": Exchange(n2, [(12, 3, True), (6, 12, False)], [(6, n2), (6, n1)]),
        "u2": Exchange(n2, [(14, 3, True)], [(6, n2)]),
    }


def scratches(n0, nx, ny):
    def planes(n, rows, columns=LANES):
        return pltpu.VMEM((n, rows, columns), F32)

    rows = n0 + 2 * BASE
    shapes = [planes(n, rows) for n in (16, 13, 36, 12, 24, 16, 12)]
    for i in (1, 2):
        r = (n0 >> i) + 2 * BASE
        shapes += [planes(n, r) for n in (8, 8, 6, 18, 6, 6, 7)]
    h = n0 >> LOCAL
    for n in (3 * h, h):
        shapes += [pltpu.VMEM((2, ny, nx // 2, n, LANES), F32)]
    for _ in range(2):
        for n in (nx, nx, ny, ny, 1, 1):
            shapes += [pltpu.SemaphoreType.DMA((n,))]
    columns = up_to(ny * h, LANES)
    for i in range(LEVELS - LOCAL + 1):
        r = ((nx * h) >> i) + 16
        shapes += [planes(n, r, columns) for n in (8, 8, 6, 18, 6, 6, 7)]
    shapes += [planes(6, (nx * h) + 16, columns)]
    return shapes


def whole_kernel(field, labels, patch, lat_t, ver_t, sto_t, wattage, out, *refs):
    n0 = field.shape[1]
    n1, n2, h = n0 // 2, n0 // 4, n0 // 8
    nx, ny = lax.axis_size("gx"), lax.axis_size("gy")
    u0, lab, coef0, rhs0, face, side, lab_own = refs[:7]
    levels = {}
    at = 7
    for i in (1, 2):
        levels[i] = tuple(refs[at : at + 7]) + (i,)
        at += 7
    gathered_coef, gathered_rhs = refs[at : at + 2]
    coef_sems, rhs_sems = refs[at + 2 : at + 8], refs[at + 8 : at + 14]
    at += 14
    for i in range(LOCAL, LEVELS + 1):
        levels[i] = tuple(refs[at : at + 7]) + (1 << (i - LOCAL),)
        at += 7
    temp3 = refs[at]
    rest = refs[at + 1 :]
    ex = exchanges(n0)
    for e in ex.values():
        rest = e.bind(rest)
        e.clear()
    greet(False)
    for ref, planes in ((u0, 16), (coef0, 12), (face, 24)):
        border(ref, planes, BASE - HALO)
    for i, level in levels.items():
        pad = BASE - HALO if i < LOCAL else 8
        for ref, planes in ((level[0], 8), (level[1], 8), (level[3], 6)):
            border(ref, planes, pad)

    r = lax.broadcasted_iota(jnp.int32, (n0, 2 * LANES), 0)
    c = lax.broadcasted_iota(jnp.int32, (n0, 2 * LANES), 1)
    spread = chosen(r == 2 * (c % LANES - LEFT) + c // LANES)
    own = slice(BASE, BASE + n0)

    def part(k, carry):
        even = even_of(n0, k, 0)
        both = split_dot(field[k], spread)
        a, b = both[:, :LANES], both[:, LANES:]
        u0[k + 1, own, :] = jnp.where(even, a, b)
        u0[k + 9, own, :] = jnp.where(even, b, a)
        both = split_dot(labels[k].astype(F32) + F32(1.0), spread, 1)
        inside = (lane_of((n0, LANES)) >= LEFT) & (lane_of((n0, LANES)) < LEFT + 64)
        a, b = both[:, :LANES], both[:, LANES:]
        lab[k, own, :] = jnp.where(inside, jnp.where(even, a, b), 0.0)
        lab[k + 6, own, :] = jnp.where(inside, jnp.where(even, b, a), 0.0)
        return carry

    lax.fori_loop(0, 6, part, 0)
    tiles = patch[...]
    small = jnp.zeros(tiles.shape, F32)
    for m in range(wattage.shape[0]):
        small = jnp.where(tiles == m, wattage[m], small)
    th, tw = tiles.shape
    r = lax.broadcasted_iota(jnp.int32, (tw, LANES), 0)
    c = lax.broadcasted_iota(jnp.int32, (tw, LANES), 1)
    flat = chosen((c >= LEFT) & ((c - LEFT) // (TILE // 2) == r))
    heat = split_dot(small, flat)
    for i in range(th):
        lab[12, BASE + i * TILE : BASE + (i + 1) * TILE, :] = jnp.broadcast_to(
            heat[i : i + 1, :], (TILE, LANES)
        )

    fields = [(u0, 1 + k + 8 * c) for c in (0, 1) for k in range(6)]
    labs = [(lab, i) for i in range(13)]
    edge = ex["near"]
    stage = lab_own

    def restage():
        for c in (0, 1):
            for r in (BASE, BASE + n0 - HALO):
                rows = slice(r, r + HALO)
                stage[6 * c : 6 * c + 6, rows, :] = u0[1 + 8 * c : 7 + 8 * c, rows, :]

    restage()
    greet(True)
    edge.start([[rows_of(*p) for p in fields], [rows_of(*p) for p in labs]], (stage, lab))

    tables = (lat_t, ver_t, sto_t)
    look(lab, coef0, tables, BASE, BASE + n0)
    coef1, coef2 = levels[1][3], levels[2][3]

    def first(i):
        t, k = i // 6, i % 6
        x = pair_rows(coef0, 12 * t + k, BASE, n1) + pair_rows(coef0, 12 * t + 6 + k, BASE, n1)
        coef1[i, BASE : BASE + n1, :] = x * F32(0.25)

    for i in range(18):
        first(i)
    restrict(coef1, coef2, 18, BASE, BASE, n2, 1)
    ex["coef1"].start([[rows_of(coef1, i) for i in range(18)]], (coef1,), False)
    ex["coef2"].start([[twins_of(coef2, i) for i in range(0, 18, 2)]], (coef2,), False)
    gx, gy = lax.axis_index("gx"), lax.axis_index("gy")
    mine = (lax.rem(gx, 2), gy, gx // 2)
    for t in range(3):
        planes = [halve(coef2, 6 * t + k, BASE, h, 2) for k in range(6)]
        gathered_coef[mine + (slice(t * h, (t + 1) * h),)] = squeeze(planes)
    coef_moves = [gather_copies(gathered_coef, coef_sems, phase) for phase in range(3)]
    begin(coef_moves[0])

    edge.finish()
    ex["coef1"].launch()
    ex["coef2"].launch()
    edge.unpack(0, fields, [(edge.tops[0], i) for i in range(12)])
    edge.unpack(1, labs, [(edge.tops[1], i) for i in range(13)])
    lo, hi0, hi1, hi2 = BASE - HALO, BASE + n0 + HALO, BASE + n1 + HALO, BASE + n2 + HALO
    look(lab, coef0, tables, lo, hi0)
    build_pair(coef0, lab, u0, rhs0, face, side, lo, hi0)
    end(coef_moves[0])
    begin(coef_moves[1])
    smooth_pair(u0, rhs0, coef0, face, side, lo, hi0)
    temp = coef0
    residual_pair(u0, rhs0, coef0, face, side, temp, BASE, BASE + n0)
    rhs1, rhs2 = levels[1][2], levels[2][2]

    for k in range(6):
        rhs1[k, BASE : BASE + n1, :] = pair_rows(temp, k, BASE, n1) * F32(0.25)
    restage()
    folded = [folds_of(ref, plane, odd) for ref, plane in fields for odd in (0, 1)]
    ex["rhs1"].start([[rows_of(rhs1, k) for k in range(6)], folded], (rhs1, stage))

    def fill(name, ref, count, first=0):
        e = ex[name]
        e.finish()
        e.unpack(0, [(ref, first + i) for i in range(count)], [(e.tops[0], i) for i in range(count)])

    def weigh(i, low, high):
        coef, wr, wc, wv, gap = levels[i][3:]
        build(coef, wr, wc, wv, 0.25**i, gap, low, high)

    fill("coef1", coef1, 18)
    weigh(1, lo, hi1)
    fill("coef2", coef2, 18)
    weigh(2, lo, hi2)

    fill("rhs1", rhs1, 6)
    smooth(levels[1], lo, hi1, True)
    u1 = levels[1][0]
    residual(levels[1], temp, BASE, BASE + n1)
    restrict(temp, rhs2, 6, BASE, BASE, n2, 1)
    folded = [folds_of(u1, k + 1, odd) for k in range(6) for odd in (0, 1)]
    ex["rhs2"].start([[twins_of(rhs2, k) for k in (0, 2, 4)], folded], (rhs2, u1.at[1:7]))
    end(coef_moves[1])
    begin(coef_moves[2])

    fill("rhs2", rhs2, 6)
    smooth(levels[2], lo, hi2, True)
    u2 = levels[2][0]
    residual(levels[2], temp, BASE, BASE + n2)
    gathered_rhs[mine] = squeeze([halve(temp, k, BASE, h, 2) for k in range(6)])
    rhs_moves = [gather_copies(gathered_rhs, rhs_sems, phase) for phase in range(3)]
    begin(rhs_moves[0])
    ex["u2"].start([[twins_of(u2, k) for k in (1, 3, 5)]], (u2.at[1:7],))
    end(coef_moves[2])
    coef3 = levels[3][3]
    place(gathered_coef, [(coef3, 0), (coef3, 6), (coef3, 12)], h)

    sizes = {i: (nx * h) >> (i - LOCAL) for i in range(LOCAL, LEVELS + 1)}
    for i in range(LOCAL, LEVELS):
        restrict(levels[i][3], levels[i + 1][3], 18, 8, 8, sizes[i + 1], levels[i][-1])
    end(rhs_moves[0])
    begin(rhs_moves[1])
    for i in range(LOCAL, LEVELS + 1):
        weigh(i, 8, 8 + sizes[i])
    e = ex["rhs2"]
    e.unpack_folded(1, [(u1, k + 1) for k in range(6)], [(e.tops[1], k) for k in range(6)])
    e = ex["rhs1"]
    e.unpack_folded(1, fields, [(e.tops[1], i) for i in range(12)])
    end(rhs_moves[1])
    begin(rhs_moves[2])
    fill("u2", u2, 6, 1)
    end(rhs_moves[2])
    place(gathered_rhs, [(levels[3][2], 0)], h)

    for i in range(LOCAL, LEVELS):
        smooth(levels[i], 8, 8 + sizes[i], True)
        residual(levels[i], temp3, 8, 8 + sizes[i])
        restrict(temp3, levels[i + 1][2], 6, 8, 8, sizes[i + 1], levels[i][-1])
    conjugate(levels[LEVELS], temp3)
    for i in reversed(range(LOCAL, LEVELS)):
        prolong(levels[i + 1][0], levels[i][0], 8, sizes[i + 1], 8, levels[i][-1])
        smooth(levels[i], 8, 8 + sizes[i], False)

    u3 = levels[3][0]
    columns = u3.shape[2]
    r = lax.broadcasted_iota(jnp.int32, (columns, LANES), 0)
    c = lax.broadcasted_iota(jnp.int32, (columns, LANES), 1)
    hit = ((c & 1) == 0) & (c // 4 - LEFT // 4 + gy * 16 == r)
    widen = chosen(hit)

    for k in range(6):
        x = u3[k + 1, pl.ds(pl.multiple_of(gx * h, 8), h + 16), :]
        x = split_dot(x, widen)
        u2[k + 1, pl.ds(0, h + 16, 2), :] += x
        u2[k + 1, pl.ds(1, h + 16, 2), :] += x
    smooth(levels[2], lo, hi2, False)
    prolong(u2, u1, lo, n2 + 16, 0, 1)
    smooth(levels[1], lo, hi1, False)

    for k in range(6):
        x = u1[k + 1, lo : lo + n1 + 16, :]
        for c in (0, 8):
            u0[c + k + 1, pl.ds(0, n1 + 16, 2), :] += x
            u0[c + k + 1, pl.ds(1, n1 + 16, 2), :] += x
    smooth_pair(u0, rhs0, coef0, face, side, lo, hi0)

    r = lax.broadcasted_iota(jnp.int32, (2 * LANES, n0), 0)
    c = lax.broadcasted_iota(jnp.int32, (2 * LANES, n0), 1)
    join = chosen(c == 2 * (r % LANES - LEFT) + r // LANES)

    def give(k, carry):
        even = even_of(n0, k, 0)
        red, black = u0[k + 1, own, :], u0[k + 9, own, :]
        both = jnp.concatenate(
            [jnp.where(even, red, black), jnp.where(even, black, red)], axis=1
        )
        out[k] = split_dot(both, join)
        return carry

    lax.fori_loop(0, 6, give, 0)


def on_device(field, substance, patch, planar, vertical, storage, wattage):
    n0 = field.shape[1]
    nx, ny = lax.axis_size("gx"), lax.axis_size("gy")
    vmem = pl.BlockSpec(memory_space=pltpu.VMEM)
    smem = pl.BlockSpec(memory_space=pltpu.SMEM)
    scratch = scratches(n0, nx, ny)
    for e in exchanges(n0).values():
        scratch += e.scratch()
    return pl.pallas_call(
        whole_kernel,
        out_shape=jax.ShapeDtypeStruct(field.shape, F32),
        in_specs=[vmem] * 3 + [smem] * 4,
        out_specs=vmem,
        scratch_shapes=scratch,
        compiler_params=pltpu.CompilerParams(vmem_limit_bytes=VM, has_side_effects=True, collective_id=0),
    )(field, substance, patch, planar, vertical, storage, wattage)


def solution(mesh):
    placed = (P(None, "gx", "gy"), P(None, "gx", "gy"), P("gx", "gy"), P(), P(), P(), P())
    return jax.shard_map(
        on_device, mesh=mesh, in_specs=placed, out_specs=P(None, "gx", "gy"), check_vma=False
    )
```

```python
import functools

import jax
import jax.numpy as jnp
from jax import lax
from jax.experimental import pallas as pl
from jax.experimental.pallas import tpu as pltpu
from jax.sharding import PartitionSpec as P

TILE = 16
LEVELS = 6
COARSE_ITERS = 12
LOCAL = 3
HALO = 8
BASE = 16
LEFT = 16
LANES = 128
F32 = jnp.float32
VM = 63 * 1024 * 1024
MESH = pl.DeviceIdType.MESH
SIDES = ((-1, 0), (1, 0), (0, -1), (0, 1), (-1, -1), (-1, 1), (1, -1), (1, 1))


def up_to(count, step):
    return -(-count // step) * step


def spans(low, high, columns):
    step = max(8, 48 * LANES // columns // 8 * 8)
    return [(r, min(step, high - r)) for r in range(low, high, step)]


def lane_of(shape):
    return lax.broadcasted_iota(jnp.int32, shape, len(shape) - 1)


def row_of(shape):
    return lax.broadcasted_iota(jnp.int32, shape, 0)


def split_dot(values, matrix, terms=3):
    total = None
    pieces = []
    for _ in range(terms):
        piece = values.astype(jnp.bfloat16)
        values = values - piece.astype(F32)
        pieces.append(piece)
    for piece in reversed(pieces):
        part = jnp.dot(piece, matrix, preferred_element_type=F32)
        total = part if total is None else total + part
    return total


def chosen(hit):
    return jnp.where(hit, F32(1.0), F32(0.0)).astype(jnp.bfloat16)


def near(dx, dy):
    ok = None
    for axis, step in (("gx", dx), ("gy", dy)):
        if step == 0:
            continue
        at = lax.axis_index(axis)
        this = (at + step < lax.axis_size(axis)) if step > 0 else (at + step >= 0)
        ok = this if ok is None else jnp.logical_and(ok, this)
    return ok


class Exchange:
    def __init__(self, rows, groups, row_refs):
        self.rows, self.row_refs = rows, row_refs
        self.twin = [g[2] for g in groups]
        self.slots, pack, lane = [], 0, 0
        for width, count, _ in groups:
            group = []
            for _ in range(count):
                if lane + width > LANES:
                    pack, lane = pack + 1, 0
                group.append((pack, lane, width))
                lane += width
            self.slots.append(group)
        self.packs = pack + 1

    def scratch(self):
        packed = pltpu.VMEM((2, self.packs, self.rows, LANES), F32)
        landed = pltpu.VMEM((2, self.packs, self.rows + 2 * HALO, LANES), F32)
        tops = [pltpu.VMEM((2, n, HALO, LANES), F32) for n, _ in self.row_refs]
        sems = pltpu.SemaphoreType.DMA((6 + 2 * len(self.row_refs),))
        return [packed, landed, sems, sems] + tops

    def bind(self, refs):
        self.packed, self.landed, self.send, self.recv = refs[:4]
        self.tops = refs[4 : 4 + len(self.row_refs)]
        return refs[4 + len(self.row_refs) :]

    def clear(self):
        self.landed[...] = jnp.zeros_like(self.landed)
        for top in self.tops:
            top[...] = jnp.zeros_like(top)

    def copies(self):
        n = self.rows
        gx, gy = lax.axis_index("gx"), lax.axis_index("gy")
        out = []
        for dy, side in ((1, 0), (-1, 1)):
            packed = self.packed.at[side]
            landed = self.landed.at[side]
            out.append((0, dy, packed, landed.at[:, HALO : HALO + n, :]))
            out.append((1, dy, packed.at[:, n - HALO : n, :], landed.at[:, 0:HALO, :]))
            out.append(
                (-1, dy, packed.at[:, 0:HALO, :], landed.at[:, HALO + n : n + 2 * HALO, :])
            )
        for source, top, (_, m) in zip(self.sources, self.tops, self.row_refs):
            out.append((1, 0, source.at[:, BASE + m - HALO : BASE + m, :], top.at[0]))
            out.append((-1, 0, source.at[:, BASE : BASE + HALO, :], top.at[1]))
        made = []
        for i, (dx, dy, source, target) in enumerate(out):
            copy = pltpu.make_async_remote_copy(
                src_ref=source,
                dst_ref=target,
                send_sem=self.send.at[i],
                recv_sem=self.recv.at[i],
                device_id=(gx + dx, gy + dy),
                device_id_type=MESH,
            )
            made.append((dx, dy, copy))
        return made

    def start(self, groups, sources, now=True):
        slots = [x for group in self.slots for x in group]
        takes = [x for group in groups for x in group]
        for r, m in spans(0, self.rows, LANES):
            lane = lane_of((m, LANES))
            packs = [[jnp.zeros((m, LANES), F32)] * 2 for _ in range(self.packs)]
            for (pack, at, w), take in zip(slots, takes):
                x = take(r, m)
                hit = (lane >= at) & (lane < at + w)
                a = pltpu.roll(x, (at - (LEFT + 64 - w)) % LANES, 1)
                b = pltpu.roll(x, (at - LEFT) % LANES, 1)
                right, left = packs[pack]
                packs[pack] = [jnp.where(hit, a, right), jnp.where(hit, b, left)]
            for pack, both in enumerate(packs):
                for side in (0, 1):
                    self.packed[side, pack, r : r + m, :] = both[side]
        self.sources = sources
        if now:
            self.launch()

    def launch(self):
        for dx, dy, copy in self.copies():
            pl.when(near(dx, dy))(copy.start)

    def finish(self):
        for dx, dy, copy in self.copies():
            pl.when(near(dx, dy))(copy.wait_send)
            pl.when(near(-dx, -dy))(copy.wait_recv)

    def merge(self, x, slot, r, m, shift=None):
        pack, at, w = slot
        lane = lane_of((m, LANES))
        inside = (lane >= LEFT - w) & (lane < LEFT)
        beyond = (lane >= LEFT + 64) & (lane < LEFT + 64 + w)
        if shift is not None:
            inside, beyond = inside & (lane % 2 == 0), beyond & (lane % 2 == 0)
        back = shift or 0
        a = pltpu.roll(self.landed[0, pack, r : r + m, :], (LEFT - w - at - back) % LANES, 1)
        b = pltpu.roll(self.landed[1, pack, r : r + m, :], (LEFT + 64 - at - back) % LANES, 1)
        return jnp.where(beyond, b, jnp.where(inside, a, x))

    def unpack(self, group, planes, tops):
        n = self.rows
        for i, (ref, plane) in enumerate(planes):
            twin = self.twin[group]
            slot = self.slots[group][i // 2 if twin else i]
            pieces = [(0, HALO, 0)]
            pieces += [(HALO + r, m, None) for r, m in spans(0, n, LANES)]
            pieces += [(HALO + n, HALO, 1)]
            for r, m, side in pieces:
                rows = slice(BASE - HALO + r, BASE - HALO + r + m)
                if side is None:
                    x = ref[plane, rows]
                else:
                    x = tops[i][0][side, tops[i][1]]
                ref[plane, rows] = self.merge(x, slot, r, m, i % 2 if twin else None)

    def unpack_folded(self, group, planes, tops):
        n = self.rows
        for i, (ref, plane) in enumerate(planes):
            top, at = tops[i]
            ref[plane, BASE - HALO : BASE] = top[0, at]
            ref[plane, BASE + 2 * n : BASE + 2 * n + HALO] = top[1, at]
            for odd in (0, 1):
                for r, m in spans(HALO // 2, n + HALO + HALO // 2, LANES):
                    rows = pl.ds(BASE + 2 * (r - HALO) + odd, m, 2)
                    slot = self.slots[group][2 * i + odd]
                    ref[plane, rows, :] = self.merge(ref[plane, rows, :], slot, r, m)


def rows_of(ref, plane):
    return lambda r, m: ref[plane, BASE + r : BASE + r + m, :]


def twins_of(ref, plane):
    def take(r, m):
        a, b = ref[plane, BASE + r : BASE + r + m, :], ref[plane + 1, BASE + r : BASE + r + m, :]
        return jnp.where(lane_of(a.shape) % 2 == 0, a, pltpu.roll(b, 1, 1))

    return take


def folds_of(ref, plane, odd):
    return lambda r, m: ref[plane, pl.ds(BASE + odd + 2 * r, m, 2), :]


def build(coef, wr, wc, wv, scale, gap, low, high):
    columns = coef.shape[2]
    half = F32(0.5 * scale)
    wv[6] = jnp.zeros(wv.shape[1:], F32)
    for k in range(6):
        for r, n in spans(low, high, columns):
            lane = lane_of((n, columns))
            here = coef[k, r : r + n, :]
            wr[k, r : r + n, :] = half * (here + coef[k, r - 1 : r - 1 + n, :])
            before = jnp.where(lane < gap, 0.0, pltpu.roll(here, gap, 1))
            wc[k, r : r + n, :] = jnp.where(lane < gap, 0.0, half * (here + before))
        here = coef[k, high : high + 8, :]
        wr[k, high : high + 8, :] = half * (here + coef[k, high - 1 : high + 7, :])
        for r, n in spans(low, high, columns):
            if k:
                inside = coef[6 + k, r : r + n, :] + coef[5 + k, r : r + n, :]
                wv[k, r : r + n, :] = F32(0.5) * inside
            else:
                wv[k, r : r + n, :] = jnp.zeros((n, columns), F32)
    for k in range(6):
        for r, n in spans(low, high, columns):
            lane = lane_of((n, columns))
            here = coef[k, r : r + n, :]
            before = jnp.where(lane < gap, 0.0, pltpu.roll(here, gap, 1))
            after = jnp.where(lane >= columns - gap, 0.0, pltpu.roll(here, columns - gap, 1))
            s = coef[12 + k, r : r + n, :]
            d = s + wr[k, r : r + n, :] + wr[k, r + 1 : r + 1 + n, :]
            d = d + half * (here + before) + half * (here + after)
            d = d + wv[k, r : r + n, :] + wv[k + 1, r : r + n, :]
            coef[12 + k, r : r + n, :] = d
            coef[6 + k, r : r + n, :] = jnp.where(
                s > 0.0, F32(1.0) / jnp.where(s > 0.0, d, 1.0), 0.0
            )


def beside(u, wr, wc, wv, gap, k, r, n, here):
    columns = u.shape[2]
    left = wc[k, r : r + n, :]
    summed = left * pltpu.roll(here, gap, 1)
    summed += pltpu.roll(left * here, columns - gap, 1)
    summed += wr[k, r : r + n, :] * u[k + 1, r - 1 : r - 1 + n, :]
    summed += wr[k, r + 1 : r + 1 + n, :] * u[k + 1, r + 1 : r + 1 + n, :]
    if k > 0:
        summed += wv[k, r : r + n, :] * u[k, r : r + n, :]
    if k < 5:
        summed += wv[k + 1, r : r + n, :] * u[k + 2, r : r + n, :]
    return summed


def coloured(n, columns, gap, k, colour):
    shape = (n, columns)
    return ((row_of(shape) + lane_of(shape) // gap + k + colour) & 1) == 0


def half_sweep(level, source, target, colour, low, high):
    rhs, coef, wr, wc, wv, gap = level[2:]
    columns = source.shape[2]
    for k in range(6):
        for r, n in spans(low, high, columns):
            here = source[k + 1, r : r + n, :]
            new = rhs[k, r : r + n, :] + beside(source, wr, wc, wv, gap, k, r, n, here)
            new = new * coef[6 + k, r : r + n, :]
            mask = coloured(n, columns, gap, k, colour)
            target[k + 1, r : r + n, :] = jnp.where(mask, new, here)


def smooth(level, low, high, fresh):
    u, v, rhs, coef, wr, wc, wv, gap = level
    columns = u.shape[2]
    if fresh:
        for k in range(6):
            for r, n in spans(low, high, columns):
                new = rhs[k, r : r + n, :] * coef[6 + k, r : r + n, :]
                v[k + 1, r : r + n, :] = jnp.where(coloured(n, columns, gap, k, 0), new, 0.0)
        half_sweep(level, v, u, 1, low, high)
        half_sweep(level, u, v, 0, low, high)
        half_sweep(level, v, u, 1, low, high)
        return

    def sweep(_, carry):
        half_sweep(level, u, v, 0, low, high)
        half_sweep(level, v, u, 1, low, high)
        return carry

    lax.fori_loop(0, 2, sweep, 0)


def residual(level, temp, low, high):
    u, _, rhs, coef, wr, wc, wv, gap = level
    columns = u.shape[2]
    for k in range(6):
        for r, n in spans(low, high, columns):
            here = u[k + 1, r : r + n, :]
            left = rhs[k, r : r + n, :] + beside(u, wr, wc, wv, gap, k, r, n, here)
            left = left - coef[12 + k, r : r + n, :] * here
            temp[k, r : r + n, :] = jnp.where(coloured(n, columns, gap, k, 0), left, 0.0)


def left_dot(matrix, values):
    a = values.astype(jnp.bfloat16)
    values = values - a.astype(F32)
    b = values.astype(jnp.bfloat16)
    c = (values - b.astype(F32)).astype(jnp.bfloat16)
    dot = functools.partial(jnp.dot, preferred_element_type=F32)
    return (dot(matrix, c) + dot(matrix, b)) + dot(matrix, a)


def pair_rows(ref, i, start, count):
    if ref.shape[2] > LANES:
        shape = (count, 2 * count)
        pick = chosen(lane_of(shape) // 2 == row_of(shape))
        return left_dot(pick, ref[i, start : start + 2 * count, :])
    return ref[i, pl.ds(start, count, 2), :] + ref[i, pl.ds(start + 1, count, 2), :]


def halve(ref, i, start, count, gap):
    x = pair_rows(ref, i, start, count)
    x = (x + pltpu.roll(x, x.shape[1] - gap, 1)) * F32(0.25)
    return jnp.where(lane_of(x.shape) % (2 * gap) == 0, x, 0.0)


def restrict(fine, coarse, planes, low_fine, low_coarse, count, gap):
    def body(i, carry):
        coarse[i, low_coarse : low_coarse + count, :] = halve(fine, i, low_fine, count, gap)
        return carry

    if fine.shape[2] > LANES:
        lax.fori_loop(0, planes, body, 0)
    else:
        for i in range(planes):
            body(i, 0)


def prolong(coarse, fine, low, count, to, gap):
    def body(k, carry):
        x = coarse[k + 1, low : low + count, :]
        x = x + pltpu.roll(x, gap, 1)
        if x.shape[1] > LANES:
            shape = (2 * count, count)
            twice = left_dot(chosen(row_of(shape) // 2 == lane_of(shape)), x)
            fine[k + 1, to : to + 2 * count, :] += twice
            return carry
        fine[k + 1, pl.ds(to, count, 2), :] += x
        fine[k + 1, pl.ds(to + 1, count, 2), :] += x
        return carry

    for k in range(6):
        body(k, 0)


def border(ref, planes, pad):
    rows = ref.shape[1]
    for start in (0, rows - pad):
        ref[0:planes, start : start + pad, :] = jnp.zeros((planes, pad, ref.shape[2]), F32)


def turned(x, even):
    return jnp.where(even, pltpu.roll(x, 1, 1), pltpu.roll(x, LANES - 1, 1))


def even_of(n, k, colour):
    return ((row_of((n, LANES)) + k + colour) & 1) == 0


def look(lab, coef, tables, low, high):
    def body(i, carry):
        for r, n in spans(low, high, LANES):
            labels = lab[i, r : r + n, :]
            found = [jnp.zeros((n, LANES), F32)] * 3
            for m in range(tables[0].shape[0]):
                hit = labels == F32(m + 1)
                found = [jnp.where(hit, t[m], x) for t, x in zip(tables, found)]
            for t in range(3):
                coef[12 * t + i, r : r + n, :] = found[t]
        return carry

    lax.fori_loop(0, 12, body, 0)


def build_pair(coef, lab, u, rhs, face, side, low, high):
    half = F32(0.5)
    for k in range(6):
        for r, n in spans(low, high, LANES):
            here = coef[k, r : r + n, :]
            other = coef[6 + k, r : r + n, :]
            face[k, r : r + n, :] = half * (here + coef[6 + k, r - 1 : r - 1 + n, :])
            face[6 + k, r : r + n, :] = half * (here + coef[6 + k, r + 1 : r + 1 + n, :])
            face[12 + k, r : r + n, :] = half * (here + other)
            face[18 + k, r : r + n, :] = half * (here + turned(other, even_of(n, k, 0)))
            v = coef[12 + k, r : r + n, :]
            if k > 0:
                side[k + 1, r : r + n, :] = half * (v + coef[17 + k, r : r + n, :])
            if k < 5:
                side[9 + k, r : r + n, :] = half * (v + coef[19 + k, r : r + n, :])
    for k in range(6):
        for r, n in spans(low, high, LANES):
            for colour in (0, 1):
                s = coef[24 + 6 * colour + k, r : r + n, :]
                if colour == 0:
                    d = s + face[k, r : r + n, :] + face[6 + k, r : r + n, :]
                    d = d + face[12 + k, r : r + n, :] + face[18 + k, r : r + n, :]
                    below, above = side[k + 1, r : r + n, :], side[9 + k, r : r + n, :]
                else:
                    d = s + face[6 + k, r - 1 : r - 1 + n, :] + face[k, r + 1 : r + 1 + n, :]
                    d = d + face[12 + k, r : r + n, :]
                    d = d + turned(face[18 + k, r : r + n, :], even_of(n, k, 1))
                    below, above = side[8 + k, r : r + n, :], side[k + 2, r : r + n, :]
                if k > 0:
                    d = d + below
                if k < 5:
                    d = d + above
                source = s * u[8 * colour + k + 1, r : r + n, :]
                if k == 0:
                    source = source + lab[12, r : r + n, :]
                rhs[6 * colour + k, r : r + n, :] = source
                coef[24 + 6 * colour + k, r : r + n, :] = d
                coef[12 + 6 * colour + k, r : r + n, :] = jnp.where(
                    s > 0.0, F32(1.0) / jnp.where(s > 0.0, d, 1.0), 0.0
                )


def beside_pair(u, face, side, colour, k, r, n):
    o = 8 * (1 - colour)
    same = u[o + k + 1, r : r + n, :]
    before = u[o + k + 1, r - 1 : r - 1 + n, :]
    after = u[o + k + 1, r + 1 : r + 1 + n, :]
    even = even_of(n, k, colour)
    if colour == 0:
        summed = face[18 + k, r : r + n, :] * turned(same, even)
        summed += face[12 + k, r : r + n, :] * same
        summed += face[k, r : r + n, :] * before + face[6 + k, r : r + n, :] * after
        below, above = k + 1, k + 9
    else:
        summed = turned(face[18 + k, r : r + n, :] * same, even)
        summed += face[12 + k, r : r + n, :] * same
        summed += face[6 + k, r - 1 : r - 1 + n, :] * before
        summed += face[k, r + 1 : r + 1 + n, :] * after
        below, above = k + 8, k + 2
    if k > 0:
        summed += side[below, r : r + n, :] * u[o + k, r : r + n, :]
    if k < 5:
        summed += side[above, r : r + n, :] * u[o + k + 2, r : r + n, :]
    return summed


def smooth_pair(u, rhs, coef, face, side, low, high):
    def sweep(_, carry):
        for colour in (0, 1):
            for k in range(6):
                for r, n in spans(low, high, LANES):
                    new = rhs[6 * colour + k, r : r + n, :]
                    new = new + beside_pair(u, face, side, colour, k, r, n)
                    new = new * coef[12 + 6 * colour + k, r : r + n, :]
                    u[8 * colour + k + 1, r : r + n, :] = new
        return carry

    lax.fori_loop(0, 2, sweep, 0)


def residual_pair(u, rhs, coef, face, side, temp, low, high):
    for k in range(6):
        for r, n in spans(low, high, LANES):
            left = rhs[k, r : r + n, :] + beside_pair(u, face, side, 0, k, r, n)
            temp[k, r : r + n, :] = left - coef[24 + k, r : r + n, :] * u[k + 1, r : r + n, :]


def greet(waiting):
    barrier = pltpu.get_barrier_semaphore()
    gx, gy = lax.axis_index("gx"), lax.axis_index("gy")
    nx, ny = lax.axis_size("gx"), lax.axis_size("gy")
    if waiting:
        across = jnp.where(gx > 0, 1, 0) + jnp.where(gx < nx - 1, 1, 0)
        along = jnp.where(gy > 0, 1, 0) + jnp.where(gy < ny - 1, 1, 0)
        pl.semaphore_wait(barrier, nx + ny - 2 + across * along)
        return
    for step in range(1, nx):
        other = (lax.rem(gx + step, nx), gy)
        pl.semaphore_signal(barrier, inc=1, device_id=other, device_id_type=MESH)
    for step in range(1, ny):
        other = (gx, lax.rem(gy + step, ny))
        pl.semaphore_signal(barrier, inc=1, device_id=other, device_id_type=MESH)
    for dx, dy in SIDES[4:]:

        @pl.when(near(dx, dy))
        def _(dx=dx, dy=dy):
            other = (gx + dx, gy + dy)
            pl.semaphore_signal(barrier, inc=1, device_id=other, device_id_type=MESH)


def gather_copies(whole, sems, phase):
    nx, ny = lax.axis_size("gx"), lax.axis_size("gy")
    gx, gy = lax.axis_index("gx"), lax.axis_index("gy")
    half = nx // 2
    kind, at = lax.rem(gx, 2), gx // 2
    moves = []
    if phase == 0:
        for step in range(1, half):
            target = (2 * lax.rem(at + step, half) + kind, gy)
            origin = lax.rem(at + half - step, half)
            moves.append((target, whole.at[kind, gy, at], whole.at[kind, gy, origin]))
    elif phase == 1:
        for step in range(1, ny):
            target = (gx, lax.rem(gy + step, ny))
            origin = lax.rem(gy + ny - step, ny)
            moves.append((target, whole.at[kind, gy], whole.at[kind, origin]))
    else:
        moves.append(((gx + 1 - 2 * kind, gy), whole.at[kind], whole.at[1 - kind]))
    made = []
    for i, (target, source, arriving) in enumerate(moves):
        both = []
        for ref in (source, arriving):
            both.append(
                pltpu.make_async_remote_copy(
                    src_ref=ref, dst_ref=ref, send_sem=sems[2 * phase].at[i],
                    recv_sem=sems[2 * phase + 1].at[i], device_id=target, device_id_type=MESH,
                )
            )
        made.append(both)
    return made


def begin(made):
    for out, _ in made:
        out.start()


def end(made):
    for out, into in made:
        out.wait_send()
        into.wait_recv()


def squeeze(planes):
    rows = 6 * LANES
    r = lax.broadcasted_iota(jnp.int32, (rows, LANES), 0)
    c = lax.broadcasted_iota(jnp.int32, (rows, LANES), 1)
    at = (c // 16) * LANES + LEFT + 4 * (c % 16)
    return split_dot(jnp.concatenate(planes, axis=1), chosen(r == at))


def place(whole, targets, h):
    _, ny, half = whole.shape[:3]
    wide = min(ny, LANES // 16)

    def body(at, carry):
        lane = lane_of((h, LANES)) // 16
        for kind in (0, 1):
            row = pl.multiple_of(8 + (2 * at + kind) * h, 8)
            for t, (ref, first) in enumerate(targets):
                for k in range(6):
                    for start in range(0, ny, wide):
                        total = jnp.zeros((h, LANES), F32)
                        for gy in range(start, min(start + wide, ny)):
                            x = whole[kind, gy, at, t * h : (t + 1) * h, :]
                            x = pltpu.roll(x, (16 * (gy - start - k)) % LANES, 1)
                            total = jnp.where(lane == gy - start, x, total)
                        ref[first + k, pl.ds(row, h), start * 16 : start * 16 + LANES] = total
        return carry

    lax.fori_loop(0, half, body, 0)


def conjugate(level, residue):
    u, v, rhs, coef, wr, wc, wv, gap = level
    n = u.shape[1] - 16
    mid = slice(8, 8 + n)

    def dot(x, y):
        x = [a * b for a, b in zip(x, y)]
        total = (x[0] + x[1]) + (x[2] + x[3]) + (x[4] + x[5])
        return jnp.sum(jnp.sum(total, axis=0, keepdims=True), axis=1, keepdims=True)

    def turn(r):
        z = [r[k] * coef[6 + k, mid, :] for k in range(6)]
        for k in range(6):
            u[k + 1, mid, :] = z[k]
        w = [
            coef[12 + k, mid, :] * z[k] - beside(u, wr, wc, wv, gap, k, 8, n, z[k])
            for k in range(6)
        ]
        return z, w, dot(r, z)

    r = [rhs[k, mid, :] for k in range(6)]
    z, w, rz = turn(r)
    for k in range(6):
        residue[k, mid, :] = r[k]
        v[k + 1, mid, :] = z[k]
        coef[k, mid, :] = w[k]
        rhs[k, mid, :] = jnp.zeros_like(r[k])

    def step(_, carry):
        rz, alpha = carry
        r = []
        for k in range(6):
            rhs[k, mid, :] += alpha * v[k + 1, mid, :]
            r.append(residue[k, mid, :] - alpha * coef[k, mid, :])
            residue[k, mid, :] = r[k]
        z, w, rz_new = turn(r)
        beta = rz_new / rz
        p = [z[k] + beta * v[k + 1, mid, :] for k in range(6)]
        q = [w[k] + beta * coef[k, mid, :] for k in range(6)]
        for k in range(6):
            v[k + 1, mid, :] = p[k]
            coef[k, mid, :] = q[k]
        return rz_new, rz_new / dot(p, q)

    _, alpha = lax.fori_loop(0, COARSE_ITERS - 1, step, (rz, rz / dot(z, w)))
    for k in range(6):
        u[k + 1, mid, :] = rhs[k, mid, :] + alpha * v[k + 1, mid, :]


def exchanges(n0):
    n1, n2 = n0 // 2, n0 // 4
    return {
        "near": Exchange(n0, [(4, 12, False), (4, 13, False)], [(12, n0), (13, n0)]),
        "coef1": Exchange(n1, [(7, 18, False)], [(18, n1)]),
        "coef2": Exchange(n2, [(14, 9, True)], [(18, n2)]),
        "rhs1": Exchange(n1, [(6, 6, False), (2, 24, False)], [(6, n1), (12, n0)]),
        "rhs2": Exchange(n2, [(12, 3, True), (6, 12, False)], [(6, n2), (6, n1)]),
        "u2": Exchange(n2, [(14, 3, True)], [(6, n2)]),
    }


def scratches(n0, nx, ny):
    def planes(n, rows, columns=LANES):
        return pltpu.VMEM((n, rows, columns), F32)

    rows = n0 + 2 * BASE
    shapes = [planes(n, rows) for n in (16, 13, 36, 12, 24, 16, 12)]
    for i in (1, 2):
        r = (n0 >> i) + 2 * BASE
        shapes += [planes(n, r) for n in (8, 8, 6, 18, 6, 6, 7)]
    h = n0 >> LOCAL
    for n in (3 * h, h):
        shapes += [pltpu.VMEM((2, ny, nx // 2, n, LANES), F32)]
    for _ in range(2):
        for n in (nx, nx, ny, ny, 1, 1):
            shapes += [pltpu.SemaphoreType.DMA((n,))]
    columns = up_to(ny * h, LANES)
    for i in range(LEVELS - LOCAL + 1):
        r = ((nx * h) >> i) + 16
        shapes += [planes(n, r, columns) for n in (8, 8, 6, 18, 6, 6, 7)]
    shapes += [planes(6, (nx * h) + 16, columns)]
    return shapes


def whole_kernel(field, labels, patch, lat_t, ver_t, sto_t, wattage, out, *refs):
    n0 = field.shape[1]
    n1, n2, h = n0 // 2, n0 // 4, n0 // 8
    nx, ny = lax.axis_size("gx"), lax.axis_size("gy")
    u0, lab, coef0, rhs0, face, side, lab_own = refs[:7]
    levels = {}
    at = 7
    for i in (1, 2):
        levels[i] = tuple(refs[at : at + 7]) + (i,)
        at += 7
    gathered_coef, gathered_rhs = refs[at : at + 2]
    coef_sems, rhs_sems = refs[at + 2 : at + 8], refs[at + 8 : at + 14]
    at += 14
    for i in range(LOCAL, LEVELS + 1):
        levels[i] = tuple(refs[at : at + 7]) + (1 << (i - LOCAL),)
        at += 7
    temp3 = refs[at]
    rest = refs[at + 1 :]
    ex = exchanges(n0)
    for e in ex.values():
        rest = e.bind(rest)
        e.clear()
    greet(False)
    for ref, planes in ((u0, 16), (coef0, 12), (face, 24)):
        border(ref, planes, BASE - HALO)
    for i, level in levels.items():
        pad = BASE - HALO if i < LOCAL else 8
        for ref, planes in ((level[0], 8), (level[1], 8), (level[3], 6)):
            border(ref, planes, pad)

    r = lax.broadcasted_iota(jnp.int32, (n0, 2 * LANES), 0)
    c = lax.broadcasted_iota(jnp.int32, (n0, 2 * LANES), 1)
    spread = chosen(r == 2 * (c % LANES - LEFT) + c // LANES)
    own = slice(BASE, BASE + n0)

    def part(k, carry):
        even = even_of(n0, k, 0)
        both = split_dot(field[k], spread)
        a, b = both[:, :LANES], both[:, LANES:]
        u0[k + 1, own, :] = jnp.where(even, a, b)
        u0[k + 9, own, :] = jnp.where(even, b, a)
        both = split_dot(labels[k].astype(F32) + F32(1.0), spread, 1)
        inside = (lane_of((n0, LANES)) >= LEFT) & (lane_of((n0, LANES)) < LEFT + 64)
        a, b = both[:, :LANES], both[:, LANES:]
        lab[k, own, :] = jnp.where(inside, jnp.where(even, a, b), 0.0)
        lab[k + 6, own, :] = jnp.where(inside, jnp.where(even, b, a), 0.0)
        return carry

    lax.fori_loop(0, 6, part, 0)
    tiles = patch[...]
    small = jnp.zeros(tiles.shape, F32)
    for m in range(wattage.shape[0]):
        small = jnp.where(tiles == m, wattage[m], small)
    th, tw = tiles.shape
    r = lax.broadcasted_iota(jnp.int32, (tw, LANES), 0)
    c = lax.broadcasted_iota(jnp.int32, (tw, LANES), 1)
    flat = chosen((c >= LEFT) & ((c - LEFT) // (TILE // 2) == r))
    heat = split_dot(small, flat)
    for i in range(th):
        lab[12, BASE + i * TILE : BASE + (i + 1) * TILE, :] = jnp.broadcast_to(
            heat[i : i + 1, :], (TILE, LANES)
        )

    fields = [(u0, 1 + k + 8 * c) for c in (0, 1) for k in range(6)]
    labs = [(lab, i) for i in range(13)]
    edge = ex["near"]
    stage = lab_own

    def restage():
        for c in (0, 1):
            for r in (BASE, BASE + n0 - HALO):
                rows = slice(r, r + HALO)
                stage[6 * c : 6 * c + 6, rows, :] = u0[1 + 8 * c : 7 + 8 * c, rows, :]

    restage()
    greet(True)
    edge.start([[rows_of(*p) for p in fields], [rows_of(*p) for p in labs]], (stage, lab))

    tables = (lat_t, ver_t, sto_t)
    look(lab, coef0, tables, BASE, BASE + n0)
    coef1, coef2 = levels[1][3], levels[2][3]

    def first(i):
        t, k = i // 6, i % 6
        x = pair_rows(coef0, 12 * t + k, BASE, n1) + pair_rows(coef0, 12 * t + 6 + k, BASE, n1)
        coef1[i, BASE : BASE + n1, :] = x * F32(0.25)

    for i in range(18):
        first(i)
    restrict(coef1, coef2, 18, BASE, BASE, n2, 1)
    ex["coef1"].start([[rows_of(coef1, i) for i in range(18)]], (coef1,), False)
    ex["coef2"].start([[twins_of(coef2, i) for i in range(0, 18, 2)]], (coef2,), False)
    gx, gy = lax.axis_index("gx"), lax.axis_index("gy")
    mine = (lax.rem(gx, 2), gy, gx // 2)
    for t in range(3):
        planes = [halve(coef2, 6 * t + k, BASE, h, 2) for k in range(6)]
        gathered_coef[mine + (slice(t * h, (t + 1) * h),)] = squeeze(planes)
    coef_moves = [gather_copies(gathered_coef, coef_sems, phase) for phase in range(3)]
    begin(coef_moves[0])

    edge.finish()
    ex["coef1"].launch()
    ex["coef2"].launch()
    edge.unpack(0, fields, [(edge.tops[0], i) for i in range(12)])
    edge.unpack(1, labs, [(edge.tops[1], i) for i in range(13)])
    lo, hi0, hi1, hi2 = BASE - HALO, BASE + n0 + HALO, BASE + n1 + HALO, BASE + n2 + HALO
    look(lab, coef0, tables, lo, hi0)
    build_pair(coef0, lab, u0, rhs0, face, side, lo, hi0)
    end(coef_moves[0])
    begin(coef_moves[1])
    smooth_pair(u0, rhs0, coef0, face, side, lo, hi0)
    temp = coef0
    residual_pair(u0, rhs0, coef0, face, side, temp, BASE, BASE + n0)
    rhs1, rhs2 = levels[1][2], levels[2][2]

    for k in range(6):
        rhs1[k, BASE : BASE + n1, :] = pair_rows(temp, k, BASE, n1) * F32(0.25)
    restage()
    folded = [folds_of(ref, plane, odd) for ref, plane in fields for odd in (0, 1)]
    ex["rhs1"].start([[rows_of(rhs1, k) for k in range(6)], folded], (rhs1, stage))

    def fill(name, ref, count, first=0):
        e = ex[name]
        e.finish()
        e.unpack(0, [(ref, first + i) for i in range(count)], [(e.tops[0], i) for i in range(count)])

    def weigh(i, low, high):
        coef, wr, wc, wv, gap = levels[i][3:]
        build(coef, wr, wc, wv, 0.25**i, gap, low, high)

    fill("coef1", coef1, 18)
    weigh(1, lo, hi1)
    fill("coef2", coef2, 18)
    weigh(2, lo, hi2)

    fill("rhs1", rhs1, 6)
    smooth(levels[1], lo, hi1, True)
    u1 = levels[1][0]
    residual(levels[1], temp, BASE, BASE + n1)
    restrict(temp, rhs2, 6, BASE, BASE, n2, 1)
    folded = [folds_of(u1, k + 1, odd) for k in range(6) for odd in (0, 1)]
    ex["rhs2"].start([[twins_of(rhs2, k) for k in (0, 2, 4)], folded], (rhs2, u1.at[1:7]))
    end(coef_moves[1])
    begin(coef_moves[2])

    fill("rhs2", rhs2, 6)
    smooth(levels[2], lo, hi2, True)
    u2 = levels[2][0]
    residual(levels[2], temp, BASE, BASE + n2)
    gathered_rhs[mine] = squeeze([halve(temp, k, BASE, h, 2) for k in range(6)])
    rhs_moves = [gather_copies(gathered_rhs, rhs_sems, phase) for phase in range(3)]
    begin(rhs_moves[0])
    ex["u2"].start([[twins_of(u2, k) for k in (1, 3, 5)]], (u2.at[1:7],))
    end(coef_moves[2])
    coef3 = levels[3][3]
    place(gathered_coef, [(coef3, 0), (coef3, 6), (coef3, 12)], h)

    sizes = {i: (nx * h) >> (i - LOCAL) for i in range(LOCAL, LEVELS + 1)}
    for i in range(LOCAL, LEVELS):
        restrict(levels[i][3], levels[i + 1][3], 18, 8, 8, sizes[i + 1], levels[i][-1])
    end(rhs_moves[0])
    begin(rhs_moves[1])
    for i in range(LOCAL, LEVELS + 1):
        weigh(i, 8, 8 + sizes[i])
    e = ex["rhs2"]
    e.unpack_folded(1, [(u1, k + 1) for k in range(6)], [(e.tops[1], k) for k in range(6)])
    e = ex["rhs1"]
    e.unpack_folded(1, fields, [(e.tops[1], i) for i in range(12)])
    end(rhs_moves[1])
    begin(rhs_moves[2])
    fill("u2", u2, 6, 1)
    end(rhs_moves[2])
    place(gathered_rhs, [(levels[3][2], 0)], h)

    for i in range(LOCAL, LEVELS):
        smooth(levels[i], 8, 8 + sizes[i], True)
        residual(levels[i], temp3, 8, 8 + sizes[i])
        restrict(temp3, levels[i + 1][2], 6, 8, 8, sizes[i + 1], levels[i][-1])
    conjugate(levels[LEVELS], temp3)
    for i in reversed(range(LOCAL, LEVELS)):
        prolong(levels[i + 1][0], levels[i][0], 8, sizes[i + 1], 8, levels[i][-1])
        smooth(levels[i], 8, 8 + sizes[i], False)

    u3 = levels[3][0]
    columns = u3.shape[2]
    r = lax.broadcasted_iota(jnp.int32, (columns, LANES), 0)
    c = lax.broadcasted_iota(jnp.int32, (columns, LANES), 1)
    hit = ((c & 1) == 0) & (c // 4 - LEFT // 4 + gy * 16 == r)
    widen = chosen(hit)

    for k in range(6):
        x = u3[k + 1, pl.ds(pl.multiple_of(gx * h, 8), h + 16), :]
        x = split_dot(x, widen)
        u2[k + 1, pl.ds(0, h + 16, 2), :] += x
        u2[k + 1, pl.ds(1, h + 16, 2), :] += x
    smooth(levels[2], lo, hi2, False)
    prolong(u2, u1, lo, n2 + 16, 0, 1)
    smooth(levels[1], lo, hi1, False)

    for k in range(6):
        x = u1[k + 1, lo : lo + n1 + 16, :]
        for c in (0, 8):
            u0[c + k + 1, pl.ds(0, n1 + 16, 2), :] += x
            u0[c + k + 1, pl.ds(1, n1 + 16, 2), :] += x
    smooth_pair(u0, rhs0, coef0, face, side, lo, hi0)

    r = lax.broadcasted_iota(jnp.int32, (2 * LANES, n0), 0)
    c = lax.broadcasted_iota(jnp.int32, (2 * LANES, n0), 1)
    join = chosen(c == 2 * (r % LANES - LEFT) + r // LANES)

    def give(k, carry):
        even = even_of(n0, k, 0)
        red, black = u0[k + 1, own, :], u0[k + 9, own, :]
        both = jnp.concatenate(
            [jnp.where(even, red, black), jnp.where(even, black, red)], axis=1
        )
        out[k] = split_dot(both, join)
        return carry

    lax.fori_loop(0, 6, give, 0)


def on_device(field, substance, patch, planar, vertical, storage, wattage):
    n0 = field.shape[1]
    nx, ny = lax.axis_size("gx"), lax.axis_size("gy")
    vmem = pl.BlockSpec(memory_space=pltpu.VMEM)
    smem = pl.BlockSpec(memory_space=pltpu.SMEM)
    scratch = scratches(n0, nx, ny)
    for e in exchanges(n0).values():
        scratch += e.scratch()
    return pl.pallas_call(
        whole_kernel,
        out_shape=jax.ShapeDtypeStruct(field.shape, F32),
        in_specs=[vmem] * 3 + [smem] * 4,
        out_specs=vmem,
        scratch_shapes=scratch,
        compiler_params=pltpu.CompilerParams(vmem_limit_bytes=VM, has_side_effects=True, collective_id=0),
    )(field, substance, patch, planar, vertical, storage, wattage)


def solution(mesh):
    placed = (P(None, "gx", "gy"), P(None, "gx", "gy"), P("gx", "gy"), P(), P(), P(), P())
    return jax.shard_map(
        on_device, mesh=mesh, in_specs=placed, out_specs=P(None, "gx", "gy"), check_vma=False
    )
```
